128 devices in a mesh: seq: 32 (over y, z, core), head: 4 (over x).
Axes of the slice: x: 4, y: 4, z: 4, core: 2. Of those that a mesh axis runs over, the one named last changes fastest.
Arguments:
- inputs: bfloat16 [8192, 2048], P('seq', 'head'), may hold values from -6 to 6
- w_query: bfloat16 [2048, 2048], P(None, 'head'), may hold values from -0.125 to 0.125
- w_key: bfloat16 [2048, 2048], P(None, 'head'), may hold values from -0.125 to 0.125
- w_value: bfloat16 [2048, 2048], P(None, 'head'), may hold values from -0.125 to 0.125
- sketch: float32 [2, 64, 32], replicated, may hold values from -0.75 to 0.75
- prefix_state: float32 [32, 1024, 64], P('head'), may hold values from -112 to 112
- prefix_norm: float32 [32, 1024], P('head'), as said below
- d_attn: bfloat16 [8192, 2048], P('seq', 'head'), may hold values from -256 to 256
- d_state_end: float32 [32, 1024, 64], P('head'), may hold values from -6 to 6
- d_norm_end: float32 [32, 1024], P('head'), may hold values from -4 to 4
Outputs:
- d_input: bfloat16 [8192, 2048], P('seq', 'head')
- d_query: bfloat16 [8192, 2048], P('seq', 'head')
- d_key: bfloat16 [8192, 2048], P('seq', 'head')
- d_value: bfloat16 [8192, 2048], P('seq', 'head')
- d_prefix_state: float32 [32, 1024, 64], P('head')
- d_prefix_norm: float32 [32, 1024], P('head')
The draws below stay inside these ranges and needn't reach their ends.
Inputs may be any that keep to these rules, and one draw needn't show every extreme that they name: For every head, prefix_norm laid out as a 32 x 32 matrix is symmetric positive semidefinite.
All inputs are finite; a program needn't handle non-finite values.
Results may differ from the reference program's by a relative error of at most 0.012.
Values may be sent and summed in bfloat16 or wider, within the bound.
A program may use at most 192 MiB of HBM per device.

```python
from functools import partial
import jax
import jax.numpy as jnp
from jax import lax

D = 2048
HEADS = 32
HD = 64
SK = 32
FEAT = 1024
TOK_DEV = 256
TOKENS = 8192


def draw_prefix_norm(key, part):
    points = jax.random.normal(jax.random.fold_in(key, 11), (HEADS, 64, SK), jnp.float32) * SK ** (-0.5)
    gram = jnp.einsum('hmi,hmj->hij', points, points) * (TOKENS / 64.0)
    return gram.reshape(HEADS, SK * SK).astype(jnp.float32)


def block_levels(stream_key, shape, shards, low, top_value):
    def one(dim, parts):
        draws = jax.random.uniform(jax.random.fold_in(jax.random.fold_in(stream_key, 6), dim), (parts,), jnp.float32, low / len(shards), top_value / len(shards))
        return jnp.repeat(jnp.exp(draws), shape[dim] // parts).reshape((-1,) + (1,) * (len(shape) - dim - 1))

    factor_of = one(*shards[0])
    for cut in shards[1:]:
        factor_of = factor_of * one(*cut)
    return factor_of


def normal_values(own_key, dims, deviation, bound, cuts=(), kind=jnp.bfloat16):
    level = block_levels(own_key, dims, cuts, -0.22, 0.18) if cuts else 1.0
    drawn = jax.random.normal(own_key, dims, jnp.float32) * deviation * level
    return jnp.minimum(jnp.maximum(drawn, -bound), bound).astype(kind)


def setup_inputs(seed: int = 0) -> dict:
    key_list = jax.random.split(jax.random.key(seed), 11)
    return {
        "inputs": normal_values(key_list[0], (TOKENS, D), 1.0, 6.0, ((0, 32), (1, 4))),
        "w_query": normal_values(key_list[1], (D, HEADS * HD), D ** -0.5, 0.125, ((1, 4),)),
        "w_key": normal_values(key_list[2], (D, HEADS * HD), D ** -0.5, 0.125, ((1, 4),)),
        "w_value": normal_values(key_list[3], (D, HEADS * HD), D ** -0.5, 0.125, ((1, 4),)),
        "sketch": normal_values(key_list[4], (2, HD, SK), HD ** -0.5, 0.75, (), jnp.float32),
        "prefix_state": normal_values(key_list[5], (HEADS, FEAT, HD), (0.2 * TOKENS ** 0.5), 112.0, ((0, 4),), jnp.float32),
        "prefix_norm": draw_prefix_norm(jax.random.fold_in(key_list[10], 71), 0),
        "d_attn": normal_values(key_list[7], (TOKENS, HEADS * HD), (0.5 * TOKENS ** 0.5), 256.0, ((0, 32), (1, 4))),
        "d_state_end": normal_values(key_list[8], (HEADS, FEAT, HD), 1.0, 6.0, ((0, 4),), jnp.float32),
        "d_norm_end": normal_values(key_list[9], (HEADS, FEAT), 0.3, 4.0, ((0, 4),), jnp.float32),
    }


HIGHEST_PRECISION = lax.Precision.HIGHEST

def sketch_map(values, sketch):
    left_map = jnp.einsum('hbd,de->hbe', values, sketch[0], precision=HIGHEST_PRECISION)
    right_map = jnp.einsum('hbd,de->hbe', values, sketch[1], precision=HIGHEST_PRECISION)
    return left_map * right_map * sketch.shape[2] ** (-0.5)

def square_features(sketched):
    outer_prod = sketched[:, :, :, None] * sketched[:, :, None, :]
    return outer_prod.reshape(sketched.shape[0], sketched.shape[1], -1)

def attend_block(carried, block_data, sketch):
    value_state, norm_state = carried
    query_block, key_block, value_block = block_data
    sketch_query = sketch_map(query_block, sketch)
    sketch_key = sketch_map(key_block, sketch)
    feat_query = square_features(sketch_query)
    feat_key = square_features(sketch_key)
    block_size = query_block.shape[1]
    causal = lax.broadcasted_iota(jnp.int32, (block_size, block_size), 0) >= lax.broadcasted_iota(jnp.int32, (block_size, block_size), 1)
    dot_prod = jnp.einsum('hid,hjd->hij', sketch_query, sketch_key, precision=HIGHEST_PRECISION)
    scores = jnp.where(causal, dot_prod * dot_prod, jnp.zeros_like(dot_prod))
    numerator = jnp.einsum('hif,hfd->hid', feat_query, value_state, precision=HIGHEST_PRECISION)
    numerator = numerator + jnp.einsum('hij,hjd->hid', scores, value_block, precision=HIGHEST_PRECISION)
    denominator = 1.0 + jnp.einsum('hif,hf->hi', feat_query, norm_state, precision=HIGHEST_PRECISION) + scores.sum(-1)
    outputs = numerator / denominator[:, :, None]
    value_state = value_state + jnp.einsum('hjf,hjd->hfd', feat_key, value_block, precision=HIGHEST_PRECISION)
    norm_state = norm_state + feat_key.sum(1)
    return ((value_state, norm_state), outputs)

def split_blocks(values, block_size):
    head_count, total_rows, depth_size = values.shape
    return values.reshape(head_count, total_rows // block_size, block_size, depth_size).transpose(1, 0, 2, 3)

def join_blocks(values):
    block_count, head_count, block_size, depth_size = values.shape
    return values.transpose(1, 0, 2, 3).reshape(head_count, block_count * block_size, depth_size)

def attend(query, key, value, value_state, norm_state, sketch):
    block_size = min(TOK_DEV, 512)
    block_step = jax.checkpoint(partial(attend_block, sketch=sketch))
    carried, outputs = lax.scan(block_step, (value_state, norm_state), (split_blocks(query, block_size), split_blocks(key, block_size), split_blocks(value, block_size)))
    return (join_blocks(outputs), carried[0], carried[1])

def reference(inputs, w_query, w_key, w_value, sketch, prefix_state, prefix_norm, d_attn, d_state_end, d_norm_end):

    def to_heads(values):
        return values.reshape(TOKENS, HEADS, HD).transpose(1, 0, 2).astype(jnp.float32)

    def flatten(values):
        return values.transpose(1, 0, 2).reshape(TOKENS, HEADS * HD).astype(jnp.bfloat16)
    query = to_heads(lax.optimization_barrier(jnp.dot(inputs, w_query, preferred_element_type=jnp.float32).astype(jnp.bfloat16)))
    key = to_heads(lax.optimization_barrier(jnp.dot(inputs, w_key, preferred_element_type=jnp.float32).astype(jnp.bfloat16)))
    value = to_heads(lax.optimization_barrier(jnp.dot(inputs, w_value, preferred_element_type=jnp.float32).astype(jnp.bfloat16)))

    def forward(query_in, key_in, value_in, state_in, norm_in):
        return attend(query_in, key_in, value_in, state_in, norm_in, sketch)
    primal, pull_back = jax.vjp(forward, query, key, value, prefix_state, prefix_norm)
    grad_query, grad_key, grad_value, grad_state, grad_norm = pull_back((to_heads(d_attn), d_state_end, d_norm_end))
    d_query = flatten(grad_query)
    d_key = flatten(grad_key)
    d_value = flatten(grad_value)
    d_input = jnp.dot(d_query, w_query.T, preferred_element_type=jnp.float32)
    d_input = d_input + jnp.dot(d_key, w_key.T, preferred_element_type=jnp.float32)
    d_input = d_input + jnp.dot(d_value, w_value.T, preferred_element_type=jnp.float32)
    return (d_input.astype(jnp.bfloat16), d_query, d_key, d_value, grad_state, grad_norm)
```

```python
import jax
import jax.numpy as jnp
from jax import lax
from jax.experimental import pallas as pl
from jax.experimental.pallas import tpu as pltpu
from jax.sharding import Mesh
from jax.sharding import PartitionSpec as P

SEQ = ("seq_0", "seq_1", "seq_2")
MESH = pl.DeviceIdType.MESH
F32 = jnp.float32
BF = jnp.bfloat16

SK = 32
NS = 17
NF = NS * SK
NP = 640
TOK = 256
CT = 512
CH = 16
ROWS = 80
OWN = 14
WIRE = OWN * ROWS
ZROW = 2 * NF


def nn(a, b):
    return lax.dot_general(a, b, (((1,), (0,)), ((), ())), preferred_element_type=F32)


def nt(a, b):
    return lax.dot_general(a, b, (((1,), (1,)), ((), ())), preferred_element_type=F32)


def kernel(
    x_hbm, wq_hbm, wk_hbm, wv_hbm, g_hbm, ps_hbm, pn_hbm, da_hbm, de_hbm, dn_hbm,
    oi_hbm, oq_hbm, ok_hbm, ov_hbm, os_hbm, on_hbm,
    xg, w, acc, qkv, xsend, ga, gt, psv, pnv, dev, dnv, dps, dpn,
    bd, bdh, bdl, bdt, lrt, skt, skb, stok, feat, vtm, vtok, dext, fold, stk, fsel,
    yloc, gtr, scr, dmat, wmat, yv, tmp, zst, zpad, dfe, dst, dvt, sext, sextt,
    wire, inb, outb, res, totb, tot, dtok, dall, acc2, rsend, rrecv, oin,
    loc, ag_s, ag_r, ex_s, ex_r, a_s, a_r, b_s, b_r, t_s, t_r, rs_s, rs_r,
):
    y = lax.axis_index("seq_0")
    z = lax.axis_index("seq_1")
    c = lax.axis_index("seq_2")
    x = lax.axis_index("head")
    m = y * 4 + z
    oc = 1 - c
    right, left, far = lax.rem(x + 1, 4), lax.rem(x + 3, 4), lax.rem(x + 2, 4)

    def rc(src, dst_, ss, rs, **where):
        return pltpu.make_async_remote_copy(
            src_ref=src, dst_ref=dst_, send_sem=ss, recv_sem=rs,
            device_id=where, device_id_type=MESH,
        )

    own_cols = pl.ds(pl.multiple_of(c * 256, 256), 256)
    oth_cols = pl.ds(pl.multiple_of(oc * 256, 256), 256)

    lx = [
        pltpu.make_async_copy(x_hbm.at[:, 256 * k : 256 * k + 256], xg.at[2 * x + k], loc.at[k])
        for k in range(2)
    ]
    lw = [
        pltpu.make_async_copy(src, w.at[t], loc.at[2 + t])
        for t, src in enumerate((wq_hbm, wk_hbm, wv_hbm))
    ]
    lg = pltpu.make_async_copy(g_hbm, gt, loc.at[5])
    la = pltpu.make_async_copy(da_hbm.at[:, own_cols], ga.at[c], loc.at[6])
    ln = pltpu.make_async_copy(pn_hbm, pnv, loc.at[7])
    lp = pltpu.make_async_copy(ps_hbm.at[pl.ds(4 * c, 4)], psv, loc.at[8])
    le = pltpu.make_async_copy(de_hbm, dev, loc.at[9])
    lm = pltpu.make_async_copy(dn_hbm, dnv, loc.at[10])
    for copy in (lx[0], lx[1], lw[1], lw[2], lw[0], lg, la, ln, lp, le, lm):
        copy.start()

    bar = pltpu.get_barrier_semaphore()
    for peer in (right, left):
        pl.semaphore_signal(bar, inc=1, device_id={"head": peer}, device_id_type=MESH)
    pl.semaphore_signal(bar, inc=1, device_id={"seq_2": oc}, device_id_type=MESH)

    def greet(d, _):
        r = lax.rem(m + d, CH)
        pl.semaphore_signal(
            bar, inc=1, device_id={"seq_0": r // 4, "seq_1": lax.rem(r, 4)}, device_id_type=MESH
        )
        return 0

    lax.fori_loop(1, CH, greet, 0)
    pl.semaphore_wait(bar, 18)

    def slab(src, k, peer, i):
        ref = xg.at[2 * src + k]
        return rc(ref, ref, ag_s.at[i], ag_r.at[i], head=peer)

    ag = [
        slab(x, 0, right, 0), slab(x, 1, left, 1), slab(x, 1, right, 2), slab(x, 0, left, 3),
        slab(left, 0, right, 4), slab(right, 1, left, 5),
    ]
    lx[0].wait()
    lx[1].wait()
    for i in range(4):
        ag[i].start()
    cga = rc(da_hbm.at[:, oth_cols], ga.at[c], ex_s.at[0], ex_r.at[0], seq_2=oc)
    cga.start()

    lg.wait()
    bd[...] = jnp.zeros((256, 256), F32)
    lane128 = lax.broadcasted_iota(jnp.int32, (SK, 128), 1) // 64
    for lr in range(2):
        wide = jnp.concatenate([gt[lr], gt[lr]], axis=1)
        for h in range(4):
            row = lr * 128 + h * SK
            col = 128 * (h // 2)
            bd[row : row + SK, col : col + 128] = jnp.where(lane128 == h % 2, wide, 0.0)
    bdh[...] = bd[...].astype(BF)
    bdl[...] = (bd[...] - bdh[...].astype(F32)).astype(BF)
    bdt[0] = jnp.transpose(bd[...]).astype(BF)
    bdt[1] = (jnp.transpose(bd[...]) - bdt[0].astype(F32)).astype(BF)

    for t in range(3):
        lw[(1, 2, 0)[t]].wait()

    def project(src, first):
        for t in range(3):
            out = nn(xg[2 * src], w[t, pl.ds(pl.multiple_of(src * 512, 512), 256), :])
            out = out + nn(xg[2 * src + 1], w[t, pl.ds(pl.multiple_of(src * 512 + 256, 256), 256), :])
            if first:
                acc[t] = out
            else:
                acc[t] += out

    project(x, True)
    ag[0].wait_recv()
    ag[4].start()
    ag[1].wait_recv()
    ag[5].start()

    def build(i, _):
        f = lax.broadcasted_iota(jnp.int32, (SK, 1024), 1)
        fi, fj = f // SK, lax.rem(f, SK)
        a = lax.broadcasted_iota(jnp.int32, (SK, 1024), 0)
        b = lax.rem(a + i, SK)
        hit = ((fi == a) & (fj == b)) | ((fi == b) & (fj == a))
        value = jnp.where(i == 16, 0.5, 1.0)
        keep = jnp.where(i < NS, value, 0.0)
        fsel[pl.ds(pl.multiple_of(i * SK, SK), SK), :] = jnp.where(hit, keep, 0.0).astype(BF)
        return 0

    lax.fori_loop(0, NP // SK, build, 0)
    for h in range(4):
        for q in range(2):
            feat[q, h, NF:NP, :] = jnp.zeros((NP - NF, CT), BF)
    zpad[...] = jnp.zeros((128, NP), F32)
    tmp[...] = jnp.zeros((NP, 128), F32)
    dext[...] = jnp.zeros(dext.shape, BF)
    stk[...] = jnp.zeros(stk.shape, BF)
    zst[...] = jnp.zeros((SK, 128), F32)
    vtm[...] = jnp.zeros(vtm.shape, BF)
    sext[...] = jnp.zeros(sext.shape, F32)

    ag[2].wait_recv()
    project(left, False)
    ag[3].wait_recv()
    project(right, False)
    ag[4].wait_recv()
    ag[5].wait_recv()

    cqkv = {}
    for t in (1, 2, 0):
        dst_ref = qkv.at[t, c]
        cqkv[t] = rc(xsend.at[t], dst_ref, ex_s.at[1 + t], ex_r.at[1 + t], seq_2=oc)
        for cols, target in ((oth_cols, None), (own_cols, c)):
            out = acc[t, :, cols] + nn(
                xg[2 * far], w[t, pl.ds(pl.multiple_of(far * 512, 512), 256), cols]
            )
            out = out + nn(
                xg[2 * far + 1], w[t, pl.ds(pl.multiple_of(far * 512 + 256, 256), 256), cols]
            )
            if target is None:
                xsend[t] = out.astype(BF)
                cqkv[t].start()
            else:
                qkv[t, target] = out.astype(BF)

    scale = SK ** (-0.5)

    def sketch(t):
        for k in range(2):
            part = slice(256 * k, 256 * k + 256)
            lrt[t, :, part] = nt(bdh[...], qkv[t, k]) + nt(bdl[...], qkv[t, k])
            tok = nt(qkv[t, k], bdh[...]) + nt(qkv[t, k], bdl[...])
            stok[t, part, :] = (tok[:, :128] * tok[:, 128:] * scale).astype(BF)
        skt[t] = lrt[t, :128, :] * lrt[t, 128:, :] * scale
        skb[t] = skt[t].astype(BF)

        def one(h, _):
            s = skt[t, pl.ds(pl.multiple_of(h * SK, SK), SK), :]
            for i in range(NS):
                other = s if i == 0 else pltpu.roll(s, SK - i, 0)
                feat[t, h, SK * i : SK * i + SK, :] = (s * other).astype(BF)
            return 0

        lax.fori_loop(0, 4, one, 0)

    lane256 = lax.broadcasted_iota(jnp.int32, (CT, 256), 1)

    def pack_z(total):
        tmp[0:NF, :] = total
        zt = jnp.transpose(tmp[...])
        for j in range(5):
            zst[4 * j : 4 * j + 4, :] = zt[0:4, 128 * j : 128 * j + 128]
        wire[ZROW:WIRE, :] = zst[...].astype(BF)

    cqkv[1].wait_recv()
    sketch(1)
    cqkv[2].wait_recv()
    for p in range(2):
        for k in range(2):
            vtok[p, 256 * k : 256 * k + 256, 0:128] = qkv[2, k, :, 128 * p : 128 * p + 128]
        vtok[p, :, 128:256] = jnp.ones((CT, 128), BF)
    ztot = None
    for p in range(2):
        out = None
        for hh in range(2):
            h = 2 * p + hh
            keep = (lane256 // 64 == hh) | (lane256 == 128 + h)
            vm = jnp.where(keep, vtok[p].astype(F32), 0.0).astype(BF)
            part = nn(feat[1, h, 0:NF, :], vm)
            out = part if out is None else out + part
        wire[NF * p : NF * p + NF, :] = out[:, 0:128].astype(BF)
        ztot = out[:, 128:256] if ztot is None else ztot + out[:, 128:256]
    pack_z(ztot)

    def scan_send(n):
        def one(d, _):
            r = lax.rem(m + d, CH)

            @pl.when(r < OWN)
            def _():
                rc(
                    wire.at[pl.ds(pl.multiple_of(r * ROWS, ROWS), ROWS)], inb.at[n, m],
                    a_s.at[n, r], a_r.at[n, m], seq_0=r // 4, seq_1=lax.rem(r, 4),
                ).start()

            return 0

        lax.fori_loop(1, CH, one, 0)

        @pl.when(m < OWN)
        def _():
            inb[n, m] = wire[pl.ds(pl.multiple_of(m * ROWS, ROWS), ROWS), :]

    def a_copy(n, r):
        return rc(
            wire.at[pl.ds(0, ROWS)], inb.at[n, r], a_s.at[n, r], a_r.at[n, r],
            seq_0=r // 4, seq_1=lax.rem(r, 4),
        )

    def mine(ref):
        return ref.at[pl.ds(pl.multiple_of(m * ROWS, ROWS), ROWS)]

    def b_copy(n, r):
        return rc(
            outb.at[n, r], mine(res.at[n]), b_s.at[n, r], b_r.at[n, m],
            seq_0=r // 4, seq_1=lax.rem(r, 4),
        )

    def t_copy(r):
        return rc(
            totb, mine(tot.at[c]), t_s.at[r], t_r.at[m], seq_0=r // 4, seq_1=lax.rem(r, 4)
        )

    def scan_own(n, reverse):
        @pl.when(m < OWN)
        def _():
            def one(i, running):
                r = CH - 1 - i if reverse else i

                @pl.when(r != m)
                def _():
                    a_copy(n, r).wait_recv()

                outb[n, r] = running.astype(BF)

                @pl.when(r != m)
                def _():
                    b_copy(n, r).start()

                @pl.when(r == m)
                def _():
                    res[n, pl.ds(pl.multiple_of(m * ROWS, ROWS), ROWS), :] = running.astype(BF)

                return running + inb[n, r].astype(F32)

            total = lax.fori_loop(0, CH, one, jnp.zeros((ROWS, 128), F32))
            if reverse:
                totb[...] = total.astype(BF)
                tot[c, pl.ds(pl.multiple_of(m * ROWS, ROWS), ROWS), :] = total.astype(BF)

                def share(d, _):
                    t_copy(lax.rem(m + d, CH)).start()
                    return 0

                lax.fori_loop(1, CH, share, 0)

    def from_owners(make):
        def one(s, _):
            @pl.when(s != m)
            def _():
                make(s).wait_recv()

            return 0

        lax.fori_loop(0, OWN, one, 0)

    def b_in(n, s):
        block = res.at[n, pl.ds(pl.multiple_of(s * ROWS, ROWS), ROWS)]
        return rc(outb.at[n, s], block, b_s.at[n, s], b_r.at[n, s], seq_0=s // 4, seq_1=lax.rem(s, 4))

    def t_in(s):
        block = tot.at[c, pl.ds(pl.multiple_of(s * ROWS, ROWS), ROWS)]
        return rc(totb, block, t_s.at[s], t_r.at[s], seq_0=s // 4, seq_1=lax.rem(s, 4))

    def sends_done(n):
        def one(d, _):
            r = lax.rem(m + d, CH)

            @pl.when(r < OWN)
            def _():
                a_copy(n, r).wait_send()

            @pl.when(m < OWN)
            def _():
                b_copy(n, r).wait_send()
                if n == 1:
                    t_copy(r).wait_send()

            return 0

        lax.fori_loop(1, CH, one, 0)

    def fold_in(state, norm):
        stk[0:256, :] = state
        pick = jnp.where(c == 0, norm[0:4, :], norm[4:8, :])
        stk[256:272, :] = jnp.concatenate([pick, jnp.zeros((12, 1024), F32)], axis=0).astype(BF)
        fold[...] = nt(fsel[...], stk[...])

    row_w = lax.broadcasted_iota(jnp.int32, (NF, 128), 0)
    weight = jnp.where((row_w < SK) | (row_w >= 16 * SK), 1.0, 2.0)

    def unpack(n):
        zst[...] = res[n, ZROW:WIRE, :].astype(F32)
        for j in range(5):
            zpad[0:4, 128 * j : 128 * j + 128] = zst[4 * j : 4 * j + 4, :]
        zc = jnp.transpose(zpad[...])[0:NF, :] * weight + fold[0:NF, 256:384]
        for p in range(2):
            part = res[n, NF * p : NF * p + NF, :].astype(F32)
            sext[p, 0:NF, 0:128] = part * weight + fold[0:NF, 128 * p : 128 * p + 128]
            sext[p, 0:NF, 128:256] = zc
            sextt[p] = jnp.transpose(sext[p])[0:144, :].astype(BF)

    scan_send(0)

    lp.wait()
    ln.wait()
    fold_in(psv[...].reshape(256, 1024).astype(BF), pnv)
    cqkv[0].wait_recv()
    sketch(0)

    scan_own(0, False)

    la.wait()
    cga.wait_recv()
    for k in range(2):
        part = slice(256 * k, 256 * k + 256)
        gtr[:, part] = jnp.transpose(ga[k].astype(F32))
        vt = jnp.transpose(qkv[2, k].astype(F32)).astype(BF)
        for h in range(4):
            vtm[h, 64 * (h % 2) : 64 * (h % 2) + 64, part] = vt[64 * h : 64 * h + 64, :]
    row16 = lax.broadcasted_iota(jnp.int32, (16, CT), 0)
    for h in range(4):
        vtm[h, 128:144, :] = jnp.where(row16 == h, 1.0, 0.0).astype(BF)

    diag = lax.broadcasted_iota(jnp.int32, (256, 256), 0) <= lax.broadcasted_iota(
        jnp.int32, (256, 256), 1
    )
    lane_k = lax.broadcasted_iota(jnp.int32, (256, 128), 1) // SK

    def scores(h, _):
        for jb in range(2):
            keys = jnp.where(lane_k == h, stok[1, 256 * jb : 256 * jb + 256, :].astype(F32), 0.0)
            keys = keys.astype(BF)
            for ib in range(jb, 2):
                d = nn(keys, skb[0, :, 256 * ib : 256 * ib + 256])
                if ib == jb:
                    d = jnp.where(diag, d, 0.0)
                at = (h, slice(256 * jb, 256 * jb + 256), slice(256 * ib, 256 * ib + 256))
                scr[at] = (d * d).astype(BF)
                dmat[at] = (d + d).astype(BF)
        yloc[h, :, 0:256] = nn(vtm[h, 0:144, 0:256], scr[h, 0:256, 0:256])
        yloc[h, :, 256:512] = nn(vtm[h, 0:144, :], scr[h, :, 256:512])
        return 0

    lax.fori_loop(0, 4, scores, 0)

    from_owners(lambda s: b_in(0, s))
    unpack(0)
    ztot = None
    for p in range(2):
        out = None
        for hh in range(2):
            h = 2 * p + hh
            yv[...] = nn(sextt[p], feat[0, h]) + yloc[h]
            num = yv[64 * hh : 64 * hh + 64, :]
            inv = 1.0 / (1.0 + yv[128 + h : 129 + h, :])
            g = gtr[64 * h : 64 * h + 64, :]
            dden = -jnp.sum(g * num, axis=0, keepdims=True) * inv * inv
            dext[h, 64 * hh : 64 * hh + 64, :] = (g * inv).astype(BF)
            dext[h, 128:144, :] = jnp.where(row16 == h, dden, 0.0).astype(BF)
            part = nt(feat[0, h, 0:NF, :], dext[h])
            out = part if out is None else out + part
        if p == 0:

            def first_sent(d, _):
                r = lax.rem(m + d, CH)

                @pl.when(r < OWN)
                def _():
                    a_copy(0, r).wait_send()

                return 0

            lax.fori_loop(1, CH, first_sent, 0)
        wire[NF * p : NF * p + NF, :] = out[:, 0:128].astype(BF)
        ztot = out[:, 128:256] if ztot is None else ztot + out[:, 128:256]
    pack_z(ztot)
    scan_send(1)

    def feature_grad(t, h, extra):
        s = skt[t, pl.ds(pl.multiple_of(h * SK, SK), SK), :]
        here = 2.0 * s * dfe[0:SK, :]
        for i in range(1, NS):
            d = dfe[SK * i : SK * i + SK, :]
            here = here + d * pltpu.roll(s, SK - i, 0) + pltpu.roll(d * s, i, 0)
        dst[t, pl.ds(pl.multiple_of(h * SK, SK), SK), :] = here + extra

    def local_grads(h, _):
        p = h // 2
        for jb in range(2):
            for ib in range(jb, 2):
                at = (h, slice(256 * jb, 256 * jb + 256), slice(256 * ib, 256 * ib + 256))
                ds = nn(vtok[p, 256 * jb : 256 * jb + 256, :], dext[h, :, 256 * ib : 256 * ib + 256])
                wmat[at] = (dmat[at].astype(F32) * ds).astype(BF)
        sk_rows = pl.ds(pl.multiple_of(h * SK, SK), SK)
        d_rows = pl.ds(pl.multiple_of(64 * lax.rem(h, 2), 64), 64)
        v_rows = pl.ds(pl.multiple_of(64 * h, 64), 64)
        dst[0, sk_rows, 0:256] = nn(skb[1, sk_rows, 0:256], wmat[h, 0:256, 0:256])
        dst[0, sk_rows, 256:512] = nn(skb[1, sk_rows, :], wmat[h, :, 256:512])
        dst[1, sk_rows, 0:256] = nt(skb[0, sk_rows, :], wmat[h, 0:256, :])
        dst[1, sk_rows, 256:512] = nt(skb[0, sk_rows, 256:512], wmat[h, 256:512, 256:512])
        dvt[v_rows, 0:256] = nt(dext[h, d_rows, :], scr[h, 0:256, :])
        dvt[v_rows, 256:512] = nt(dext[h, d_rows, 256:512], scr[h, 256:512, 256:512])
        return 0

    def through_sketch(t):
        lt, rt = lrt[t, :128, :], lrt[t, 128:, :]
        ds = dst[t] * scale
        dlr = jnp.concatenate([ds * rt, ds * lt], axis=0).astype(BF)
        return nn(bdt[0], dlr) + nn(bdt[1], dlr)

    own_rows = pl.ds(pl.multiple_of(c * 256, 256), 256)
    oth_rows = pl.ds(pl.multiple_of(oc * 256, 256), 256)

    def hand_over(t, grad):
        dtok[t] = jnp.transpose(grad).astype(BF)
        copy = rc(dtok.at[t, oth_rows], dall.at[t, c], ex_s.at[4 + t], ex_r.at[4 + t], seq_2=oc)
        copy.start()
        dall[t, c] = dtok[t, own_rows, :]
        return copy

    lax.fori_loop(0, 4, local_grads, 0)

    def grad_q(h, _):
        dfe[...] = nn(sext[h // 2, 0:NF, :].astype(BF), dext[h])
        feature_grad(0, h, dst[0, pl.ds(pl.multiple_of(h * SK, SK), SK), :])
        return 0

    lax.fori_loop(0, 4, grad_q, 0)
    copy_q = hand_over(0, through_sketch(0))

    scan_own(1, True)

    le.wait()
    lm.wait()
    fold_in(dev[pl.ds(4 * c, 4)].reshape(256, 1024).astype(BF), dnv)
    copy_q.wait_recv()

    def store(t, ref, base):
        made = [
            pltpu.make_async_copy(dall.at[t, k], ref.at[:, 256 * k : 256 * k + 256], loc.at[base + k])
            for k in range(2)
        ]
        for one in made:
            one.start()
        return made

    stores = store(0, oq_hbm, 11)

    def pull(t, b):
        out = None
        for k in range(2):
            part = nt(dall[t, k], w[t, pl.ds(pl.multiple_of(b * 512, 512), 512), 256 * k : 256 * k + 256])
            out = part if out is None else out + part
        return out

    def pull_q(b, _):
        acc2[b] = pull(0, b)
        return 0

    lax.fori_loop(0, 4, pull_q, 0)

    from_owners(lambda s: b_in(1, s))
    unpack(1)

    def grad_v(h, _):
        v_rows = pl.ds(pl.multiple_of(64 * h, 64), 64)
        d_rows = pl.ds(pl.multiple_of(64 * lax.rem(h, 2), 64), 64)
        dvt[v_rows, :] += nn(sextt[h // 2, d_rows, :], feat[1, h])
        return 0

    def grad_k(h, _):
        dfe[...] = nn(sext[h // 2, 0:NF, :].astype(BF), vtm[h])
        feature_grad(1, h, dst[1, pl.ds(pl.multiple_of(h * SK, SK), SK), :])
        return 0

    lax.fori_loop(0, 4, grad_v, 0)
    copy_v = hand_over(2, dvt[...])
    lax.fori_loop(0, 4, grad_k, 0)
    copy_k = hand_over(1, through_sketch(1))
    copy_v.wait_recv()
    stores += store(2, ov_hbm, 13)
    copy_k.wait_recv()
    stores += store(1, ok_hbm, 15)

    def block(b):
        return acc2[b] + pull(1, b) + pull(2, b)

    rs = [
        rc(rsend.at[i], rrecv.at[i], rs_s.at[i], rs_r.at[i], head=right if i in (0, 2, 4) else left)
        for i in range(6)
    ]
    out = block(far)
    rsend[0] = out[:, 0:256].astype(BF)
    rs[0].start()
    rsend[1] = out[:, 256:512].astype(BF)
    rs[1].start()
    out = block(right)
    rsend[2] = out[:, 256:512].astype(BF)
    rs[2].start()
    keep_a = out[:, 0:256]
    acc2[right, :, 0:256] = keep_a
    out = block(left)
    rsend[3] = out[:, 0:256].astype(BF)
    rs[3].start()
    rs[0].wait_recv()
    rsend[4] = (acc2[right, :, 0:256] + rrecv[0].astype(F32)).astype(BF)
    rs[4].start()
    acc2[left, :, 256:512] = out[:, 256:512]
    rs[1].wait_recv()
    rsend[5] = (acc2[left, :, 256:512] + rrecv[1].astype(F32)).astype(BF)
    rs[5].start()
    acc2[x] = block(x)

    from_owners(t_in)
    whole = tot.at[c]
    copy_t = rc(whole, whole, ex_s.at[7], ex_r.at[7], seq_2=oc)
    copy_t.start()

    def totals(k):
        for p in range(2):
            tmp[0:NF, :] = tot[k, NF * p : NF * p + NF, :].astype(F32)
            part = nn(jnp.transpose(tmp[...]).astype(BF), fsel[...])
            for hh in range(2):
                h = 4 * k + 2 * p + hh
                dps[h] = dev[h] + part[64 * hh : 64 * hh + 64, :]
        zst[...] = tot[k, ZROW:WIRE, :].astype(F32)
        for j in range(5):
            zpad[pl.ds(pl.multiple_of(8 * k, 8), 4), 128 * j : 128 * j + 128] = zst[4 * j : 4 * j + 4, :]

    def put_state(k, sem):
        heads = pl.ds(4 * k, 4)
        return pltpu.make_async_copy(dps.at[heads], os_hbm.at[heads], loc.at[sem])

    totals(c)
    put_state(c, 17).start()
    copy_t.wait_recv()
    totals(oc)
    put_state(oc, 18).start()
    norms = nn(zpad[0:16, :].astype(BF), fsel[...])
    dpn[0:4, :] = dnv[0:4, :] + norms[0:4, :]
    dpn[4:8, :] = dnv[4:8, :] + norms[8:12, :]
    put_norm = pltpu.make_async_copy(dpn, on_hbm, loc.at[19])
    put_norm.start()

    rs[2].wait_recv()
    rs[3].wait_recv()
    rs[4].wait_recv()
    oin[:, 0:256] = (acc2[x, :, 0:256] + rrecv[3].astype(F32) + rrecv[4].astype(F32)).astype(BF)
    rs[5].wait_recv()
    oin[:, 256:512] = (acc2[x, :, 256:512] + rrecv[2].astype(F32) + rrecv[5].astype(F32)).astype(BF)
    put_in = pltpu.make_async_copy(oin, oi_hbm, loc.at[20])
    put_in.start()

    for one in ag + list(cqkv.values()) + [cga, copy_q, copy_v, copy_k, copy_t] + rs:
        one.wait_send()

    def rest_sent(d, _):
        r = lax.rem(m + d, CH)

        @pl.when(r < OWN)
        def _():
            a_copy(1, r).wait_send()

        @pl.when(m < OWN)
        def _():
            b_copy(0, r).wait_send()
            b_copy(1, r).wait_send()
            t_copy(r).wait_send()

        return 0

    lax.fori_loop(1, CH, rest_sent, 0)
    for one in stores:
        one.wait()
    put_state(c, 17).wait()
    put_state(oc, 18).wait()
    put_norm.wait()
    put_in.wait()


def body(x, wq, wk, wv, sketch, prefix_state, prefix_norm, d_attn, d_state, d_norm):
    any_ = pl.BlockSpec(memory_space=pl.ANY)
    out_shape = (
        jax.ShapeDtypeStruct((TOK, 512), BF),
        jax.ShapeDtypeStruct((TOK, 512), BF),
        jax.ShapeDtypeStruct((TOK, 512), BF),
        jax.ShapeDtypeStruct((TOK, 512), BF),
        jax.ShapeDtypeStruct((8, 64, 1024), F32),
        jax.ShapeDtypeStruct((8, 1024), F32),
    )
    v = pltpu.VMEM
    scratch = [
        v((8, TOK, 256), BF),
        v((3, 2048, 512), BF),
        v((3, TOK, 512), F32),
        v((3, 2, TOK, 256), BF),
        v((3, TOK, 256), BF),
        v((2, TOK, 256), BF),
        v((2, SK, 64), F32),
        v((4, 64, 1024), F32),
        v((8, 1024), F32),
        v((8, 64, 1024), F32),
        v((8, 1024), F32),
        v((8, 64, 1024), F32),
        v((8, 1024), F32),
        v((256, 256), F32),
        v((256, 256), BF),
        v((256, 256), BF),
        v((2, 256, 256), BF),
        v((2, 256, CT), F32),
        v((2, 128, CT), F32),
        v((2, 128, CT), BF),
        v((2, CT, 128), BF),
        v((2, 4, NP, CT), BF),
        v((4, 256, CT), BF),
        v((2, CT, 256), BF),
        v((4, 256, CT), BF),
        v((NP, 384), F32),
        v((384, 1024), BF),
        v((NP, 1024), BF),
        v((4, 144, CT), F32),
        v((256, CT), F32),
        v((4, CT, CT), BF),
        v((4, CT, CT), BF),
        v((4, CT, CT), BF),
        v((144, CT), F32),
        v((NP, 128), F32),
        v((SK, 128), F32),
        v((128, NP), F32),
        v((NF, CT), F32),
        v((2, 128, CT), F32),
        v((256, CT), F32),
        v((2, NP, 256), F32),
        v((2, 144, NP), BF),
        v((WIRE, 128), BF),
        v((2, CH, ROWS, 128), BF),
        v((2, CH, ROWS, 128), BF),
        v((2, WIRE, 128), BF),
        v((ROWS, 128), BF),
        v((2, WIRE, 128), BF),
        v((3, CT, 256), BF),
        v((3, 2, TOK, 256), BF),
        v((4, TOK, 512), F32),
        v((6, TOK, 256), BF),
        v((6, TOK, 256), BF),
        v((TOK, 512), BF),
    ]
    sem = pltpu.SemaphoreType.DMA
    scratch += [
        sem((21,)), sem((6,)), sem((6,)), sem((8,)), sem((8,)), sem((2, CH)), sem((2, CH)),
        sem((2, CH)), sem((2, CH)), sem((CH,)), sem((CH,)), sem((6,)), sem((6,)),
    ]
    swap = (0, 2, 1)
    outs = pl.pallas_call(
        kernel,
        out_shape=out_shape,
        in_specs=[any_] * 10,
        out_specs=(any_,) * 6,
        scratch_shapes=scratch,
        compiler_params=pltpu.CompilerParams(
            collective_id=0, has_side_effects=True, vmem_limit_bytes=60 * 1024 * 1024
        ),
        name="sketch_bwd",
    )(
        x, wq, wk, wv, jnp.transpose(sketch, swap), jnp.transpose(prefix_state, swap),
        prefix_norm, d_attn, jnp.transpose(d_state, swap), d_norm,
    )
    return outs[:4] + (jnp.transpose(outs[4], swap), outs[5])


def solution(mesh):
    finer = Mesh(
        mesh.devices.reshape(4, 4, 2, mesh.shape["head"]), ("seq_0", "seq_1", "seq_2", "head")
    )
    state, rows = P("head", None, None), P("head", None)
    tokens, weight = P(SEQ, "head"), P(None, "head")
    return jax.shard_map(
        body,
        mesh=finer,
        in_specs=(tokens, weight, weight, weight, P(), state, rows, tokens, state, rows),
        out_specs=(tokens, tokens, tokens, tokens, state, rows),
        check_vma=False,
    )
```

```python
import jax
import jax.numpy as jnp
from jax import lax
from jax.experimental import pallas as pl
from jax.experimental.pallas import tpu as pltpu
from jax.sharding import Mesh
from jax.sharding import PartitionSpec as P

SEQ = ("seq_0", "seq_1", "seq_2")
MESH = pl.DeviceIdType.MESH
F32 = jnp.float32
BF = jnp.bfloat16

SK = 32
NS = 17
NF = NS * SK
NP = 640
TOK = 256
CT = 512
CH = 16
ROWS = 80
OWN = 14
WIRE = OWN * ROWS
FAR_FIRST = (10, 9, 11, 6, 14, 2, 8, 5, 7, 13, 15, 1, 3, 4, 12)
ZROW = 2 * NF
SPLIT = NF // ROWS


def nn(a, b):
    return lax.dot_general(a, b, (((1,), (0,)), ((), ())), preferred_element_type=F32)


def nt(a, b):
    return lax.dot_general(a, b, (((1,), (1,)), ((), ())), preferred_element_type=F32)


def kernel(
    x_hbm, wq_hbm, wk_hbm, wv_hbm, g_hbm, ps_hbm, pn_hbm, da_hbm, de_hbm, dn_hbm,
    oin, oqkv, dps, dpn,
    xg, w, acc, qkv, xsend, ga, gt, psv, pnv, dev, dnv,
    bd, bdh, bdl, bdt, lrt, skt, skb, stok, feat, vtm, vtok, dext, fold, stk, fsel,
    yloc, gtr, scr, dmat, wmat, yv, tmp, zst, zpad, dfe, dst, dvt, sext, sextt, sextb,
    wire, inb, outb, res, totb, tot, dtok, dall, acc2, rsend, rrecv,
    loc, ag_s, ag_r, ex_s, ex_r, a_s, a_r, b_s, b_r, t_s, t_r, rs_s, rs_r,
):
    y = lax.axis_index("seq_0")
    z = lax.axis_index("seq_1")
    c = lax.axis_index("seq_2")
    x = lax.axis_index("head")
    m = y * 4 + z
    oc = 1 - c
    right, left, far = lax.rem(x + 1, 4), lax.rem(x + 3, 4), lax.rem(x + 2, 4)

    def rc(src, dst_, ss, rs, **where):
        return pltpu.make_async_remote_copy(
            src_ref=src, dst_ref=dst_, send_sem=ss, recv_sem=rs,
            device_id=where, device_id_type=MESH,
        )

    own_cols = pl.ds(pl.multiple_of(c * 256, 256), 256)
    oth_cols = pl.ds(pl.multiple_of(oc * 256, 256), 256)

    lx = [
        pltpu.make_async_copy(x_hbm.at[:, 256 * k : 256 * k + 256], xg.at[2 * x + k], loc.at[k])
        for k in range(2)
    ]
    lw = [
        pltpu.make_async_copy(src, w.at[t], loc.at[2 + t])
        for t, src in enumerate((wq_hbm, wk_hbm, wv_hbm))
    ]
    lg = pltpu.make_async_copy(g_hbm, gt, loc.at[5])
    la = pltpu.make_async_copy(da_hbm.at[:, own_cols], ga.at[c], loc.at[6])
    ln = pltpu.make_async_copy(pn_hbm, pnv, loc.at[7])
    lp = pltpu.make_async_copy(ps_hbm.at[pl.ds(4 * c, 4)], psv, loc.at[8])
    le = pltpu.make_async_copy(de_hbm, dev, loc.at[9])
    lm = pltpu.make_async_copy(dn_hbm, dnv, loc.at[10])
    for copy in (lx[0], lx[1], lw[1], lw[2], lw[0], lg, la, ln, lp, le, lm):
        copy.start()

    bar = pltpu.get_barrier_semaphore()
    for peer in (right, left):
        pl.semaphore_signal(bar, inc=1, device_id={"head": peer}, device_id_type=MESH)
    pl.semaphore_signal(bar, inc=1, device_id={"seq_2": oc}, device_id_type=MESH)

    def greet(d, _):
        r = lax.rem(m + d, CH)
        pl.semaphore_signal(
            bar, inc=1, device_id={"seq_0": r // 4, "seq_1": lax.rem(r, 4)}, device_id_type=MESH
        )
        return 0

    lax.fori_loop(1, CH, greet, 0)
    pl.semaphore_wait(bar, 18)

    def slab(src, k, peer, i):
        ref = xg.at[2 * src + k]
        return rc(ref, ref, ag_s, ag_r.at[i], head=peer)

    ag = [
        slab(x, 0, right, 0), slab(x, 1, left, 1), slab(x, 1, right, 2), slab(x, 0, left, 3),
        slab(left, 0, right, 4), slab(right, 1, left, 5),
    ]
    lx[0].wait()
    lx[1].wait()
    for i in range(4):
        ag[i].start()
    cga = rc(da_hbm.at[:, oth_cols], ga.at[c], ex_s.at[0], ex_r.at[0], seq_2=oc)
    cga.start()

    lg.wait()
    bd[...] = jnp.zeros((256, 256), F32)
    lane128 = lax.broadcasted_iota(jnp.int32, (SK, 128), 1) // 64
    for lr in range(2):
        wide = jnp.concatenate([gt[lr], gt[lr]], axis=1)
        for h in range(4):
            row = lr * 128 + h * SK
            col = 128 * (h // 2)
            bd[row : row + SK, col : col + 128] = jnp.where(lane128 == h % 2, wide, 0.0)
    bdh[...] = bd[...].astype(BF)
    bdl[...] = (bd[...] - bdh[...].astype(F32)).astype(BF)
    bdt[0] = jnp.transpose(bd[...]).astype(BF)
    bdt[1] = (jnp.transpose(bd[...]) - bdt[0].astype(F32)).astype(BF)

    for t in range(3):
        lw[(1, 2, 0)[t]].wait()

    def project(src, first):
        for t in range(3):
            out = nn(xg[2 * src], w[t, pl.ds(pl.multiple_of(src * 512, 512), 256), :])
            out = out + nn(xg[2 * src + 1], w[t, pl.ds(pl.multiple_of(src * 512 + 256, 256), 256), :])
            if first:
                acc[t] = out
            else:
                acc[t] += out

    project(x, True)
    ag[0].wait_recv()
    ag[4].start()
    ag[1].wait_recv()
    ag[5].start()

    def build(i, _):
        f = lax.broadcasted_iota(jnp.int32, (SK, 1024), 1)
        fi, fj = f // SK, lax.rem(f, SK)
        a = lax.broadcasted_iota(jnp.int32, (SK, 1024), 0)
        b = lax.rem(a + i, SK)
        hit = ((fi == a) & (fj == b)) | ((fi == b) & (fj == a))
        value = jnp.where(i == 16, 0.5, 1.0)
        keep = jnp.where(i < NS, value, 0.0)
        fsel[pl.ds(pl.multiple_of(i * SK, SK), SK), :] = jnp.where(hit, keep, 0.0).astype(BF)
        return 0

    lax.fori_loop(0, NP // SK, build, 0)
    for h in range(4):
        for q in range(2):
            feat[q, h, NF:NP, :] = jnp.zeros((NP - NF, CT), BF)
    zpad[...] = jnp.zeros((128, NP), F32)
    tmp[...] = jnp.zeros((NP, 128), F32)
    dext[...] = jnp.zeros(dext.shape, BF)
    stk[...] = jnp.zeros(stk.shape, BF)
    zst[...] = jnp.zeros((SK, 128), F32)
    vtm[...] = jnp.zeros(vtm.shape, BF)
    sext[...] = jnp.zeros(sext.shape, F32)

    ag[2].wait_recv()
    project(left, False)
    ag[3].wait_recv()
    project(right, False)
    ag[4].wait_recv()
    ag[5].wait_recv()

    cqkv = {}

    def last_projection(t):
        cqkv[t] = rc(xsend.at[t], qkv.at[t, c], ex_s.at[1 + t], ex_r.at[1 + t], seq_2=oc)
        for cols, target in ((oth_cols, None), (own_cols, c)):
            out = acc[t, :, cols] + nn(
                xg[2 * far], w[t, pl.ds(pl.multiple_of(far * 512, 512), 256), cols]
            )
            out = out + nn(
                xg[2 * far + 1], w[t, pl.ds(pl.multiple_of(far * 512 + 256, 256), 256), cols]
            )
            if target is None:
                xsend[t] = out.astype(BF)
                cqkv[t].start()
            else:
                qkv[t, target] = out.astype(BF)

    last_projection(1)
    last_projection(2)

    scale = SK ** (-0.5)

    def eights(v, k):
        return v if k == 0 else jnp.concatenate([v[8 * k :], v[: 8 * k]], axis=0)

    def ones(v, k):
        return v if k == 0 else pltpu.roll(v, SK - k, 0)

    def sketch(t, k):
        part = pl.ds(pl.multiple_of(256 * k, 256), 256)
        src = qkv[t, k]
        lr = nt(bdh[...], src) + nt(bdl[...], src)
        lrt[t, :, part] = lr
        tok = nt(src, bdh[...]) + nt(src, bdl[...])
        stok[t, part, :] = (tok[:, :128] * tok[:, 128:] * scale).astype(BF)
        st = lr[:128] * lr[128:] * scale
        skt[t, :, part] = st
        skb[t, :, part] = st.astype(BF)

        def one(h, _):
            for q in range(2):
                cols = pl.ds(pl.multiple_of(256 * k + 128 * q, 128), 128)
                s = skt[t, pl.ds(pl.multiple_of(h * SK, SK), SK), cols]
                for b in range(8):
                    turned = ones(s, b)
                    for a in range(3 if b == 0 else 2):
                        i = 8 * a + b
                        feat[t, h, SK * i : SK * i + SK, cols] = (s * eights(turned, a)).astype(BF)
            return 0

        lax.fori_loop(0, 4, one, 0)

    lane256 = lax.broadcasted_iota(jnp.int32, (CT, 256), 1)

    def pack_z(n, total):
        tmp[0:NF, :] = total
        zt = jnp.transpose(tmp[...])
        for j in range(5):
            zst[4 * j : 4 * j + 4, :] = zt[0:4, 128 * j : 128 * j + 128]
        wire[n, ZROW:WIRE, :] = zst[...].astype(BF)

    def others():
        for d in FAR_FIRST:
            py, pz = lax.rem(y + d // 4, 4), lax.rem(z + d % 4, 4)
            yield py * 4 + pz, {"seq_0": py, "seq_1": pz}

    def scan_send(n, lo, hi):
        for r, where in others():

            @pl.when((r >= lo) & (r < hi))
            def _(r=r, where=where):
                rc(
                    wire.at[n, pl.ds(pl.multiple_of(r * ROWS, ROWS), ROWS)], inb.at[n, m],
                    a_s.at[n], a_r.at[n], **where,
                ).start()

        @pl.when((m >= lo) & (m < hi))
        def _():
            inb[n, m] = wire[n, pl.ds(pl.multiple_of(m * ROWS, ROWS), ROWS), :]

    def mine(ref):
        return ref.at[pl.ds(pl.multiple_of(m * ROWS, ROWS), ROWS)]

    def scan_own(n, reverse):
        @pl.when(m < OWN)
        def _():
            part = inb.at[n, 0 : CH - 1]
            rc(part, part, t_s, a_r.at[n], seq_2=oc).wait_recv()
            running = jnp.zeros((ROWS, 128), F32)
            for i in range(CH):
                r = CH - 1 - i if reverse else i
                outb[n, r] = running.astype(BF)
                running = running + inb[n, r].astype(F32)
            if reverse:
                totb[...] = running.astype(BF)
            for r, where in others():
                rc(outb.at[n, r], mine(res.at[n]), b_s.at[n], b_r.at[n], **where).start()
            res[n, pl.ds(pl.multiple_of(m * ROWS, ROWS), ROWS), :] = outb[n, m]
            if reverse:
                tot[c, pl.ds(pl.multiple_of(m * ROWS, ROWS), ROWS), :] = totb[...]
                for r, where in others():
                    rc(totb, mine(tot.at[c]), t_s, t_r, **where).start()

    def from_owners(ref, sem):
        def all_of(count):
            part = ref.at[pl.ds(0, count * ROWS)]
            rc(part, part, t_s, sem, seq_2=oc).wait_recv()

        @pl.when(m < OWN)
        def _():
            all_of(OWN - 1)

        @pl.when(m >= OWN)
        def _():
            all_of(OWN)

    def sends_done():
        for n in range(2):
            def all_of(count):
                part = wire.at[n, pl.ds(0, count * ROWS)]
                rc(part, part, a_s.at[n], t_r, seq_2=oc).wait_send()

            @pl.when(m < OWN)
            def _():
                all_of(OWN - 1)
                part = outb.at[n, 0 : CH - 1]
                rc(part, part, b_s.at[n], t_r, seq_2=oc).wait_send()

            @pl.when(m >= OWN)
            def _():
                all_of(OWN)

        @pl.when(m < OWN)
        def _():
            part = outb.at[0, 0 : CH - 1]
            rc(part, part, t_s, t_r, seq_2=oc).wait_send()

    def fold_in(state, norm):
        stk[0:256, :] = state
        pick = jnp.where(c == 0, norm[0:4, :], norm[4:8, :])
        stk[256:272, :] = jnp.concatenate([pick, jnp.zeros((12, 1024), F32)], axis=0).astype(BF)
        fold[...] = nt(fsel[...], stk[...])

    row_w = lax.broadcasted_iota(jnp.int32, (NF, 128), 0)
    weight = jnp.where((row_w < SK) | (row_w >= 16 * SK), 1.0, 2.0)

    def unpack(n):
        zst[...] = res[n, ZROW:WIRE, :].astype(F32)
        for j in range(5):
            zpad[0:4, 128 * j : 128 * j + 128] = zst[4 * j : 4 * j + 4, :]
        zc = jnp.transpose(zpad[...])[0:NF, :] * weight + fold[0:NF, 256:384]
        for p in range(2):
            part = res[n, NF * p : NF * p + NF, :].astype(F32)
            sext[p, 0:NF, 0:128] = part * weight + fold[0:NF, 128 * p : 128 * p + 128]
            sext[p, 0:NF, 128:256] = zc
            sextt[p] = jnp.transpose(sext[p])[0:144, :].astype(BF)

    sketch(1, c)
    cqkv[1].wait_recv()
    sketch(1, oc)
    cqkv[2].wait_recv()
    for p in range(2):
        for k in range(2):
            vtok[p, 256 * k : 256 * k + 256, 0:128] = qkv[2, k, :, 128 * p : 128 * p + 128]
        vtok[p, :, 128:256] = jnp.ones((CT, 128), BF)
    ztot = None
    for p in range(2):
        out = None
        for hh in range(2):
            h = 2 * p + hh
            keep = (lane256 // 64 == hh) | (lane256 == 128 + h)
            vm = jnp.where(keep, vtok[p].astype(F32), 0.0).astype(BF)
            part = nn(feat[1, h, 0:NF, :], vm)
            out = part if out is None else out + part
        wire[0, NF * p : NF * p + NF, :] = out[:, 0:128].astype(BF)
        ztot = out[:, 128:256] if ztot is None else ztot + out[:, 128:256]
        if p == 0:
            scan_send(0, 0, SPLIT)
    pack_z(0, ztot)
    scan_send(0, SPLIT, OWN)


    last_projection(0)
    lp.wait()
    ln.wait()
    fold_in(psv[...].reshape(256, 1024).astype(BF), pnv)
    sketch(0, c)
    cqkv[0].wait_recv()
    sketch(0, oc)

    scan_own(0, False)

    la.wait()
    cga.wait_recv()
    for k in range(2):
        part = slice(256 * k, 256 * k + 256)
        gtr[:, part] = jnp.transpose(ga[k].astype(F32))
        vt = jnp.transpose(qkv[2, k].astype(F32)).astype(BF)
        for h in range(4):
            vtm[h, 64 * (h % 2) : 64 * (h % 2) + 64, part] = vt[64 * h : 64 * h + 64, :]
    row16 = lax.broadcasted_iota(jnp.int32, (16, CT), 0)
    for h in range(4):
        vtm[h, 128:144, :] = jnp.where(row16 == h, 1.0, 0.0).astype(BF)

    diag = lax.broadcasted_iota(jnp.int32, (256, 256), 0) <= lax.broadcasted_iota(
        jnp.int32, (256, 256), 1
    )
    lane_k = lax.broadcasted_iota(jnp.int32, (256, 128), 1) // SK

    def scores(h, _):
        for jb in range(2):
            keys = jnp.where(lane_k == h, stok[1, 256 * jb : 256 * jb + 256, :].astype(F32), 0.0)
            keys = keys.astype(BF)
            for ib in range(jb, 2):
                d = nn(keys, skb[0, :, 256 * ib : 256 * ib + 256])
                if ib == jb:
                    d = jnp.where(diag, d, 0.0)
                at = (h, slice(256 * jb, 256 * jb + 256), slice(256 * ib, 256 * ib + 256))
                scr[at] = (d * d).astype(BF)
                dmat[at] = (d + d).astype(BF)
        yloc[h, :, 0:256] = nn(vtm[h, 0:144, 0:256], scr[h, 0:256, 0:256])
        yloc[h, :, 256:512] = nn(vtm[h, 0:144, :], scr[h, :, 256:512])
        return 0

    lax.fori_loop(0, 4, scores, 0)

    from_owners(res.at[0], b_r.at[0])
    unpack(0)
    ztot = None
    for p in range(2):
        out = None
        for hh in range(2):
            h = 2 * p + hh
            yv[h] = nn(sextt[p], feat[0, h]) + yloc[h]
            num = yv[h, 64 * hh : 64 * hh + 64, :]
            inv = 1.0 / (1.0 + yv[h, 128 + h : 129 + h, :])
            g = gtr[64 * h : 64 * h + 64, :]
            dden = -jnp.sum(g * num, axis=0, keepdims=True) * inv * inv
            dext[h, 64 * hh : 64 * hh + 64, :] = (g * inv).astype(BF)
            dext[h, 128:144, :] = jnp.where(row16 == h, dden, 0.0).astype(BF)
            part = nt(feat[0, h, 0:NF, :], dext[h])
            out = part if out is None else out + part
        wire[1, NF * p : NF * p + NF, :] = out[:, 0:128].astype(BF)
        ztot = out[:, 128:256] if ztot is None else ztot + out[:, 128:256]
        if p == 0:
            scan_send(1, 0, SPLIT)
    pack_z(1, ztot)
    scan_send(1, SPLIT, OWN)

    def lanes(ref, at, u):
        return jnp.concatenate(
            [ref[at + (slice(128 * u, 128 * u + 128),)], ref[at + (slice(256 + 128 * u, 384 + 128 * u),)]],
            axis=1,
        )

    def feature_grad(t, h, u, slot):
        rows = pl.ds(pl.multiple_of(h * SK, SK), SK)
        for q in range(2):
            cols = slice(256 * q + 128 * u, 256 * q + 128 * u + 128)
            mine_ = slice(128 * q, 128 * q + 128)
            s = skt[t, rows, cols]
            here = dst[t, rows, cols] + 2.0 * s * dfe[slot, 0:SK, mine_]
            for b in range(8):
                turned = ones(s, b)
                back = None
                for a in range(3 if b == 0 else 2):
                    i = 8 * a + b
                    if i == 0:
                        continue
                    d = dfe[slot, SK * i : SK * i + SK, mine_]
                    here = here + d * eights(turned, a)
                    term = eights(d * s, (4 - a) % 4)
                    back = term if back is None else back + term
                here = here + (back if b == 0 else pltpu.roll(back, b, 0))
            dst[t, rows, cols] = here

    def local_grads(h, _):
        p = h // 2
        for jb in range(2):
            for ib in range(jb, 2):
                at = (h, slice(256 * jb, 256 * jb + 256), slice(256 * ib, 256 * ib + 256))
                ds = nn(vtok[p, 256 * jb : 256 * jb + 256, :], dext[h, :, 256 * ib : 256 * ib + 256])
                wmat[at] = (dmat[at].astype(F32) * ds).astype(BF)
        sk_rows = pl.ds(pl.multiple_of(h * SK, SK), SK)
        d_rows = pl.ds(pl.multiple_of(64 * lax.rem(h, 2), 64), 64)
        v_rows = pl.ds(pl.multiple_of(64 * h, 64), 64)
        dst[0, sk_rows, 0:256] = nn(skb[1, sk_rows, 0:256], wmat[h, 0:256, 0:256])
        dst[0, sk_rows, 256:512] = nn(skb[1, sk_rows, :], wmat[h, :, 256:512])
        dst[1, sk_rows, 0:256] = nt(skb[0, sk_rows, :], wmat[h, 0:256, :])
        dst[1, sk_rows, 256:512] = nt(skb[0, sk_rows, 256:512], wmat[h, 256:512, 256:512])
        dvt[v_rows, 0:256] = nt(dext[h, d_rows, :], scr[h, 0:256, :])
        dvt[v_rows, 256:512] = nt(dext[h, d_rows, 256:512], scr[h, 256:512, 256:512])
        return 0

    def through_sketch(t, u):
        at = (slice(0, 128),)
        lt, rt = lanes(lrt.at[t], at, u), lanes(lrt.at[t], (slice(128, 256),), u)
        ds = lanes(dst.at[t], at, u) * scale
        dlr = jnp.concatenate([ds * rt, ds * lt], axis=0).astype(BF)
        return nn(bdt[0], dlr) + nn(bdt[1], dlr)

    def keep(t, u, grad):
        dtok[u, t] = jnp.transpose(grad).astype(BF)
        dall[t, c, 128 * u : 128 * u + 128, :] = dtok[
            u, t, pl.ds(pl.multiple_of(128 * c, 128), 128), :
        ]

    oth_half = pl.ds(pl.multiple_of(128 * oc, 128), 128)

    def hand_q(u):
        copy = rc(
            dtok.at[u, 0, oth_half], dall.at[0, c, 128 * u : 128 * u + 128],
            ex_s.at[4 + u], ex_r.at[4 + u], seq_2=oc,
        )
        copy.start()
        return copy

    def hand_kv(u):
        copy = rc(
            dtok.at[u, 1:3, oth_half], dall.at[1:3, c, 128 * u : 128 * u + 128],
            ex_s.at[6 + u], ex_r.at[6 + u], seq_2=oc,
        )
        copy.start()
        return copy

    lax.fori_loop(0, 4, local_grads, 0)

    copy_q = []
    for u in range(2):

        def grad_q(p, _, u=u):
            for hh in range(2):
                h = 2 * p + hh
                dfe[hh] = nn(sext[p, 0:NF, :].astype(BF), lanes(dext.at[h], (slice(0, 256),), u))
                feature_grad(0, h, u, hh)
            return 0

        lax.fori_loop(0, 2, grad_q, 0)
        keep(0, u, through_sketch(0, u))
        copy_q.append(hand_q(u))
    scan_own(1, True)

    le.wait()
    lm.wait()
    fold_in(dev[pl.ds(4 * c, 4)].reshape(256, 1024).astype(BF), dnv)
    for u in range(2):
        copy_q[u].wait_recv()

    def pull(t, b, rows):
        out = None
        for k in range(2):
            part = nt(
                dall[t, k, rows], w[t, pl.ds(pl.multiple_of(b * 512, 512), 512), 256 * k : 256 * k + 256]
            )
            out = part if out is None else out + part
        return out

    def pull_q(b, _):
        acc2[b] = pull(0, b, slice(0, 256))
        return 0

    lax.fori_loop(0, 4, pull_q, 0)

    from_owners(res.at[1], b_r.at[1])
    unpack(1)

    def grads(u):
        for h in range(4):
            v_rows = slice(64 * h, 64 * h + 64)
            d_rows = slice(64 * (h % 2), 64 * (h % 2) + 64)
            out = nn(sextt[h // 2, d_rows, :], lanes(feat.at[1, h], (slice(0, NP),), u))
            for q in range(2):
                cols = slice(256 * q + 128 * u, 256 * q + 128 * u + 128)
                dvt[v_rows, cols] += out[:, 128 * q : 128 * q + 128]
        keep(2, u, lanes(dvt, (slice(0, 256),), u))
        for h in range(4):
            dfe[h] = nn(sextb[h // 2], lanes(vtm.at[h], (slice(0, 256),), u))
            feature_grad(1, h, u, h)
        keep(1, u, through_sketch(1, u))
        return hand_kv(u)

    for p in range(2):
        sextb[p] = sext[p, 0:NF, :].astype(BF)
    copy_kv = [grads(0)]
    copy_kv.append(grads(1))

    rs = [
        [
            rc(
                rsend.at[u, i], rrecv.at[u, i], rs_s, rs_r.at[u, i],
                head=right if i in (0, 2, 4) else left,
            )
            for i in range(6)
        ]
        for u in range(2)
    ]

    def block(b, u):
        rows = slice(128 * u, 128 * u + 128)
        return acc2[b, rows, :] + pull(1, b, rows) + pull(2, b, rows)

    def outgoing(u):
        rows = slice(128 * u, 128 * u + 128)
        out = block(far, u)
        rsend[u, 0] = out[:, 0:256].astype(BF)
        rs[u][0].start()
        rsend[u, 1] = out[:, 256:512].astype(BF)
        rs[u][1].start()
        out = block(right, u)
        rsend[u, 2] = out[:, 256:512].astype(BF)
        rs[u][2].start()
        acc2[right, rows, 0:256] = out[:, 0:256]
        out = block(left, u)
        rsend[u, 3] = out[:, 0:256].astype(BF)
        rs[u][3].start()
        acc2[left, rows, 256:512] = out[:, 256:512]

    def merge(u):
        rows = slice(128 * u, 128 * u + 128)
        rs[u][0].wait_recv()
        rsend[u, 4] = (acc2[right, rows, 0:256] + rrecv[u, 0].astype(F32)).astype(BF)
        rs[u][4].start()
        rs[u][1].wait_recv()
        rsend[u, 5] = (acc2[left, rows, 256:512] + rrecv[u, 1].astype(F32)).astype(BF)
        rs[u][5].start()

    def arrived(u):
        rows = slice(128 * u, 128 * u + 128)
        rs[u][3].wait_recv()
        rs[u][4].wait_recv()
        oin[rows, 0:256] = (
            acc2[x, rows, 0:256] + rrecv[u, 3].astype(F32) + rrecv[u, 4].astype(F32)
        ).astype(BF)
        rs[u][2].wait_recv()
        rs[u][5].wait_recv()
        oin[rows, 256:512] = (
            acc2[x, rows, 256:512] + rrecv[u, 2].astype(F32) + rrecv[u, 5].astype(F32)
        ).astype(BF)

    copy_kv[0].wait_recv()
    outgoing(0)
    copy_kv[1].wait_recv()
    outgoing(1)
    merge(0)
    for u in range(2):
        acc2[x, 128 * u : 128 * u + 128, :] = block(x, u)
    merge(1)
    for t in range(3):
        for k in range(2):
            oqkv[t, :, 256 * k : 256 * k + 256] = dall[t, k]

    from_owners(tot.at[c], t_r)
    whole = tot.at[c]
    copy_t = rc(whole, whole, ex_s.at[8], ex_r.at[8], seq_2=oc)
    copy_t.start()

    def totals(k):
        for p in range(2):
            tmp[0:NF, :] = tot[k, NF * p : NF * p + NF, :].astype(F32)
            part = nn(jnp.transpose(tmp[...]).astype(BF), fsel[...])
            for hh in range(2):
                h = 4 * k + 2 * p + hh
                dps[h] = dev[h] + part[64 * hh : 64 * hh + 64, :]
        zst[...] = tot[k, ZROW:WIRE, :].astype(F32)
        for j in range(5):
            zpad[pl.ds(pl.multiple_of(8 * k, 8), 4), 128 * j : 128 * j + 128] = zst[4 * j : 4 * j + 4, :]

    totals(c)
    copy_t.wait_recv()
    totals(oc)
    norms = nn(zpad[0:16, :].astype(BF), fsel[...])
    dpn[0:4, :] = dnv[0:4, :] + norms[0:4, :]
    dpn[4:8, :] = dnv[4:8, :] + norms[8:12, :]

    arrived(0)
    arrived(1)

    sends = xg.at[0:6]
    rc(sends, sends, ag_s, t_r, seq_2=oc).wait_send()
    for one in list(cqkv.values()) + [cga, copy_t] + copy_q + copy_kv:
        one.wait_send()
    sends = rsend.at[:]
    rc(sends, sends, rs_s, t_r, seq_2=oc).wait_send()
    sends_done()


def put_kernel(oin, oqkv, dps, dpn, oi_hbm, oq_hbm, ok_hbm, ov_hbm, os_hbm, on_hbm, sem):
    copies = [
        pltpu.make_async_copy(dps.at[4 * k : 4 * k + 4], os_hbm.at[4 * k : 4 * k + 4], sem.at[k])
        for k in range(2)
    ]
    copies += [
        pltpu.make_async_copy(oqkv.at[t], ref, sem.at[2 + t])
        for t, ref in enumerate((oq_hbm, ok_hbm, ov_hbm))
    ]
    copies.append(pltpu.make_async_copy(oin, oi_hbm, sem.at[5]))
    copies.append(pltpu.make_async_copy(dpn, on_hbm, sem.at[6]))
    for copy in copies:
        copy.start()
    for copy in copies:
        copy.wait()


def body(x, wq, wk, wv, sketch, prefix_state, prefix_norm, d_attn, d_state, d_norm):
    any_ = pl.BlockSpec(memory_space=pl.ANY)
    v = pltpu.VMEM
    scratch = [
        v((8, TOK, 256), BF),
        v((3, 2048, 512), BF),
        v((3, TOK, 512), F32),
        v((3, 2, TOK, 256), BF),
        v((3, TOK, 256), BF),
        v((2, TOK, 256), BF),
        v((2, SK, 64), F32),
        v((4, 64, 1024), F32),
        v((8, 1024), F32),
        v((8, 64, 1024), F32),
        v((8, 1024), F32),
        v((256, 256), F32),
        v((256, 256), BF),
        v((256, 256), BF),
        v((2, 256, 256), BF),
        v((2, 256, CT), F32),
        v((2, 128, CT), F32),
        v((2, 128, CT), BF),
        v((2, CT, 128), BF),
        v((2, 4, NP, CT), BF),
        v((4, 256, CT), BF),
        v((2, CT, 256), BF),
        v((4, 256, CT), BF),
        v((NP, 384), F32),
        v((384, 1024), BF),
        v((NP, 1024), BF),
        v((4, 144, CT), F32),
        v((256, CT), F32),
        v((4, CT, CT), BF),
        v((4, CT, CT), BF),
        v((4, CT, CT), BF),
        v((4, 144, CT), F32),
        v((NP, 128), F32),
        v((SK, 128), F32),
        v((128, NP), F32),
        v((4, NF, 256), F32),
        v((2, 128, CT), F32),
        v((256, CT), F32),
        v((2, NP, 256), F32),
        v((2, 144, NP), BF),
        v((2, NF, 256), BF),
        v((2, WIRE, 128), BF),
        v((2, CH, ROWS, 128), BF),
        v((2, CH, ROWS, 128), BF),
        v((2, WIRE, 128), BF),
        v((ROWS, 128), BF),
        v((2, WIRE, 128), BF),
        v((2, 3, 256, 256), BF),
        v((3, 2, TOK, 256), BF),
        v((4, TOK, 512), F32),
        v((2, 6, 128, 256), BF),
        v((2, 6, 128, 256), BF),
    ]
    sem = pltpu.SemaphoreType.DMA
    scratch += [
        sem((11,)), sem, sem((6,)), sem((9,)), sem((9,)), sem((2,)), sem((2,)),
        sem((2,)), sem((2,)), sem, sem, sem, sem((2, 6)),
    ]
    swap = (0, 2, 1)
    made = (
        v((TOK, 512), BF),
        v((3, TOK, 512), BF),
        v((8, 64, 1024), F32),
        v((8, 1024), F32),
    )
    held = pl.BlockSpec(memory_space=pltpu.VMEM)
    outs = pl.pallas_call(
        kernel,
        out_shape=made,
        in_specs=[any_] * 10,
        out_specs=(held,) * 4,
        scratch_shapes=scratch,
        compiler_params=pltpu.CompilerParams(
            collective_id=0, has_side_effects=True, vmem_limit_bytes=60 * 1024 * 1024
        ),
        name="sketch_bwd",
    )(
        x, wq, wk, wv, jnp.transpose(sketch, swap), jnp.transpose(prefix_state, swap),
        prefix_norm, d_attn, jnp.transpose(d_state, swap), d_norm,
    )
    rows = jax.ShapeDtypeStruct((TOK, 512), BF)
    outs = pl.pallas_call(
        put_kernel,
        out_shape=(
            rows, rows, rows, rows,
            jax.ShapeDtypeStruct((8, 64, 1024), F32),
            jax.ShapeDtypeStruct((8, 1024), F32),
        ),
        in_specs=[held] * 4,
        out_specs=(any_,) * 6,
        scratch_shapes=[sem((7,))],
        compiler_params=pltpu.CompilerParams(vmem_limit_bytes=1024 * 1024),
        name="put_out",
    )(*(pltpu.with_memory_space_constraint(o, pltpu.VMEM) for o in outs))
    return outs[:4] + (jnp.transpose(outs[4], swap), outs[5])


def solution(mesh):
    finer = Mesh(
        mesh.devices.reshape(4, 4, 2, mesh.shape["head"]), ("seq_0", "seq_1", "seq_2", "head")
    )
    state, rows = P("head", None, None), P("head", None)
    tokens, weight = P(SEQ, "head"), P(None, "head")
    return jax.shard_map(
        body,
        mesh=finer,
        in_specs=(tokens, weight, weight, weight, P(), state, rows, tokens, state, rows),
        out_specs=(tokens, tokens, tokens, tokens, state, rows),
        check_vma=False,
    )
```

```python
import jax
import jax.numpy as jnp
from jax import lax
from jax.experimental import pallas as pl
from jax.experimental.pallas import tpu as pltpu
from jax.sharding import Mesh
from jax.sharding import PartitionSpec as P

SEQ = ("seq_0", "seq_1", "seq_2")
MESH = pl.DeviceIdType.MESH
F32 = jnp.float32
BF = jnp.bfloat16

SK = 32
NS = 17
NF = NS * SK
NP = 640
TOK = 256
CT = 512
CH = 16
ROWS = 80
OWN = 14
WIRE = OWN * ROWS
FAR_FIRST = (10, 9, 11, 6, 14, 2, 8, 5, 7, 13, 15, 1, 3, 4, 12)
ZROW = 2 * NF
SPLIT = NF // ROWS


def nn(a, b):
    return lax.dot_general(a, b, (((1,), (0,)), ((), ())), preferred_element_type=F32)


def nt(a, b):
    return lax.dot_general(a, b, (((1,), (1,)), ((), ())), preferred_element_type=F32)


def kernel(
    x_hbm, wq_hbm, wk_hbm, wv_hbm, g_hbm, ps_hbm, pn_hbm, da_hbm, de_hbm, dn_hbm,
    oin, oqkv, dps, dpn,
    xg, w, acc, qkv, xsend, ga, gt, psv, pnv, dev, dnv,
    bd, bdh, bdl, bdt, lrt, skt, skb, stok, st, feat, vtm, vtok, dext, fold, stk, fsel,
    yloc, gtr, scr, dmat, wmat, yv, tmp, zst, zpad, dfe, dst, dvt, sext, sextt, sextb,
    wire, inb, outb, res, totb, tot, dtok, dall, acc2, rsend, rrecv,
    loc, ag_s, ag_r, ex_s, ex_r, a_s, a_r, b_s, b_r, t_s, t_r, rs_s, rs_r,
):
    y = lax.axis_index("seq_0")
    z = lax.axis_index("seq_1")
    c = lax.axis_index("seq_2")
    x = lax.axis_index("head")
    m = y * 4 + z
    oc = 1 - c
    right, left, far = lax.rem(x + 1, 4), lax.rem(x + 3, 4), lax.rem(x + 2, 4)

    def rc(src, dst_, ss, rs, **where):
        return pltpu.make_async_remote_copy(
            src_ref=src, dst_ref=dst_, send_sem=ss, recv_sem=rs,
            device_id=where, device_id_type=MESH,
        )

    own_cols = pl.ds(pl.multiple_of(c * 256, 256), 256)
    oth_cols = pl.ds(pl.multiple_of(oc * 256, 256), 256)

    lx = [
        pltpu.make_async_copy(x_hbm.at[:, 256 * k : 256 * k + 256], xg.at[2 * x + k], loc.at[k])
        for k in range(2)
    ]
    lw = [
        pltpu.make_async_copy(src, w.at[t], loc.at[2 + t])
        for t, src in enumerate((wq_hbm, wk_hbm, wv_hbm))
    ]
    lg = pltpu.make_async_copy(g_hbm, gt, loc.at[5])
    la = pltpu.make_async_copy(da_hbm.at[:, own_cols], ga.at[c], loc.at[6])
    ln = pltpu.make_async_copy(pn_hbm, pnv, loc.at[7])
    lp = pltpu.make_async_copy(ps_hbm.at[pl.ds(4 * c, 4)], psv, loc.at[8])
    le = pltpu.make_async_copy(de_hbm, dev, loc.at[9])
    lm = pltpu.make_async_copy(dn_hbm, dnv, loc.at[10])
    for copy in (lx[0], lx[1], lw[1], lw[2], lw[0], lg, la, ln, lp, le, lm):
        copy.start()

    bar = pltpu.get_barrier_semaphore()
    for peer in (right, left):
        pl.semaphore_signal(bar, inc=1, device_id={"head": peer}, device_id_type=MESH)
    pl.semaphore_signal(bar, inc=1, device_id={"seq_2": oc}, device_id_type=MESH)

    def greet(d, _):
        r = lax.rem(m + d, CH)
        pl.semaphore_signal(
            bar, inc=1, device_id={"seq_0": r // 4, "seq_1": lax.rem(r, 4)}, device_id_type=MESH
        )
        return 0

    lax.fori_loop(1, CH, greet, 0)
    pl.semaphore_wait(bar, 18)

    def slab(src, k, peer, i):
        ref = xg.at[2 * src + k]
        return rc(ref, ref, ag_s.at[min(i, 2)], ag_r.at[i], head=peer)

    ag = [
        slab(x, 0, right, 0), slab(x, 1, left, 1), slab(x, 1, right, 2), slab(x, 0, left, 3),
        slab(left, 0, right, 4), slab(right, 1, left, 5),
    ]
    lx[0].wait()
    lx[1].wait()
    for i in range(2):
        ag[i].start()
    cga = rc(da_hbm.at[:, oth_cols], ga.at[c], ex_s.at[0], ex_r.at[0], seq_2=oc)
    cga.start()

    lg.wait()
    bd[...] = jnp.zeros((256, 256), F32)
    lane128 = lax.broadcasted_iota(jnp.int32, (SK, 128), 1) // 64
    for lr in range(2):
        wide = jnp.concatenate([gt[lr], gt[lr]], axis=1)
        for h in range(4):
            row = lr * 128 + h * SK
            col = 128 * (h // 2)
            bd[row : row + SK, col : col + 128] = jnp.where(lane128 == h % 2, wide, 0.0)
    bdh[...] = bd[...].astype(BF)
    bdl[...] = (bd[...] - bdh[...].astype(F32)).astype(BF)
    bdt[0] = jnp.transpose(bd[...]).astype(BF)
    bdt[1] = (jnp.transpose(bd[...]) - bdt[0].astype(F32)).astype(BF)

    for t in range(3):
        lw[(1, 2, 0)[t]].wait()

    def project(src, first):
        for t in range(3):
            out = nn(xg[2 * src], w[t, pl.ds(pl.multiple_of(src * 512, 512), 256), :])
            out = out + nn(xg[2 * src + 1], w[t, pl.ds(pl.multiple_of(src * 512 + 256, 256), 256), :])
            if first:
                acc[t] = out
            else:
                acc[t] += out

    project(x, True)
    def build(i, _):
        f = lax.broadcasted_iota(jnp.int32, (SK, 1024), 1)
        fi, fj = f // SK, lax.rem(f, SK)
        a = lax.broadcasted_iota(jnp.int32, (SK, 1024), 0)
        b = lax.rem(a + i, SK)
        hit = ((fi == a) & (fj == b)) | ((fi == b) & (fj == a))
        value = jnp.where(i == 16, 0.5, 1.0)
        keep = jnp.where(i < NS, value, 0.0)
        fsel[pl.ds(pl.multiple_of(i * SK, SK), SK), :] = jnp.where(hit, keep, 0.0).astype(BF)
        return 0

    lax.fori_loop(0, NP // SK, build, 0)
    for h in range(4):
        for q in range(2):
            feat[q, h, NF:NP, :] = jnp.zeros((NP - NF, CT), BF)
    zpad[...] = jnp.zeros((128, NP), F32)
    tmp[...] = jnp.zeros((NP, 128), F32)
    dext[...] = jnp.zeros(dext.shape, BF)
    stk[...] = jnp.zeros(stk.shape, BF)
    zst[...] = jnp.zeros((SK, 128), F32)
    vtm[...] = jnp.zeros(vtm.shape, BF)
    sext[...] = jnp.zeros(sext.shape, F32)

    for i in range(2):
        ag[i].wait_send()
        ag[2 + i].start()
    ag[0].wait_recv()
    ag[4].start()
    ag[1].wait_recv()
    ag[5].start()
    ag[2].wait_recv()
    project(left, False)
    ag[3].wait_recv()
    project(right, False)
    ag[4].wait_recv()
    ag[5].wait_recv()

    cqkv = {}

    def last_projection(t):
        cqkv[t] = rc(xsend.at[t], qkv.at[t, c], ex_s.at[1 + t], ex_r.at[1 + t], seq_2=oc)
        for cols, target in ((oth_cols, None), (own_cols, c)):
            out = acc[t, :, cols] + nn(
                xg[2 * far], w[t, pl.ds(pl.multiple_of(far * 512, 512), 256), cols]
            )
            out = out + nn(
                xg[2 * far + 1], w[t, pl.ds(pl.multiple_of(far * 512 + 256, 256), 256), cols]
            )
            if target is None:
                xsend[t] = out.astype(BF)
                cqkv[t].start()
            else:
                qkv[t, target] = out.astype(BF)

    last_projection(1)
    last_projection(2)

    scale = SK ** (-0.5)

    def eights(v, k):
        return v if k == 0 else jnp.concatenate([v[8 * k :], v[: 8 * k]], axis=0)

    def ones(v, k):
        return v if k == 0 else pltpu.roll(v, SK - k, 0)

    def sketch(t, k):
        part = pl.ds(pl.multiple_of(256 * k, 256), 256)
        src = qkv[t, k]
        lr = nt(bdh[...], src) + nt(bdl[...], src)
        lrt[t, :, part] = lr
        st = lr[:128] * lr[128:] * scale
        skt[t, :, part] = st
        skb[t, :, part] = st.astype(BF)

        def one(h, _):
            for q in range(2):
                cols = pl.ds(pl.multiple_of(256 * k + 128 * q, 128), 128)
                s = skt[t, pl.ds(pl.multiple_of(h * SK, SK), SK), cols]
                for b in range(8):
                    turned = ones(s, b)
                    for a in range(3 if b == 0 else 2):
                        i = 8 * a + b
                        feat[t, h, SK * i : SK * i + SK, cols] = (s * eights(turned, a)).astype(BF)
            return 0

        lax.fori_loop(0, 4, one, 0)

    def sketch_tokens(t):
        for k in range(2):
            tok = nt(qkv[t, k], bdh[...]) + nt(qkv[t, k], bdl[...])
            stok[256 * k : 256 * k + 256, :] = (tok[:, :128] * tok[:, 128:] * scale).astype(BF)

    lane256 = lax.broadcasted_iota(jnp.int32, (256, 256), 1)

    def pack_z(n, total):
        tmp[0:NF, :] = total
        zt = jnp.transpose(tmp[...])
        for j in range(5):
            zst[4 * j : 4 * j + 4, :] = zt[0:4, 128 * j : 128 * j + 128]
        wire[n, ZROW:WIRE, :] = zst[...].astype(BF)

    def others():
        for d in FAR_FIRST:
            py, pz = lax.rem(y + d // 4, 4), lax.rem(z + d % 4, 4)
            yield py * 4 + pz, {"seq_0": py, "seq_1": pz}

    def rows_of(r):
        return pl.ds(pl.multiple_of(r * ROWS, ROWS), ROWS)

    def scan_send(n, lo, hi):
        for r, where in others():

            @pl.when((r >= lo) & (r < hi))
            def _(r=r, where=where):
                rc(wire.at[n, rows_of(r)], inb.at[n, m], a_s.at[n], a_r.at[n], **where).start()

        @pl.when((m >= lo) & (m < hi))
        def _():
            inb[n, m] = wire[n, rows_of(m), :]

    def scan_own(n, reverse):
        @pl.when(m < OWN)
        def _():
            part = inb.at[n, 0 : CH - 1]
            rc(part, part, t_s, a_r.at[n], seq_2=oc).wait_recv()
            running = jnp.zeros((ROWS, 128), F32)
            for i in range(CH):
                r = CH - 1 - i if reverse else i
                outb[n, r] = running.astype(BF)
                running = running + inb[n, r].astype(F32)
            if reverse:
                totb[...] = running.astype(BF)
            for r, where in others():
                rc(outb.at[n, r], res.at[n, rows_of(m)], b_s.at[n], b_r.at[n], **where).start()
            res[n, rows_of(m), :] = outb[n, m]

    def share_totals():
        @pl.when(m < OWN)
        def _():
            for r, where in others():
                rc(totb, tot.at[c, rows_of(m)], t_s, t_r, **where).start()
            tot[c, rows_of(m), :] = totb[...]

    def from_owners(ref, sem):
        def all_of(count):
            part = ref.at[pl.ds(0, count * ROWS)]
            rc(part, part, t_s, sem, seq_2=oc).wait_recv()

        @pl.when(m < OWN)
        def _():
            all_of(OWN - 1)

        @pl.when(m >= OWN)
        def _():
            all_of(OWN)

    def sends_done():
        def all_of(part, sem):
            rc(part, part, sem, t_r, seq_2=oc).wait_send()

        @pl.when(m < OWN)
        def _():
            for n in range(2):
                all_of(wire.at[n, pl.ds(0, (OWN - 1) * ROWS)], a_s.at[n])
                all_of(outb.at[n, 0 : CH - 1], b_s.at[n])
            all_of(outb.at[0, 0 : CH - 1], t_s)

        @pl.when(m >= OWN)
        def _():
            for n in range(2):
                all_of(wire.at[n, pl.ds(0, OWN * ROWS)], a_s.at[n])

    def fold_in(state, norm):
        stk[0:256, :] = state
        pick = jnp.where(c == 0, norm[0:4, :], norm[4:8, :])
        stk[256:272, :] = jnp.concatenate([pick, jnp.zeros((12, 1024), F32)], axis=0).astype(BF)
        fold[...] = nt(fsel[...], stk[...])

    row_w = lax.broadcasted_iota(jnp.int32, (NF, 128), 0)
    weight = jnp.where((row_w < SK) | (row_w >= 16 * SK), 1.0, 2.0)

    def unpack(n):
        zst[...] = res[n, ZROW:WIRE, :].astype(F32)
        for j in range(5):
            zpad[0:4, 128 * j : 128 * j + 128] = zst[4 * j : 4 * j + 4, :]
        zc = jnp.transpose(zpad[...])[0:NF, :] * weight + fold[0:NF, 256:384]
        for p in range(2):
            part = res[n, NF * p : NF * p + NF, :].astype(F32)
            sext[p, 0:NF, 0:128] = part * weight + fold[0:NF, 128 * p : 128 * p + 128]
            sext[p, 0:NF, 128:256] = zc
            sextt[p] = jnp.transpose(sext[p])[0:144, :].astype(BF)

    def state_half(k, last):
        part = pl.ds(pl.multiple_of(256 * k, 256), 256)
        for p in range(2):
            vtok[p, part, 0:128] = qkv[2, k, :, 128 * p : 128 * p + 128]
            vtok[p, part, 128:256] = jnp.ones((256, 128), BF)
        ztot = None
        for p in range(2):
            out = st[p] if last else None
            for hh in range(2):
                h = 2 * p + hh
                keep = (lane256 // 64 == hh) | (lane256 == 128 + h)
                vm = jnp.where(keep, vtok[p, part, :].astype(F32), 0.0).astype(BF)
                term = nn(feat[1, h, 0:NF, part], vm)
                out = term if out is None else out + term
            if not last:
                st[p] = out
                continue
            wire[0, NF * p : NF * p + NF, :] = out[:, 0:128].astype(BF)
            ztot = out[:, 128:256] if ztot is None else ztot + out[:, 128:256]
            if p == 0:
                scan_send(0, 0, SPLIT)
        if last:
            pack_z(0, ztot)
            scan_send(0, SPLIT, OWN)

    sketch(1, c)
    state_half(c, False)
    cqkv[1].wait_recv()
    sketch(1, oc)
    cqkv[2].wait_recv()
    state_half(oc, True)

    last_projection(0)
    sketch_tokens(1)
    lp.wait()
    ln.wait()
    fold_in(psv[...].reshape(256, 1024).astype(BF), pnv)
    sketch(0, c)
    cqkv[0].wait_recv()
    sketch(0, oc)

    scan_own(0, False)

    la.wait()
    cga.wait_recv()
    for k in range(2):
        part = slice(256 * k, 256 * k + 256)
        gtr[:, part] = jnp.transpose(ga[k].astype(F32))
        vt = jnp.transpose(qkv[2, k].astype(F32)).astype(BF)
        for h in range(4):
            vtm[h, 64 * (h % 2) : 64 * (h % 2) + 64, part] = vt[64 * h : 64 * h + 64, :]
    row16 = lax.broadcasted_iota(jnp.int32, (16, CT), 0)
    for h in range(4):
        vtm[h, 128:144, :] = jnp.where(row16 == h, 1.0, 0.0).astype(BF)

    diag = lax.broadcasted_iota(jnp.int32, (256, 256), 0) <= lax.broadcasted_iota(
        jnp.int32, (256, 256), 1
    )
    lane_k = lax.broadcasted_iota(jnp.int32, (256, 128), 1) // SK

    def scores(h, _):
        for jb in range(2):
            keys = jnp.where(lane_k == h, stok[256 * jb : 256 * jb + 256, :].astype(F32), 0.0)
            keys = keys.astype(BF)
            for ib in range(jb, 2):
                d = nn(keys, skb[0, :, 256 * ib : 256 * ib + 256])
                if ib == jb:
                    d = jnp.where(diag, d, 0.0)
                at = (h, slice(256 * jb, 256 * jb + 256), slice(256 * ib, 256 * ib + 256))
                scr[at] = (d * d).astype(BF)
                dmat[at] = (d + d).astype(BF)
        yloc[h, :, 0:256] = nn(vtm[h, 0:144, 0:256], scr[h, 0:256, 0:256])
        yloc[h, :, 256:512] = nn(vtm[h, 0:144, :], scr[h, :, 256:512])
        return 0

    lax.fori_loop(0, 4, scores, 0)

    from_owners(res.at[0], b_r.at[0])
    unpack(0)
    ztot = None
    for p in range(2):
        out = None
        for hh in range(2):
            h = 2 * p + hh
            yv[h] = nn(sextt[p], feat[0, h]) + yloc[h]
            num = yv[h, 64 * hh : 64 * hh + 64, :]
            inv = 1.0 / (1.0 + yv[h, 128 + h : 129 + h, :])
            g = gtr[64 * h : 64 * h + 64, :]
            dden = -jnp.sum(g * num, axis=0, keepdims=True) * inv * inv
            dext[h, 64 * hh : 64 * hh + 64, :] = (g * inv).astype(BF)
            dext[h, 128:144, :] = jnp.where(row16 == h, dden, 0.0).astype(BF)
            part = nt(feat[0, h, 0:NF, :], dext[h])
            out = part if out is None else out + part
        wire[1, NF * p : NF * p + NF, :] = out[:, 0:128].astype(BF)
        ztot = out[:, 128:256] if ztot is None else ztot + out[:, 128:256]
        if p == 0:
            scan_send(1, 0, SPLIT)
    pack_z(1, ztot)
    scan_send(1, SPLIT, OWN)

    def lanes(ref, at, u):
        return jnp.concatenate(
            [ref[at + (slice(128 * u, 128 * u + 128),)], ref[at + (slice(256 + 128 * u, 384 + 128 * u),)]],
            axis=1,
        )

    def feature_grad(t, h, u, slot):
        rows = pl.ds(pl.multiple_of(h * SK, SK), SK)
        for q in range(2):
            cols = slice(256 * q + 128 * u, 256 * q + 128 * u + 128)
            mine_ = slice(128 * q, 128 * q + 128)
            s = skt[t, rows, cols]
            here = dst[t, rows, cols] + 2.0 * s * dfe[slot, 0:SK, mine_]
            for b in range(8):
                turned = ones(s, b)
                back = None
                for a in range(3 if b == 0 else 2):
                    i = 8 * a + b
                    if i == 0:
                        continue
                    d = dfe[slot, SK * i : SK * i + SK, mine_]
                    here = here + d * eights(turned, a)
                    term = eights(d * s, (4 - a) % 4)
                    back = term if back is None else back + term
                here = here + (back if b == 0 else pltpu.roll(back, b, 0))
            dst[t, rows, cols] = here

    def local_grads(h, _):
        p = h // 2
        for jb in range(2):
            for ib in range(jb, 2):
                at = (h, slice(256 * jb, 256 * jb + 256), slice(256 * ib, 256 * ib + 256))
                ds = nn(vtok[p, 256 * jb : 256 * jb + 256, :], dext[h, :, 256 * ib : 256 * ib + 256])
                wmat[at] = (dmat[at].astype(F32) * ds).astype(BF)
        sk_rows = pl.ds(pl.multiple_of(h * SK, SK), SK)
        d_rows = pl.ds(pl.multiple_of(64 * lax.rem(h, 2), 64), 64)
        v_rows = pl.ds(pl.multiple_of(64 * h, 64), 64)
        dst[0, sk_rows, 0:256] = nn(skb[1, sk_rows, 0:256], wmat[h, 0:256, 0:256])
        dst[0, sk_rows, 256:512] = nn(skb[1, sk_rows, :], wmat[h, :, 256:512])
        dst[1, sk_rows, 0:256] = nt(skb[0, sk_rows, :], wmat[h, 0:256, :])
        dst[1, sk_rows, 256:512] = nt(skb[0, sk_rows, 256:512], wmat[h, 256:512, 256:512])
        dvt[v_rows, 0:256] = nt(dext[h, d_rows, :], scr[h, 0:256, :])
        dvt[v_rows, 256:512] = nt(dext[h, d_rows, 256:512], scr[h, 256:512, 256:512])
        return 0

    def through_sketch(t, u):
        at = (slice(0, 128),)
        lt, rt = lanes(lrt.at[t], at, u), lanes(lrt.at[t], (slice(128, 256),), u)
        ds = lanes(dst.at[t], at, u) * scale
        dlr = jnp.concatenate([ds * rt, ds * lt], axis=0).astype(BF)
        return nn(bdt[0], dlr) + nn(bdt[1], dlr)

    def keep(t, u, grad):
        dtok[u, t] = jnp.transpose(grad).astype(BF)
        dall[t, c, 128 * u : 128 * u + 128, :] = dtok[
            u, t, pl.ds(pl.multiple_of(128 * c, 128), 128), :
        ]

    oth_half = pl.ds(pl.multiple_of(128 * oc, 128), 128)

    def hand_q(u):
        copy = rc(
            dtok.at[u, 0, oth_half], dall.at[0, c, 128 * u : 128 * u + 128],
            ex_s.at[4 + u], ex_r.at[4 + u], seq_2=oc,
        )
        copy.start()
        return copy

    def hand_kv(u):
        copy = rc(
            dtok.at[u, 1:3, oth_half], dall.at[1:3, c, 128 * u : 128 * u + 128],
            ex_s.at[6 + u], ex_r.at[6 + u], seq_2=oc,
        )
        copy.start()
        return copy

    lax.fori_loop(0, 4, local_grads, 0)

    copy_q = []

    def queries_half(u):
        def grad_q(p, _):
            for hh in range(2):
                h = 2 * p + hh
                dfe[hh] = nn(sext[p, 0:NF, :].astype(BF), lanes(dext.at[h], (slice(0, 256),), u))
                feature_grad(0, h, u, hh)
            return 0

        lax.fori_loop(0, 2, grad_q, 0)
        keep(0, u, through_sketch(0, u))
        copy_q.append(hand_q(u))

    queries_half(0)
    scan_own(1, True)
    queries_half(1)

    le.wait()
    lm.wait()
    fold_in(dev[pl.ds(4 * c, 4)].reshape(256, 1024).astype(BF), dnv)
    for u in range(2):
        copy_q[u].wait_recv()

    def pull(t, b, rows, k):
        cols = pl.ds(pl.multiple_of(256 * k, 256), 256)
        return nt(dall[t, k, rows], w[t, pl.ds(pl.multiple_of(b * 512, 512), 512), cols])

    def pull_q(b, _):
        acc2[b] = pull(0, b, slice(0, 256), 0) + pull(0, b, slice(0, 256), 1)
        return 0

    lax.fori_loop(0, 4, pull_q, 0)

    from_owners(res.at[1], b_r.at[1])
    share_totals()
    unpack(1)

    def grads(u):
        for h in range(4):
            v_rows = slice(64 * h, 64 * h + 64)
            d_rows = slice(64 * (h % 2), 64 * (h % 2) + 64)
            out = nn(sextt[h // 2, d_rows, :], lanes(feat.at[1, h], (slice(0, NP),), u))
            for q in range(2):
                cols = slice(256 * q + 128 * u, 256 * q + 128 * u + 128)
                dvt[v_rows, cols] += out[:, 128 * q : 128 * q + 128]
        keep(2, u, lanes(dvt, (slice(0, 256),), u))
        for h in range(4):
            dfe[h] = nn(sextb[h // 2], lanes(vtm.at[h], (slice(0, 256),), u))
            feature_grad(1, h, u, h)
        keep(1, u, through_sketch(1, u))
        return hand_kv(u)

    for p in range(2):
        sextb[p] = sext[p, 0:NF, :].astype(BF)
    copy_kv = [grads(0)]
    copy_kv.append(grads(1))

    rs = [
        [
            rc(
                rsend.at[u, i], rrecv.at[u, i], rs_s, rs_r.at[u, i],
                head=right if i in (0, 2, 4) else left,
            )
            for i in range(6)
        ]
        for u in range(2)
    ]

    def block(b, u, ahead=False):
        rows = slice(128 * u, 128 * u + 128)
        out = acc2[b, rows, :] + pull(1, b, rows, oc) + pull(2, b, rows, oc)
        return out if ahead else out + pull(1, b, rows, c) + pull(2, b, rows, c)

    def own_part(b, u):
        rows = slice(128 * u, 128 * u + 128)
        acc2[b, rows, :] += pull(1, b, rows, c) + pull(2, b, rows, c)

    def outgoing(u):
        rows = slice(128 * u, 128 * u + 128)
        out = block(far, u, u == 0)
        rsend[u, 0] = out[:, 0:256].astype(BF)
        rs[u][0].start()
        rsend[u, 1] = out[:, 256:512].astype(BF)
        rs[u][1].start()
        out = block(right, u)
        rsend[u, 2] = out[:, 256:512].astype(BF)
        rs[u][2].start()
        acc2[right, rows, 0:256] = out[:, 0:256]
        out = block(left, u)
        rsend[u, 3] = out[:, 0:256].astype(BF)
        rs[u][3].start()
        acc2[left, rows, 256:512] = out[:, 256:512]

    def merge(u):
        rows = slice(128 * u, 128 * u + 128)
        rs[u][0].wait_recv()
        rsend[u, 4] = (acc2[right, rows, 0:256] + rrecv[u, 0].astype(F32)).astype(BF)
        rs[u][4].start()
        rs[u][1].wait_recv()
        rsend[u, 5] = (acc2[left, rows, 256:512] + rrecv[u, 1].astype(F32)).astype(BF)
        rs[u][5].start()

    def arrived(u):
        rows = slice(128 * u, 128 * u + 128)
        rs[u][3].wait_recv()
        rs[u][4].wait_recv()
        oin[rows, 0:256] = (
            acc2[x, rows, 0:256] + rrecv[u, 3].astype(F32) + rrecv[u, 4].astype(F32)
        ).astype(BF)
        rs[u][2].wait_recv()
        rs[u][5].wait_recv()
        oin[rows, 256:512] = (
            acc2[x, rows, 256:512] + rrecv[u, 2].astype(F32) + rrecv[u, 5].astype(F32)
        ).astype(BF)

    own_part(far, 0)
    copy_kv[0].wait_recv()
    outgoing(0)
    copy_kv[1].wait_recv()
    outgoing(1)
    merge(0)
    for u in range(2):
        acc2[x, 128 * u : 128 * u + 128, :] = block(x, u)
    merge(1)
    for t in range(3):
        for k in range(2):
            oqkv[t, :, 256 * k : 256 * k + 256] = dall[t, k]

    from_owners(tot.at[c], t_r)
    whole = tot.at[c]
    copy_t = rc(whole, whole, ex_s.at[8], ex_r.at[8], seq_2=oc)
    copy_t.start()

    def totals(k):
        for p in range(2):
            tmp[0:NF, :] = tot[k, NF * p : NF * p + NF, :].astype(F32)
            part = nn(jnp.transpose(tmp[...]).astype(BF), fsel[...])
            for hh in range(2):
                h = 4 * k + 2 * p + hh
                dps[h] = dev[h] + part[64 * hh : 64 * hh + 64, :]
        zst[...] = tot[k, ZROW:WIRE, :].astype(F32)
        for j in range(5):
            zpad[pl.ds(pl.multiple_of(8 * k, 8), 4), 128 * j : 128 * j + 128] = zst[4 * j : 4 * j + 4, :]

    totals(c)
    copy_t.wait_recv()
    totals(oc)
    norms = nn(zpad[0:16, :].astype(BF), fsel[...])
    dpn[0:4, :] = dnv[0:4, :] + norms[0:4, :]
    dpn[4:8, :] = dnv[4:8, :] + norms[8:12, :]

    arrived(0)
    arrived(1)

    sends = xg.at[0:4]
    rc(sends, sends, ag_s.at[2], t_r, seq_2=oc).wait_send()
    for one in list(cqkv.values()) + [cga, copy_t] + copy_q + copy_kv:
        one.wait_send()
    sends = rsend.at[:]
    rc(sends, sends, rs_s, t_r, seq_2=oc).wait_send()
    sends_done()


def put_kernel(oin, oqkv, dps, dpn, oi_hbm, oq_hbm, ok_hbm, ov_hbm, os_hbm, on_hbm, sem):
    copies = [
        pltpu.make_async_copy(dps.at[4 * k : 4 * k + 4], os_hbm.at[4 * k : 4 * k + 4], sem.at[k])
        for k in range(2)
    ]
    copies += [
        pltpu.make_async_copy(oqkv.at[t], ref, sem.at[2 + t])
        for t, ref in enumerate((oq_hbm, ok_hbm, ov_hbm))
    ]
    copies.append(pltpu.make_async_copy(oin, oi_hbm, sem.at[5]))
    copies.append(pltpu.make_async_copy(dpn, on_hbm, sem.at[6]))
    for copy in copies:
        copy.start()
    for copy in copies:
        copy.wait()


def body(x, wq, wk, wv, sketch, prefix_state, prefix_norm, d_attn, d_state, d_norm):
    any_ = pl.BlockSpec(memory_space=pl.ANY)
    v = pltpu.VMEM
    scratch = [
        v((8, TOK, 256), BF),
        v((3, 2048, 512), BF),
        v((3, TOK, 512), F32),
        v((3, 2, TOK, 256), BF),
        v((3, TOK, 256), BF),
        v((2, TOK, 256), BF),
        v((2, SK, 64), F32),
        v((4, 64, 1024), F32),
        v((8, 1024), F32),
        v((8, 64, 1024), F32),
        v((8, 1024), F32),
        v((256, 256), F32),
        v((256, 256), BF),
        v((256, 256), BF),
        v((2, 256, 256), BF),
        v((2, 256, CT), F32),
        v((2, 128, CT), F32),
        v((2, 128, CT), BF),
        v((CT, 128), BF),
        v((2, NF, 256), F32),
        v((2, 4, NP, CT), BF),
        v((4, 256, CT), BF),
        v((2, CT, 256), BF),
        v((4, 256, CT), BF),
        v((NP, 384), F32),
        v((384, 1024), BF),
        v((NP, 1024), BF),
        v((4, 144, CT), F32),
        v((256, CT), F32),
        v((4, CT, CT), BF),
        v((4, CT, CT), BF),
        v((4, CT, CT), BF),
        v((4, 144, CT), F32),
        v((NP, 128), F32),
        v((SK, 128), F32),
        v((128, NP), F32),
        v((4, NF, 256), F32),
        v((2, 128, CT), F32),
        v((256, CT), F32),
        v((2, NP, 256), F32),
        v((2, 144, NP), BF),
        v((2, NF, 256), BF),
        v((2, WIRE, 128), BF),
        v((2, CH, ROWS, 128), BF),
        v((2, CH, ROWS, 128), BF),
        v((2, WIRE, 128), BF),
        v((ROWS, 128), BF),
        v((2, WIRE, 128), BF),
        v((2, 3, 256, 256), BF),
        v((3, 2, TOK, 256), BF),
        v((4, TOK, 512), F32),
        v((2, 6, 128, 256), BF),
        v((2, 6, 128, 256), BF),
    ]
    sem = pltpu.SemaphoreType.DMA
    scratch += [
        sem((11,)), sem((3,)), sem((6,)), sem((9,)), sem((9,)), sem((2,)), sem((2,)),
        sem((2,)), sem((2,)), sem, sem, sem, sem((2, 6)),
    ]
    swap = (0, 2, 1)
    made = (
        v((TOK, 512), BF),
        v((3, TOK, 512), BF),
        v((8, 64, 1024), F32),
        v((8, 1024), F32),
    )
    held = pl.BlockSpec(memory_space=pltpu.VMEM)
    outs = pl.pallas_call(
        kernel,
        out_shape=made,
        in_specs=[any_] * 10,
        out_specs=(held,) * 4,
        scratch_shapes=scratch,
        compiler_params=pltpu.CompilerParams(
            collective_id=0, has_side_effects=True, vmem_limit_bytes=60 * 1024 * 1024
        ),
        name="sketch_bwd",
    )(
        x, wq, wk, wv, jnp.transpose(sketch, swap), jnp.transpose(prefix_state, swap),
        prefix_norm, d_attn, jnp.transpose(d_state, swap), d_norm,
    )
    rows = jax.ShapeDtypeStruct((TOK, 512), BF)
    outs = pl.pallas_call(
        put_kernel,
        out_shape=(
            rows, rows, rows, rows,
            jax.ShapeDtypeStruct((8, 64, 1024), F32),
            jax.ShapeDtypeStruct((8, 1024), F32),
        ),
        in_specs=[held] * 4,
        out_specs=(any_,) * 6,
        scratch_shapes=[sem((7,))],
        compiler_params=pltpu.CompilerParams(vmem_limit_bytes=1024 * 1024),
        name="put_out",
    )(*(pltpu.with_memory_space_constraint(o, pltpu.VMEM) for o in outs))
    return outs[:4] + (jnp.transpose(outs[4], swap), outs[5])


def solution(mesh):
    finer = Mesh(
        mesh.devices.reshape(4, 4, 2, mesh.shape["head"]), ("seq_0", "seq_1", "seq_2", "head")
    )
    state, rows = P("head", None, None), P("head", None)
    tokens, weight = P(SEQ, "head"), P(None, "head")
    return jax.shard_map(
        body,
        mesh=finer,
        in_specs=(tokens, weight, weight, weight, P(), state, rows, tokens, state, rows),
        out_specs=(tokens, tokens, tokens, tokens, state, rows),
        check_vma=False,
    )
```

```python
import jax
import jax.numpy as jnp
from jax import lax
from jax.experimental import pallas as pl
from jax.experimental.pallas import tpu as pltpu
from jax.sharding import Mesh
from jax.sharding import PartitionSpec as P

SEQ = ("seq_0", "seq_1", "seq_2")
MESH = pl.DeviceIdType.MESH
F32 = jnp.float32
BF = jnp.bfloat16

SK = 32
NS = 17
NF = NS * SK
NP = 640
TOK = 256
CT = 512
CH = 16
ROWS = 80
OWN = 14
WIRE = OWN * ROWS
FAR_FIRST = (10, 9, 11, 6, 14, 2, 8, 5, 7, 13, 15, 1, 3, 4, 12)
ZROW = 2 * NF
SPLIT = NF // ROWS


def nn(a, b):
    return lax.dot_general(a, b, (((1,), (0,)), ((), ())), preferred_element_type=F32)


def nt(a, b):
    return lax.dot_general(a, b, (((1,), (1,)), ((), ())), preferred_element_type=F32)


def kernel(
    x_hbm, wq_hbm, wk_hbm, wv_hbm, g_hbm, ps_hbm, pn_hbm, da_hbm, de_hbm, dn_hbm,
    oin, oqkv, dps, dpn,
    xg, w, acc, qkv, xsend, ga, gt, psv, pnv, dev, dnv,
    bd, bdh, bdl, bdt, lrt, skt, skb, stok, st, feat, vtm, vtok, dext, fold, stk, fsel,
    yloc, gtr, scr, dmat, wmat, yv, tmp, zst, zpad, dfe, dst, dvt, sext, sextt, sextb,
    wire, inb, outb, res, totb, tot, dtok, dall, acc2, rsend, rrecv,
    loc, ag_s, ag_r, ex_s, ex_r, a_s, a_r, b_s, b_r, t_s, t_r, rs_s, rs_r,
):
    y = lax.axis_index("seq_0")
    z = lax.axis_index("seq_1")
    c = lax.axis_index("seq_2")
    x = lax.axis_index("head")
    m = y * 4 + z
    oc = 1 - c
    right, left, far = lax.rem(x + 1, 4), lax.rem(x + 3, 4), lax.rem(x + 2, 4)

    def rc(src, dst_, ss, rs, **where):
        return pltpu.make_async_remote_copy(
            src_ref=src, dst_ref=dst_, send_sem=ss, recv_sem=rs,
            device_id=where, device_id_type=MESH,
        )

    own_cols = pl.ds(pl.multiple_of(c * 256, 256), 256)
    oth_cols = pl.ds(pl.multiple_of(oc * 256, 256), 256)

    lx = [
        pltpu.make_async_copy(x_hbm.at[:, 256 * k : 256 * k + 256], xg.at[2 * x + k], loc.at[k])
        for k in range(2)
    ]
    lw = [
        pltpu.make_async_copy(src, w.at[t], loc.at[2 + t])
        for t, src in enumerate((wq_hbm, wk_hbm, wv_hbm))
    ]
    lg = pltpu.make_async_copy(g_hbm, gt, loc.at[5])
    la = pltpu.make_async_copy(da_hbm.at[:, own_cols], ga.at[c], loc.at[6])
    ln = pltpu.make_async_copy(pn_hbm, pnv, loc.at[7])
    lp = pltpu.make_async_copy(ps_hbm.at[pl.ds(4 * c, 4)], psv, loc.at[8])
    le = pltpu.make_async_copy(de_hbm, dev, loc.at[9])
    lm = pltpu.make_async_copy(dn_hbm, dnv, loc.at[10])
    for copy in (lx[0], lx[1], lw[1], lw[2], lw[0], lg, la, ln, lp, le, lm):
        copy.start()

    bar = pltpu.get_barrier_semaphore()
    for peer in (right, left):
        pl.semaphore_signal(bar, inc=1, device_id={"head": peer}, device_id_type=MESH)
    pl.semaphore_signal(bar, inc=1, device_id={"seq_2": oc}, device_id_type=MESH)

    def greet(d, _):
        r = lax.rem(m + d, CH)
        pl.semaphore_signal(
            bar, inc=1, device_id={"seq_0": r // 4, "seq_1": lax.rem(r, 4)}, device_id_type=MESH
        )
        return 0

    lax.fori_loop(1, CH, greet, 0)
    pl.semaphore_wait(bar, 18)

    def slab(src, k, peer, i):
        ref = xg.at[2 * src + k]
        return rc(ref, ref, ag_s.at[min(i, 2)], ag_r.at[i], head=peer)

    ag = [
        slab(x, 0, right, 0), slab(x, 1, left, 1), slab(x, 1, right, 2), slab(x, 0, left, 3),
        slab(left, 0, right, 4), slab(right, 1, left, 5),
    ]
    lx[0].wait()
    lx[1].wait()
    for i in range(2):
        ag[i].start()
    cga = rc(da_hbm.at[:, oth_cols], ga.at[c], ex_s.at[0], ex_r.at[0], seq_2=oc)
    cga.start()

    lg.wait()
    bd[...] = jnp.zeros((256, 256), F32)
    lane128 = lax.broadcasted_iota(jnp.int32, (SK, 128), 1) // 64
    for lr in range(2):
        wide = jnp.concatenate([gt[lr], gt[lr]], axis=1)
        for h in range(4):
            row = lr * 128 + h * SK
            col = 128 * (h // 2)
            bd[row : row + SK, col : col + 128] = jnp.where(lane128 == h % 2, wide, 0.0)
    bdh[...] = bd[...].astype(BF)
    bdl[...] = (bd[...] - bdh[...].astype(F32)).astype(BF)
    bdt[0] = jnp.transpose(bd[...]).astype(BF)
    bdt[1] = (jnp.transpose(bd[...]) - bdt[0].astype(F32)).astype(BF)

    for t in range(3):
        lw[(1, 2, 0)[t]].wait()

    def project(src, first):
        for t in range(3):
            out = nn(xg[2 * src], w[t, pl.ds(pl.multiple_of(src * 512, 512), 256), :])
            out = out + nn(xg[2 * src + 1], w[t, pl.ds(pl.multiple_of(src * 512 + 256, 256), 256), :])
            if first:
                acc[t] = out
            else:
                acc[t] += out

    project(x, True)
    def build(i, _):
        f = lax.broadcasted_iota(jnp.int32, (SK, 1024), 1)
        fi, fj = f // SK, lax.rem(f, SK)
        a = lax.broadcasted_iota(jnp.int32, (SK, 1024), 0)
        b = lax.rem(a + i, SK)
        hit = ((fi == a) & (fj == b)) | ((fi == b) & (fj == a))
        value = jnp.where(i == 16, 0.5, 1.0)
        keep = jnp.where(i < NS, value, 0.0)
        fsel[pl.ds(pl.multiple_of(i * SK, SK), SK), :] = jnp.where(hit, keep, 0.0).astype(BF)
        return 0

    lax.fori_loop(0, NP // SK, build, 0)
    for h in range(4):
        for q in range(2):
            feat[q, h, NF:NP, :] = jnp.zeros((NP - NF, CT), BF)
    zpad[...] = jnp.zeros((128, NP), F32)
    tmp[...] = jnp.zeros((NP, 128), F32)
    dext[...] = jnp.zeros(dext.shape, BF)
    stk[...] = jnp.zeros(stk.shape, BF)
    zst[...] = jnp.zeros((SK, 128), F32)
    vtm[...] = jnp.zeros(vtm.shape, BF)
    sext[...] = jnp.zeros(sext.shape, F32)

    for i in range(2):
        ag[i].wait_send()
        ag[2 + i].start()
    ag[0].wait_recv()
    ag[4].start()
    ag[1].wait_recv()
    ag[5].start()
    ag[2].wait_recv()
    project(left, False)
    ag[3].wait_recv()
    project(right, False)
    ag[4].wait_recv()
    ag[5].wait_recv()

    cqkv = {}

    def last_projection(t):
        cqkv[t] = rc(xsend.at[t], qkv.at[t, c], ex_s.at[1 + t], ex_r.at[1 + t], seq_2=oc)
        for cols, target in ((oth_cols, None), (own_cols, c)):
            out = acc[t, :, cols] + nn(
                xg[2 * far], w[t, pl.ds(pl.multiple_of(far * 512, 512), 256), cols]
            )
            out = out + nn(
                xg[2 * far + 1], w[t, pl.ds(pl.multiple_of(far * 512 + 256, 256), 256), cols]
            )
            if target is None:
                xsend[t] = out.astype(BF)
                cqkv[t].start()
            else:
                qkv[t, target] = out.astype(BF)

    last_projection(1)
    last_projection(2)

    scale = SK ** (-0.5)

    def eights(v, k):
        return v if k == 0 else jnp.concatenate([v[8 * k :], v[: 8 * k]], axis=0)

    def ones(v, k):
        return v if k == 0 else pltpu.roll(v, SK - k, 0)

    def sketch(t, k):
        part = pl.ds(pl.multiple_of(256 * k, 256), 256)
        src = qkv[t, k]
        lr = nt(bdh[...], src) + nt(bdl[...], src)
        lrt[t, :, part] = lr
        st_ = lr[:128] * lr[128:] * scale
        skt[t, :, part] = st_
        skb[t, :, part] = st_.astype(BF)

        for h in range(4):
            for q in range(2):
                cols = pl.ds(pl.multiple_of(256 * k + 128 * q, 128), 128)
                s = st_[SK * h : SK * h + SK, 128 * q : 128 * q + 128]
                for b in range(8):
                    turned = ones(s, b)
                    for a in range(3 if b == 0 else 2):
                        i = 8 * a + b
                        feat[t, h, SK * i : SK * i + SK, cols] = (s * eights(turned, a)).astype(BF)

    def sketch_tokens(t):
        for k in range(2):
            tok = nt(qkv[t, k], bdh[...]) + nt(qkv[t, k], bdl[...])
            stok[256 * k : 256 * k + 256, :] = (tok[:, :128] * tok[:, 128:] * scale).astype(BF)

    lane256 = lax.broadcasted_iota(jnp.int32, (256, 256), 1)

    def pack_z(n, total):
        tmp[0:NF, :] = total
        zt = jnp.transpose(tmp[...])
        for j in range(5):
            zst[4 * j : 4 * j + 4, :] = zt[0:4, 128 * j : 128 * j + 128]
        wire[n, ZROW:WIRE, :] = zst[...].astype(BF)

    def others():
        for d in FAR_FIRST:
            py, pz = lax.rem(y + d // 4, 4), lax.rem(z + d % 4, 4)
            yield py * 4 + pz, {"seq_0": py, "seq_1": pz}

    def rows_of(r):
        return pl.ds(pl.multiple_of(r * ROWS, ROWS), ROWS)

    def scan_send(n, lo, hi):
        for r, where in others():

            @pl.when((r >= lo) & (r < hi))
            def _(r=r, where=where):
                rc(wire.at[n, rows_of(r)], inb.at[n, m], a_s.at[n], a_r.at[n], **where).start()

        @pl.when((m >= lo) & (m < hi))
        def _():
            inb[n, m] = wire[n, rows_of(m), :]

    def scan_own(n, reverse):
        @pl.when(m < OWN)
        def _():
            part = inb.at[n, 0 : CH - 1]
            rc(part, part, t_s, a_r.at[n], seq_2=oc).wait_recv()
            running = jnp.zeros((ROWS, 128), F32)
            for i in range(CH):
                r = CH - 1 - i if reverse else i
                outb[n, r] = running.astype(BF)
                running = running + inb[n, r].astype(F32)
            if reverse:
                totb[...] = running.astype(BF)
            for r, where in others():
                rc(outb.at[n, r], res.at[n, rows_of(m)], b_s.at[n], b_r.at[n], **where).start()
            res[n, rows_of(m), :] = outb[n, m]

    def share_totals():
        @pl.when(m < OWN)
        def _():
            for r, where in others():
                rc(totb, tot.at[c, rows_of(m)], t_s, t_r, **where).start()
            tot[c, rows_of(m), :] = totb[...]

    def from_owners(ref, sem):
        def all_of(count):
            part = ref.at[pl.ds(0, count * ROWS)]
            rc(part, part, t_s, sem, seq_2=oc).wait_recv()

        @pl.when(m < OWN)
        def _():
            all_of(OWN - 1)

        @pl.when(m >= OWN)
        def _():
            all_of(OWN)

    def sends_done():
        def all_of(part, sem):
            rc(part, part, sem, t_r, seq_2=oc).wait_send()

        @pl.when(m < OWN)
        def _():
            for n in range(2):
                all_of(wire.at[n, pl.ds(0, (OWN - 1) * ROWS)], a_s.at[n])
                all_of(outb.at[n, 0 : CH - 1], b_s.at[n])
            all_of(outb.at[0, 0 : CH - 1], t_s)

        @pl.when(m >= OWN)
        def _():
            for n in range(2):
                all_of(wire.at[n, pl.ds(0, OWN * ROWS)], a_s.at[n])

    def fold_in(n, state, norm):
        stk[0:256, :] = state
        pick = jnp.where(c == 0, norm[0:4, :], norm[4:8, :])
        stk[256:272, :] = jnp.concatenate([pick, jnp.zeros((12, 1024), F32)], axis=0).astype(BF)
        fold[n] = nt(fsel[...], stk[...])

    row_w = lax.broadcasted_iota(jnp.int32, (NF, 128), 0)
    weight = jnp.where((row_w < SK) | (row_w >= 16 * SK), 1.0, 2.0)

    def unpack(n):
        zst[...] = res[n, ZROW:WIRE, :].astype(F32)
        for j in range(5):
            zpad[0:4, 128 * j : 128 * j + 128] = zst[4 * j : 4 * j + 4, :]
        zc = jnp.transpose(zpad[...])[0:NF, :] * weight + fold[n, 0:NF, 256:384]
        for p in range(2):
            part = res[n, NF * p : NF * p + NF, :].astype(F32)
            sext[p, 0:NF, 0:128] = part * weight + fold[n, 0:NF, 128 * p : 128 * p + 128]
            sext[p, 0:NF, 128:256] = zc
            turned = jnp.transpose(sext[p]).astype(BF)
            for hh in range(2):
                sextt[2 * p + hh, 0:64, :] = turned[64 * hh : 64 * hh + 64, :]
                sextt[2 * p + hh, 64:80, :] = turned[128:144, :]

    def state_half(k, last):
        part = pl.ds(pl.multiple_of(256 * k, 256), 256)
        for p in range(2):
            vtok[p, part, 0:128] = qkv[2, k, :, 128 * p : 128 * p + 128]
            vtok[p, part, 128:256] = jnp.ones((256, 128), BF)
        ztot = None
        for p in range(2):
            out = st[p] if last else None
            for hh in range(2):
                h = 2 * p + hh
                keep = (lane256 // 64 == hh) | (lane256 == 128 + h)
                vm = jnp.where(keep, vtok[p, part, :].astype(F32), 0.0).astype(BF)
                term = nn(feat[1, h, 0:NF, part], vm)
                out = term if out is None else out + term
            if not last:
                st[p] = out
                continue
            wire[0, NF * p : NF * p + NF, :] = out[:, 0:128].astype(BF)
            ztot = out[:, 128:256] if ztot is None else ztot + out[:, 128:256]
            if p == 0:
                scan_send(0, 0, SPLIT)
        if last:
            pack_z(0, ztot)
            scan_send(0, SPLIT, OWN)

    sketch(1, c)
    state_half(c, False)
    cqkv[1].wait_recv()
    sketch(1, oc)
    cqkv[2].wait_recv()
    state_half(oc, True)

    last_projection(0)
    sketch_tokens(1)
    lp.wait()
    ln.wait()
    fold_in(0, psv[...].reshape(256, 1024).astype(BF), pnv)
    sketch(0, c)
    cqkv[0].wait_recv()
    sketch(0, oc)

    scan_own(0, False)

    la.wait()
    cga.wait_recv()
    for k in range(2):
        part = slice(256 * k, 256 * k + 256)
        gtr[:, part] = jnp.transpose(ga[k].astype(F32))
        vt = jnp.transpose(qkv[2, k].astype(F32)).astype(BF)
        for h in range(4):
            vtm[h, 64 * (h % 2) : 64 * (h % 2) + 64, part] = vt[64 * h : 64 * h + 64, :]
    row16 = lax.broadcasted_iota(jnp.int32, (16, CT), 0)
    for h in range(4):
        vtm[h, 128:144, :] = jnp.where(row16 == h, 1.0, 0.0).astype(BF)

    diag = lax.broadcasted_iota(jnp.int32, (256, 256), 0) <= lax.broadcasted_iota(
        jnp.int32, (256, 256), 1
    )
    lane_k = lax.broadcasted_iota(jnp.int32, (256, 128), 1) // SK

    def scores(h, hh):
        d_rows = slice(64 * hh, 64 * hh + 64)
        for jb in range(2):
            keys = jnp.where(lane_k == h, stok[256 * jb : 256 * jb + 256, :].astype(F32), 0.0)
            keys = keys.astype(BF)
            for ib in range(jb, 2):
                d = nn(keys, skb[0, :, 256 * ib : 256 * ib + 256])
                if ib == jb:
                    d = jnp.where(diag, d, 0.0)
                at = (h, slice(256 * jb, 256 * jb + 256), slice(256 * ib, 256 * ib + 256))
                scr[at] = (d * d).astype(BF)
                dmat[at] = (d + d).astype(BF)
        values = jnp.concatenate([vtm[h, d_rows, :], vtm[h, 128:144, :]], axis=0)
        yloc[h, :, 0:256] = nn(values[:, 0:256], scr[h, 0:256, 0:256])
        yloc[h, :, 256:512] = nn(values, scr[h, :, 256:512])

    def by_pairs(make):
        def one(p, _):
            for hh in range(2):
                make(2 * p + hh, hh)
            return 0

        lax.fori_loop(0, 2, one, 0)

    by_pairs(scores)
    le.wait()
    lm.wait()
    fold_in(1, dev[pl.ds(4 * c, 4)].reshape(256, 1024).astype(BF), dnv)

    from_owners(res.at[0], b_r.at[0])
    unpack(0)
    for h in range(4):
        yv[h] = nn(sextt[h], feat[0, h]) + yloc[h]
    for h in range(4):
        inv = 1.0 / (1.0 + yv[h, 64 + h : 65 + h, :])
        g = gtr[64 * h : 64 * h + 64, :]
        dden = -jnp.sum(g * yv[h, 0:64, :], axis=0, keepdims=True) * inv * inv
        dext[h, 64 * (h % 2) : 64 * (h % 2) + 64, :] = (g * inv).astype(BF)
        dext[h, 128:144, :] = jnp.where(row16 == h, dden, 0.0).astype(BF)
    ztot = None
    for p in range(2):
        out = nt(feat[0, 2 * p, 0:NF, :], dext[2 * p])
        out = out + nt(feat[0, 2 * p + 1, 0:NF, :], dext[2 * p + 1])
        wire[1, NF * p : NF * p + NF, :] = out[:, 0:128].astype(BF)
        ztot = out[:, 128:256] if ztot is None else ztot + out[:, 128:256]
        if p == 0:
            scan_send(1, 0, SPLIT)
    pack_z(1, ztot)
    scan_send(1, SPLIT, OWN)

    def lanes(ref, at, u):
        return jnp.concatenate(
            [ref[at + (slice(128 * u, 128 * u + 128),)], ref[at + (slice(256 + 128 * u, 384 + 128 * u),)]],
            axis=1,
        )

    def feature_grad(t, h, u, slot):
        rows = pl.ds(pl.multiple_of(h * SK, SK), SK)
        for q in range(2):
            cols = slice(256 * q + 128 * u, 256 * q + 128 * u + 128)
            mine_ = slice(128 * q, 128 * q + 128)
            s = skt[t, rows, cols]
            here = dst[t, rows, cols] + 2.0 * s * dfe[slot, 0:SK, mine_]
            for b in range(8):
                turned = ones(s, b)
                back = None
                for a in range(3 if b == 0 else 2):
                    i = 8 * a + b
                    if i == 0:
                        continue
                    d = dfe[slot, SK * i : SK * i + SK, mine_]
                    here = here + d * eights(turned, a)
                    term = eights(d * s, (4 - a) % 4)
                    back = term if back is None else back + term
                here = here + (back if b == 0 else pltpu.roll(back, b, 0))
            dst[t, rows, cols] = here

    def local_grads(h, hh):
        p = h // 2
        for jb in range(2):
            for ib in range(jb, 2):
                at = (h, slice(256 * jb, 256 * jb + 256), slice(256 * ib, 256 * ib + 256))
                ds = nn(vtok[p, 256 * jb : 256 * jb + 256, :], dext[h, :, 256 * ib : 256 * ib + 256])
                wmat[at] = (dmat[at].astype(F32) * ds).astype(BF)
        sk_rows = pl.ds(pl.multiple_of(h * SK, SK), SK)
        d_rows = slice(64 * hh, 64 * hh + 64)
        v_rows = pl.ds(pl.multiple_of(64 * h, 64), 64)
        dst[0, sk_rows, 0:256] = nn(skb[1, sk_rows, 0:256], wmat[h, 0:256, 0:256])
        dst[0, sk_rows, 256:512] = nn(skb[1, sk_rows, :], wmat[h, :, 256:512])
        dst[1, sk_rows, 0:256] = nt(skb[0, sk_rows, :], wmat[h, 0:256, :])
        dst[1, sk_rows, 256:512] = nt(skb[0, sk_rows, 256:512], wmat[h, 256:512, 256:512])
        dvt[v_rows, 0:256] = nt(dext[h, d_rows, :], scr[h, 0:256, :])
        dvt[v_rows, 256:512] = nt(dext[h, d_rows, 256:512], scr[h, 256:512, 256:512])

    def through_sketch(t, u):
        at = (slice(0, 128),)
        lt, rt = lanes(lrt.at[t], at, u), lanes(lrt.at[t], (slice(128, 256),), u)
        ds = lanes(dst.at[t], at, u) * scale
        dlr = jnp.concatenate([ds * rt, ds * lt], axis=0).astype(BF)
        return nn(bdt[0], dlr) + nn(bdt[1], dlr)

    def keep(t, u, grad):
        dtok[u, t] = jnp.transpose(grad).astype(BF)
        dall[t, c, 128 * u : 128 * u + 128, :] = dtok[
            u, t, pl.ds(pl.multiple_of(128 * c, 128), 128), :
        ]

    oth_half = pl.ds(pl.multiple_of(128 * oc, 128), 128)

    def hand_q(u):
        copy = rc(
            dtok.at[u, 0, oth_half], dall.at[0, c, 128 * u : 128 * u + 128],
            ex_s.at[4 + u], ex_r.at[4 + u], seq_2=oc,
        )
        copy.start()
        return copy

    def hand_kv(u):
        copy = rc(
            dtok.at[u, 1:3, oth_half], dall.at[1:3, c, 128 * u : 128 * u + 128],
            ex_s.at[6 + u], ex_r.at[6 + u], seq_2=oc,
        )
        copy.start()
        return copy

    by_pairs(local_grads)

    copy_q = []

    def queries_half(u):
        def grad_q(p, _):
            for hh in range(2):
                h = 2 * p + hh
                dfe[hh] = nn(sext[p, 0:NF, :].astype(BF), lanes(dext.at[h], (slice(0, 256),), u))
                feature_grad(0, h, u, hh)
            return 0

        lax.fori_loop(0, 2, grad_q, 0)
        keep(0, u, through_sketch(0, u))
        copy_q.append(hand_q(u))

    queries_half(0)
    scan_own(1, True)
    queries_half(1)

    for u in range(2):
        copy_q[u].wait_recv()

    def pull(t, b, rows, k):
        cols = pl.ds(pl.multiple_of(256 * k, 256), 256)
        return nt(dall[t, k, rows], w[t, pl.ds(pl.multiple_of(b * 512, 512), 512), cols])

    def pull_q(b, _):
        acc2[b] = pull(0, b, slice(0, 256), 0) + pull(0, b, slice(0, 256), 1)
        return 0

    lax.fori_loop(0, 4, pull_q, 0)

    from_owners(res.at[1], b_r.at[1])
    share_totals()
    unpack(1)

    def grads(u):
        def key_state(h):
            dfe[h] = nn(sextb[h // 2], lanes(vtm.at[h], (slice(0, 256),), u))

        key_state(0)
        for h in range(4):
            if h < 3:
                key_state(h + 1)
            v_rows = slice(64 * h, 64 * h + 64)
            out = nn(sextt[h, 0:64, :], lanes(feat.at[1, h], (slice(0, NP),), u))
            for q in range(2):
                cols = slice(256 * q + 128 * u, 256 * q + 128 * u + 128)
                dvt[v_rows, cols] += out[:, 128 * q : 128 * q + 128]
            feature_grad(1, h, u, h)
        keep(2, u, lanes(dvt, (slice(0, 256),), u))
        keep(1, u, through_sketch(1, u))
        return hand_kv(u)

    for p in range(2):
        sextb[p] = sext[p, 0:NF, :].astype(BF)
    copy_kv = [grads(0)]
    copy_kv.append(grads(1))

    rs = [
        [
            rc(
                rsend.at[u, i], rrecv.at[u, i], rs_s, rs_r.at[u, i],
                head=right if i in (0, 2, 4) else left,
            )
            for i in range(6)
        ]
        for u in range(2)
    ]

    def block(b, u, ahead=False):
        rows = slice(128 * u, 128 * u + 128)
        out = acc2[b, rows, :] + pull(1, b, rows, oc) + pull(2, b, rows, oc)
        return out if ahead else out + pull(1, b, rows, c) + pull(2, b, rows, c)

    def own_part(b, u):
        rows = slice(128 * u, 128 * u + 128)
        acc2[b, rows, :] += pull(1, b, rows, c) + pull(2, b, rows, c)

    def outgoing(u):
        rows = slice(128 * u, 128 * u + 128)
        out = block(far, u, u == 0)
        rsend[u, 0] = out[:, 0:256].astype(BF)
        rs[u][0].start()
        rsend[u, 1] = out[:, 256:512].astype(BF)
        rs[u][1].start()
        out = block(right, u)
        rsend[u, 2] = out[:, 256:512].astype(BF)
        rs[u][2].start()
        acc2[right, rows, 0:256] = out[:, 0:256]
        out = block(left, u)
        rsend[u, 3] = out[:, 0:256].astype(BF)
        rs[u][3].start()
        acc2[left, rows, 256:512] = out[:, 256:512]

    def merge(u):
        rows = slice(128 * u, 128 * u + 128)
        rs[u][0].wait_recv()
        rsend[u, 4] = (acc2[right, rows, 0:256] + rrecv[u, 0].astype(F32)).astype(BF)
        rs[u][4].start()
        rs[u][1].wait_recv()
        rsend[u, 5] = (acc2[left, rows, 256:512] + rrecv[u, 1].astype(F32)).astype(BF)
        rs[u][5].start()

    def arrived(u):
        rows = slice(128 * u, 128 * u + 128)
        rs[u][3].wait_recv()
        rs[u][4].wait_recv()
        oin[rows, 0:256] = (
            acc2[x, rows, 0:256] + rrecv[u, 3].astype(F32) + rrecv[u, 4].astype(F32)
        ).astype(BF)
        rs[u][2].wait_recv()
        rs[u][5].wait_recv()
        oin[rows, 256:512] = (
            acc2[x, rows, 256:512] + rrecv[u, 2].astype(F32) + rrecv[u, 5].astype(F32)
        ).astype(BF)

    own_part(far, 0)
    copy_kv[0].wait_recv()
    outgoing(0)
    copy_kv[1].wait_recv()
    outgoing(1)
    merge(0)
    for u in range(2):
        acc2[x, 128 * u : 128 * u + 128, :] = block(x, u)
    merge(1)
    for t in range(3):
        for k in range(2):
            oqkv[t, :, 256 * k : 256 * k + 256] = dall[t, k]

    from_owners(tot.at[c], t_r)
    whole = tot.at[c]
    copy_t = rc(whole, whole, ex_s.at[8], ex_r.at[8], seq_2=oc)
    copy_t.start()

    def totals(k):
        for p in range(2):
            tmp[0:NF, :] = tot[k, NF * p : NF * p + NF, :].astype(F32)
            part = nn(jnp.transpose(tmp[...]).astype(BF), fsel[...])
            for hh in range(2):
                h = 4 * k + 2 * p + hh
                dps[h] = dev[h] + part[64 * hh : 64 * hh + 64, :]
        zst[...] = tot[k, ZROW:WIRE, :].astype(F32)
        for j in range(5):
            zpad[pl.ds(pl.multiple_of(8 * k, 8), 4), 128 * j : 128 * j + 128] = zst[4 * j : 4 * j + 4, :]

    totals(c)
    copy_t.wait_recv()
    totals(oc)
    norms = nn(zpad[0:16, :].astype(BF), fsel[...])
    dpn[0:4, :] = dnv[0:4, :] + norms[0:4, :]
    dpn[4:8, :] = dnv[4:8, :] + norms[8:12, :]

    arrived(0)
    arrived(1)

    sends = xg.at[0:4]
    rc(sends, sends, ag_s.at[2], t_r, seq_2=oc).wait_send()
    for one in list(cqkv.values()) + [cga, copy_t] + copy_q + copy_kv:
        one.wait_send()
    sends = rsend.at[:]
    rc(sends, sends, rs_s, t_r, seq_2=oc).wait_send()
    sends_done()


def put_kernel(oin, oqkv, dps, dpn, oi_hbm, oq_hbm, ok_hbm, ov_hbm, os_hbm, on_hbm, sem):
    copies = [
        pltpu.make_async_copy(dps.at[4 * k : 4 * k + 4], os_hbm.at[4 * k : 4 * k + 4], sem.at[k])
        for k in range(2)
    ]
    copies += [
        pltpu.make_async_copy(oqkv.at[t], ref, sem.at[2 + t])
        for t, ref in enumerate((oq_hbm, ok_hbm, ov_hbm))
    ]
    copies.append(pltpu.make_async_copy(oin, oi_hbm, sem.at[5]))
    copies.append(pltpu.make_async_copy(dpn, on_hbm, sem.at[6]))
    for copy in copies:
        copy.start()
    for copy in copies:
        copy.wait()


def body(x, wq, wk, wv, sketch, prefix_state, prefix_norm, d_attn, d_state, d_norm):
    any_ = pl.BlockSpec(memory_space=pl.ANY)
    v = pltpu.VMEM
    scratch = [
        v((8, TOK, 256), BF),
        v((3, 2048, 512), BF),
        v((3, TOK, 512), F32),
        v((3, 2, TOK, 256), BF),
        v((3, TOK, 256), BF),
        v((2, TOK, 256), BF),
        v((2, SK, 64), F32),
        v((4, 64, 1024), F32),
        v((8, 1024), F32),
        v((8, 64, 1024), F32),
        v((8, 1024), F32),
        v((256, 256), F32),
        v((256, 256), BF),
        v((256, 256), BF),
        v((2, 256, 256), BF),
        v((2, 256, CT), F32),
        v((2, 128, CT), F32),
        v((2, 128, CT), BF),
        v((CT, 128), BF),
        v((2, NF, 256), F32),
        v((2, 4, NP, CT), BF),
        v((4, 256, CT), BF),
        v((2, CT, 256), BF),
        v((4, 256, CT), BF),
        v((2, NP, 384), F32),
        v((384, 1024), BF),
        v((NP, 1024), BF),
        v((4, 80, CT), F32),
        v((256, CT), F32),
        v((4, CT, CT), BF),
        v((4, CT, CT), BF),
        v((4, CT, CT), BF),
        v((4, 80, CT), F32),
        v((NP, 128), F32),
        v((SK, 128), F32),
        v((128, NP), F32),
        v((4, NF, 256), F32),
        v((2, 128, CT), F32),
        v((256, CT), F32),
        v((2, NP, 256), F32),
        v((4, 80, NP), BF),
        v((2, NF, 256), BF),
        v((2, WIRE, 128), BF),
        v((2, CH, ROWS, 128), BF),
        v((2, CH, ROWS, 128), BF),
        v((2, WIRE, 128), BF),
        v((ROWS, 128), BF),
        v((2, WIRE, 128), BF),
        v((2, 3, 256, 256), BF),
        v((3, 2, TOK, 256), BF),
        v((4, TOK, 512), F32),
        v((2, 6, 128, 256), BF),
        v((2, 6, 128, 256), BF),
    ]
    sem = pltpu.SemaphoreType.DMA
    scratch += [
        sem((11,)), sem((3,)), sem((6,)), sem((9,)), sem((9,)), sem((2,)), sem((2,)),
        sem((2,)), sem((2,)), sem, sem, sem, sem((2, 6)),
    ]
    swap = (0, 2, 1)
    made = (
        v((TOK, 512), BF),
        v((3, TOK, 512), BF),
        v((8, 64, 1024), F32),
        v((8, 1024), F32),
    )
    held = pl.BlockSpec(memory_space=pltpu.VMEM)
    outs = pl.pallas_call(
        kernel,
        out_shape=made,
        in_specs=[any_] * 10,
        out_specs=(held,) * 4,
        scratch_shapes=scratch,
        compiler_params=pltpu.CompilerParams(
            collective_id=0, has_side_effects=True, vmem_limit_bytes=60 * 1024 * 1024
        ),
        name="sketch_bwd",
    )(
        x, wq, wk, wv, jnp.transpose(sketch, swap), jnp.transpose(prefix_state, swap),
        prefix_norm, d_attn, jnp.transpose(d_state, swap), d_norm,
    )
    rows = jax.ShapeDtypeStruct((TOK, 512), BF)
    outs = pl.pallas_call(
        put_kernel,
        out_shape=(
            rows, rows, rows, rows,
            jax.ShapeDtypeStruct((8, 64, 1024), F32),
            jax.ShapeDtypeStruct((8, 1024), F32),
        ),
        in_specs=[held] * 4,
        out_specs=(any_,) * 6,
        scratch_shapes=[sem((7,))],
        compiler_params=pltpu.CompilerParams(vmem_limit_bytes=1024 * 1024),
        name="put_out",
    )(*(pltpu.with_memory_space_constraint(o, pltpu.VMEM) for o in outs))
    return outs[:4] + (jnp.transpose(outs[4], swap), outs[5])


def solution(mesh):
    finer = Mesh(
        mesh.devices.reshape(4, 4, 2, mesh.shape["head"]), ("seq_0", "seq_1", "seq_2", "head")
    )
    state, rows = P("head", None, None), P("head", None)
    tokens, weight = P(SEQ, "head"), P(None, "head")
    return jax.shard_map(
        body,
        mesh=finer,
        in_specs=(tokens, weight, weight, weight, P(), state, rows, tokens, state, rows),
        out_specs=(tokens, tokens, tokens, tokens, state, rows),
        check_vma=False,
    )
```

```python
import jax
import jax.numpy as jnp
from jax import lax
from jax.experimental import pallas as pl
from jax.experimental.pallas import tpu as pltpu
from jax.sharding import Mesh
from jax.sharding import PartitionSpec as P

SEQ = ("seq_0", "seq_1", "seq_2")
MESH = pl.DeviceIdType.MESH
F32 = jnp.float32
BF = jnp.bfloat16

SK = 32
NS = 17
NF = NS * SK
NP = 640
TOK = 256
CT = 512
CH = 16
ROWS = 80
OWN = 14
WIRE = OWN * ROWS
FAR_FIRST = (10, 9, 11, 6, 14, 2, 8, 5, 7, 13, 15, 1, 3, 4, 12)
ZROW = 2 * NF


def nn(a, b):
    return lax.dot_general(a, b, (((1,), (0,)), ((), ())), preferred_element_type=F32)


def nt(a, b):
    return lax.dot_general(a, b, (((1,), (1,)), ((), ())), preferred_element_type=F32)


def kernel(
    x_hbm, wq_hbm, wk_hbm, wv_hbm, g_hbm, ps_hbm, pn_hbm, da_hbm, de_hbm, dn_hbm,
    oin, oqkv, dps, dpn,
    xg, w, acc, qkv, xsend, ga, gt, psv, pnv, dev, dnv,
    bd, bdh, bdl, bdt, lrt, skt, skb, stok, st, feat, vtm, vtok, dext, fold, stk, fsel,
    yloc, gtr, scr, dmat, wmat, yv, tmp, zst, zpad, dfe, dst, dvt, sext, sextt, sextb,
    wire, inb, outb, res, totb, tot, dtok, dall, acc2, rsend, rrecv,
    loc, ag_s, ag_r, ex_s, ex_r, a_s, a_r, b_s, b_r, t_s, t_r, rs_s, rs_r,
):
    y = lax.axis_index("seq_0")
    z = lax.axis_index("seq_1")
    c = lax.axis_index("seq_2")
    x = lax.axis_index("head")
    m = y * 4 + z
    oc = 1 - c
    right, left, far = lax.rem(x + 1, 4), lax.rem(x + 3, 4), lax.rem(x + 2, 4)

    def rc(src, dst_, ss, rs, **where):
        return pltpu.make_async_remote_copy(
            src_ref=src, dst_ref=dst_, send_sem=ss, recv_sem=rs,
            device_id=where, device_id_type=MESH,
        )

    own_cols = pl.ds(pl.multiple_of(c * 256, 256), 256)
    oth_cols = pl.ds(pl.multiple_of(oc * 256, 256), 256)

    lx = [
        pltpu.make_async_copy(x_hbm.at[:, 256 * k : 256 * k + 256], xg.at[2 * x + k], loc.at[k])
        for k in range(2)
    ]
    lw = [
        pltpu.make_async_copy(src, w.at[t], loc.at[2 + t])
        for t, src in enumerate((wq_hbm, wk_hbm, wv_hbm))
    ]
    lg = pltpu.make_async_copy(g_hbm, gt, loc.at[5])
    la = pltpu.make_async_copy(da_hbm.at[:, own_cols], ga.at[c], loc.at[6])
    ln = pltpu.make_async_copy(pn_hbm, pnv, loc.at[7])
    lp = pltpu.make_async_copy(ps_hbm.at[pl.ds(4 * c, 4)], psv, loc.at[8])
    le = pltpu.make_async_copy(de_hbm, dev, loc.at[9])
    lm = pltpu.make_async_copy(dn_hbm, dnv, loc.at[10])
    for copy in (lx[0], lx[1], lw[1], lw[2], lw[0], lg, la, ln, lp, le, lm):
        copy.start()

    bar = pltpu.get_barrier_semaphore()
    for peer in (right, left):
        pl.semaphore_signal(bar, inc=1, device_id={"head": peer}, device_id_type=MESH)
    pl.semaphore_signal(bar, inc=1, device_id={"seq_2": oc}, device_id_type=MESH)

    def greet(d, _):
        r = lax.rem(m + d, CH)
        pl.semaphore_signal(
            bar, inc=1, device_id={"seq_0": r // 4, "seq_1": lax.rem(r, 4)}, device_id_type=MESH
        )
        return 0

    lax.fori_loop(1, CH, greet, 0)
    pl.semaphore_wait(bar, 18)

    def slab(src, k, peer, i):
        ref = xg.at[2 * src + k]
        return rc(ref, ref, ag_s.at[min(i, 2)], ag_r.at[i], head=peer)

    ag = [
        slab(x, 0, right, 0), slab(x, 1, left, 1), slab(x, 1, right, 2), slab(x, 0, left, 3),
        slab(left, 0, right, 4), slab(right, 1, left, 5),
    ]
    lx[0].wait()
    lx[1].wait()
    for i in range(2):
        ag[i].start()
    cga = rc(da_hbm.at[:, oth_cols], ga.at[c], ex_s.at[0], ex_r.at[0], seq_2=oc)
    cga.start()

    lg.wait()
    bd[...] = jnp.zeros((256, 256), F32)
    lane128 = lax.broadcasted_iota(jnp.int32, (SK, 128), 1) // 64
    for lr in range(2):
        wide = jnp.concatenate([gt[lr], gt[lr]], axis=1)
        for h in range(4):
            row = lr * 128 + h * SK
            col = 128 * (h // 2)
            bd[row : row + SK, col : col + 128] = jnp.where(lane128 == h % 2, wide, 0.0)
    bdh[...] = bd[...].astype(BF)
    bdl[...] = (bd[...] - bdh[...].astype(F32)).astype(BF)
    bdt[0] = jnp.transpose(bd[...]).astype(BF)
    bdt[1] = (jnp.transpose(bd[...]) - bdt[0].astype(F32)).astype(BF)

    for t in range(3):
        lw[(1, 2, 0)[t]].wait()

    def project(src, first):
        for t in range(3):
            out = nn(xg[2 * src], w[t, pl.ds(pl.multiple_of(src * 512, 512), 256), :])
            out = out + nn(xg[2 * src + 1], w[t, pl.ds(pl.multiple_of(src * 512 + 256, 256), 256), :])
            if first:
                acc[t] = out
            else:
                acc[t] += out

    project(x, True)
    def build(i, _):
        f = lax.broadcasted_iota(jnp.int32, (SK, 1024), 1)
        fi, fj = f // SK, lax.rem(f, SK)
        a = lax.broadcasted_iota(jnp.int32, (SK, 1024), 0)
        b = lax.rem(a + i, SK)
        hit = ((fi == a) & (fj == b)) | ((fi == b) & (fj == a))
        value = jnp.where(i == 16, 0.5, 1.0)
        keep = jnp.where(i < NS, value, 0.0)
        fsel[pl.ds(pl.multiple_of(i * SK, SK), SK), :] = jnp.where(hit, keep, 0.0).astype(BF)
        return 0

    lax.fori_loop(0, NP // SK, build, 0)
    for h in range(4):
        for q in range(2):
            feat[q, h, NF:NP, :] = jnp.zeros((NP - NF, CT), BF)
    zpad[...] = jnp.zeros((128, NP), F32)
    tmp[...] = jnp.zeros((NP, 128), F32)
    dext[...] = jnp.zeros(dext.shape, BF)
    stk[...] = jnp.zeros(stk.shape, BF)
    zst[...] = jnp.zeros((SK, 128), F32)
    vtm[...] = jnp.zeros(vtm.shape, BF)
    sext[...] = jnp.zeros(sext.shape, F32)

    for i in range(2):
        ag[i].wait_send()
        ag[2 + i].start()
    ag[0].wait_recv()
    ag[4].start()
    ag[1].wait_recv()
    ag[5].start()
    ag[2].wait_recv()
    project(left, False)
    ag[3].wait_recv()
    project(right, False)
    ag[4].wait_recv()
    ag[5].wait_recv()

    cqkv = {}

    def last_projection(t):
        cqkv[t] = rc(xsend.at[t], qkv.at[t, c], ex_s.at[1 + t], ex_r.at[1 + t], seq_2=oc)
        for cols, target in ((oth_cols, None), (own_cols, c)):
            out = acc[t, :, cols] + nn(
                xg[2 * far], w[t, pl.ds(pl.multiple_of(far * 512, 512), 256), cols]
            )
            out = out + nn(
                xg[2 * far + 1], w[t, pl.ds(pl.multiple_of(far * 512 + 256, 256), 256), cols]
            )
            if target is None:
                xsend[t] = out.astype(BF)
            else:
                qkv[t, target] = out.astype(BF)
        cqkv[t].start()

    last_projection(1)
    last_projection(2)

    scale = SK ** (-0.5)

    def eights(v, k):
        return v if k == 0 else jnp.concatenate([v[8 * k :], v[: 8 * k]], axis=0)

    def ones(v, k):
        return v if k == 0 else pltpu.roll(v, SK - k, 0)

    def sketch(t, k):
        part = pl.ds(pl.multiple_of(256 * k, 256), 256)
        src = qkv[t, k]
        lr = nt(bdh[...], src) + nt(bdl[...], src)
        lrt[t, :, part] = lr
        st_ = lr[:128] * lr[128:] * scale
        skt[t, :, part] = st_
        skb[t, :, part] = st_.astype(BF)

        for h in range(4):
            for q in range(2):
                cols = pl.ds(pl.multiple_of(256 * k + 128 * q, 128), 128)
                s = st_[SK * h : SK * h + SK, 128 * q : 128 * q + 128]
                for b in range(8):
                    turned = ones(s, b)
                    for a in range(3 if b == 0 else 2):
                        i = 8 * a + b
                        feat[t, h, SK * i : SK * i + SK, cols] = (s * eights(turned, a)).astype(BF)

    def sketch_tokens(t):
        for k in range(2):
            tok = nt(qkv[t, k], bdh[...]) + nt(qkv[t, k], bdl[...])
            stok[256 * k : 256 * k + 256, :] = (tok[:, :128] * tok[:, 128:] * scale).astype(BF)

    lane256 = lax.broadcasted_iota(jnp.int32, (256, 256), 1)

    def pack_z(n, total):
        tmp[0:NF, :] = total
        zt = jnp.transpose(tmp[...])
        for j in range(5):
            zst[4 * j : 4 * j + 4, :] = zt[0:4, 128 * j : 128 * j + 128]
        wire[n, ZROW:WIRE, :] = zst[...].astype(BF)

    def others():
        for d in FAR_FIRST:
            py, pz = lax.rem(y + d // 4, 4), lax.rem(z + d % 4, 4)
            yield py * 4 + pz, {"seq_0": py, "seq_1": pz}

    def rows_of(r):
        return pl.ds(pl.multiple_of(r * ROWS, ROWS), ROWS)

    def scan_send(n, lo, hi):
        for r, where in others():

            @pl.when((r >= lo) & (r < hi))
            def _(r=r, where=where):
                rc(wire.at[n, rows_of(r)], inb.at[n, m], a_s.at[n], a_r.at[n], **where).start()

        @pl.when((m >= lo) & (m < hi))
        def _():
            inb[n, m] = wire[n, rows_of(m), :]

    def scan_own(n, reverse):
        @pl.when(m < OWN)
        def _():
            part = inb.at[n, 0 : CH - 1]
            rc(part, part, t_s, a_r.at[n], seq_2=oc).wait_recv()
            running = jnp.zeros((ROWS, 128), F32)
            for i in range(CH):
                r = CH - 1 - i if reverse else i
                outb[n, r] = running.astype(BF)
                running = running + inb[n, r].astype(F32)
            if reverse:
                totb[...] = running.astype(BF)
            for r, where in others():
                rc(outb.at[n, r], res.at[n, rows_of(m)], b_s.at[n], b_r.at[n], **where).start()
            res[n, rows_of(m), :] = outb[n, m]

    def share_totals():
        @pl.when(m < OWN)
        def _():
            for r, where in others():
                rc(totb, tot.at[c, rows_of(m)], t_s, t_r, **where).start()
            tot[c, rows_of(m), :] = totb[...]

    def from_owners(ref, sem):
        def all_of(count):
            part = ref.at[pl.ds(0, count * ROWS)]
            rc(part, part, t_s, sem, seq_2=oc).wait_recv()

        @pl.when(m < OWN)
        def _():
            all_of(OWN - 1)

        @pl.when(m >= OWN)
        def _():
            all_of(OWN)

    def sends_done():
        def all_of(part, sem):
            rc(part, part, sem, t_r, seq_2=oc).wait_send()

        @pl.when(m < OWN)
        def _():
            for n in range(2):
                all_of(wire.at[n, pl.ds(0, (OWN - 1) * ROWS)], a_s.at[n])
                all_of(outb.at[n, 0 : CH - 1], b_s.at[n])
            all_of(outb.at[0, 0 : CH - 1], t_s)

        @pl.when(m >= OWN)
        def _():
            for n in range(2):
                all_of(wire.at[n, pl.ds(0, OWN * ROWS)], a_s.at[n])

    def fold_in(n, state, norm):
        stk[0:256, :] = state
        pick = jnp.where(c == 0, norm[0:4, :], norm[4:8, :])
        stk[256:272, :] = jnp.concatenate([pick, jnp.zeros((12, 1024), F32)], axis=0).astype(BF)
        fold[n] = nt(fsel[...], stk[...])

    row_w = lax.broadcasted_iota(jnp.int32, (NF, 128), 0)
    weight = jnp.where((row_w < SK) | (row_w >= 16 * SK), 1.0, 2.0)

    def unpack(n):
        zst[...] = res[n, ZROW:WIRE, :].astype(F32)
        for j in range(5):
            zpad[0:4, 128 * j : 128 * j + 128] = zst[4 * j : 4 * j + 4, :]
        zc = jnp.transpose(zpad[...])[0:NF, :] * weight + fold[n, 0:NF, 256:384]
        for p in range(2):
            part = res[n, NF * p : NF * p + NF, :].astype(F32)
            sext[p, 0:NF, 0:128] = part * weight + fold[n, 0:NF, 128 * p : 128 * p + 128]
            sext[p, 0:NF, 128:256] = zc
            turned = jnp.transpose(sext[p]).astype(BF)
            for hh in range(2):
                sextt[2 * p + hh, 0:64, :] = turned[64 * hh : 64 * hh + 64, :]
                sextt[2 * p + hh, 64:80, :] = turned[128:144, :]

    def state_half(k, last):
        part = pl.ds(pl.multiple_of(256 * k, 256), 256)
        for p in range(2):
            vtok[p, part, 0:128] = qkv[2, k, :, 128 * p : 128 * p + 128]
            vtok[p, part, 128:256] = jnp.ones((256, 128), BF)
        ztot = None
        for p in range(2):
            out = st[p] if last else None
            for hh in range(2):
                h = 2 * p + hh
                keep = (lane256 // 64 == hh) | (lane256 == 128 + h)
                vm = jnp.where(keep, vtok[p, part, :].astype(F32), 0.0).astype(BF)
                term = nn(feat[1, h, 0:NF, part], vm)
                out = term if out is None else out + term
            if not last:
                st[p] = out
                continue
            wire[0, NF * p : NF * p + NF, :] = out[:, 0:128].astype(BF)
            ztot = out[:, 128:256] if ztot is None else ztot + out[:, 128:256]
        if last:
            pack_z(0, ztot)
            scan_send(0, 0, OWN)

    sketch(1, c)
    state_half(c, False)
    cqkv[1].wait_recv()
    sketch(1, oc)
    cqkv[2].wait_recv()
    state_half(oc, True)

    last_projection(0)
    sketch_tokens(1)
    lp.wait()
    ln.wait()
    fold_in(0, psv[...].reshape(256, 1024).astype(BF), pnv)
    sketch(0, c)
    cqkv[0].wait_recv()
    sketch(0, oc)

    scan_own(0, False)

    la.wait()
    cga.wait_recv()
    for k in range(2):
        part = slice(256 * k, 256 * k + 256)
        gtr[:, part] = jnp.transpose(ga[k].astype(F32))
        vt = jnp.transpose(qkv[2, k].astype(F32)).astype(BF)
        for h in range(4):
            vtm[h, 64 * (h % 2) : 64 * (h % 2) + 64, part] = vt[64 * h : 64 * h + 64, :]
    row16 = lax.broadcasted_iota(jnp.int32, (16, CT), 0)
    for h in range(4):
        vtm[h, 128:144, :] = jnp.where(row16 == h, 1.0, 0.0).astype(BF)

    diag = lax.broadcasted_iota(jnp.int32, (256, 256), 0) <= lax.broadcasted_iota(
        jnp.int32, (256, 256), 1
    )
    lane_k = lax.broadcasted_iota(jnp.int32, (256, 128), 1) // SK

    def scores(h, hh):
        d_rows = slice(64 * hh, 64 * hh + 64)
        for jb in range(2):
            keys = jnp.where(lane_k == h, stok[256 * jb : 256 * jb + 256, :].astype(F32), 0.0)
            keys = keys.astype(BF)
            for ib in range(jb, 2):
                d = nn(keys, skb[0, :, 256 * ib : 256 * ib + 256])
                if ib == jb:
                    d = jnp.where(diag, d, 0.0)
                at = (h, slice(256 * jb, 256 * jb + 256), slice(256 * ib, 256 * ib + 256))
                scr[at] = (d * d).astype(BF)
                dmat[at] = (d + d).astype(BF)
        values = jnp.concatenate([vtm[h, d_rows, :], vtm[h, 128:144, :]], axis=0)
        yloc[h, :, 0:256] = nn(values[:, 0:256], scr[h, 0:256, 0:256])
        yloc[h, :, 256:512] = nn(values, scr[h, :, 256:512])

    def by_pairs(make):
        def one(p, _):
            for hh in range(2):
                make(2 * p + hh, hh)
            return 0

        lax.fori_loop(0, 2, one, 0)

    by_pairs(scores)
    le.wait()
    lm.wait()
    fold_in(1, dev[pl.ds(4 * c, 4)].reshape(256, 1024).astype(BF), dnv)

    from_owners(res.at[0], b_r.at[0])
    unpack(0)
    for h in range(4):
        yv[h] = nn(sextt[h], feat[0, h]) + yloc[h]
    for h in range(4):
        inv = 1.0 / (1.0 + yv[h, 64 + h : 65 + h, :])
        g = gtr[64 * h : 64 * h + 64, :]
        dden = -jnp.sum(g * yv[h, 0:64, :], axis=0, keepdims=True) * inv * inv
        dext[h, 64 * (h % 2) : 64 * (h % 2) + 64, :] = (g * inv).astype(BF)
        dext[h, 128:144, :] = jnp.where(row16 == h, dden, 0.0).astype(BF)
    ztot = None
    for p in range(2):
        out = nt(feat[0, 2 * p, 0:NF, :], dext[2 * p])
        out = out + nt(feat[0, 2 * p + 1, 0:NF, :], dext[2 * p + 1])
        wire[1, NF * p : NF * p + NF, :] = out[:, 0:128].astype(BF)
        ztot = out[:, 128:256] if ztot is None else ztot + out[:, 128:256]
    pack_z(1, ztot)
    scan_send(1, 0, OWN)

    def lanes(ref, at, u):
        return jnp.concatenate(
            [ref[at + (slice(128 * u, 128 * u + 128),)], ref[at + (slice(256 + 128 * u, 384 + 128 * u),)]],
            axis=1,
        )

    def feature_grad(t, h, u, slot):
        rows = pl.ds(pl.multiple_of(h * SK, SK), SK)
        for q in range(2):
            cols = slice(256 * q + 128 * u, 256 * q + 128 * u + 128)
            mine_ = slice(128 * q, 128 * q + 128)
            s = skt[t, rows, cols]
            here = dst[t, rows, cols] + 2.0 * s * dfe[slot, 0:SK, mine_]
            for b in range(8):
                turned = ones(s, b)
                back = None
                for a in range(3 if b == 0 else 2):
                    i = 8 * a + b
                    if i == 0:
                        continue
                    d = dfe[slot, SK * i : SK * i + SK, mine_]
                    here = here + d * eights(turned, a)
                    term = eights(d * s, (4 - a) % 4)
                    back = term if back is None else back + term
                here = here + (back if b == 0 else pltpu.roll(back, b, 0))
            dst[t, rows, cols] = here

    def local_grads(h, hh):
        p = h // 2
        for jb in range(2):
            for ib in range(jb, 2):
                at = (h, slice(256 * jb, 256 * jb + 256), slice(256 * ib, 256 * ib + 256))
                ds = nn(vtok[p, 256 * jb : 256 * jb + 256, :], dext[h, :, 256 * ib : 256 * ib + 256])
                wmat[at] = (dmat[at].astype(F32) * ds).astype(BF)
        sk_rows = pl.ds(pl.multiple_of(h * SK, SK), SK)
        d_rows = slice(64 * hh, 64 * hh + 64)
        v_rows = pl.ds(pl.multiple_of(64 * h, 64), 64)
        dst[0, sk_rows, 0:256] = nn(skb[1, sk_rows, 0:256], wmat[h, 0:256, 0:256])
        dst[0, sk_rows, 256:512] = nn(skb[1, sk_rows, :], wmat[h, :, 256:512])
        dst[1, sk_rows, 0:256] = nt(skb[0, sk_rows, :], wmat[h, 0:256, :])
        dst[1, sk_rows, 256:512] = nt(skb[0, sk_rows, 256:512], wmat[h, 256:512, 256:512])
        dvt[v_rows, 0:256] = nt(dext[h, d_rows, :], scr[h, 0:256, :])
        dvt[v_rows, 256:512] = nt(dext[h, d_rows, 256:512], scr[h, 256:512, 256:512])

    def through_sketch(t, u):
        at = (slice(0, 128),)
        lt, rt = lanes(lrt.at[t], at, u), lanes(lrt.at[t], (slice(128, 256),), u)
        ds = lanes(dst.at[t], at, u) * scale
        dlr = jnp.concatenate([ds * rt, ds * lt], axis=0).astype(BF)
        return nn(bdt[0], dlr) + nn(bdt[1], dlr)

    def keep(t, u, grad):
        dtok[u, t] = jnp.transpose(grad).astype(BF)
        dall[t, c, 128 * u : 128 * u + 128, :] = dtok[
            u, t, pl.ds(pl.multiple_of(128 * c, 128), 128), :
        ]

    oth_half = pl.ds(pl.multiple_of(128 * oc, 128), 128)

    def hand_q(u):
        copy = rc(
            dtok.at[u, 0, oth_half], dall.at[0, c, 128 * u : 128 * u + 128],
            ex_s.at[4 + u], ex_r.at[4 + u], seq_2=oc,
        )
        copy.start()
        return copy

    def hand_kv(u):
        copy = rc(
            dtok.at[u, 1:3, oth_half], dall.at[1:3, c, 128 * u : 128 * u + 128],
            ex_s.at[6 + u], ex_r.at[6 + u], seq_2=oc,
        )
        copy.start()
        return copy

    by_pairs(local_grads)

    copy_q = []

    def queries_half(u):
        def grad_q(p, _):
            for hh in range(2):
                h = 2 * p + hh
                dfe[hh] = nn(sext[p, 0:NF, :].astype(BF), lanes(dext.at[h], (slice(0, 256),), u))
                feature_grad(0, h, u, hh)
            return 0

        lax.fori_loop(0, 2, grad_q, 0)
        keep(0, u, through_sketch(0, u))
        copy_q.append(hand_q(u))

    queries_half(0)
    scan_own(1, True)
    queries_half(1)

    for u in range(2):
        copy_q[u].wait_recv()

    def pull(t, b, rows, k):
        cols = pl.ds(pl.multiple_of(256 * k, 256), 256)
        return nt(dall[t, k, rows], w[t, pl.ds(pl.multiple_of(b * 512, 512), 512), cols])

    def pull_q(b, _):
        acc2[b] = pull(0, b, slice(0, 256), 0) + pull(0, b, slice(0, 256), 1)
        return 0

    lax.fori_loop(0, 4, pull_q, 0)

    from_owners(res.at[1], b_r.at[1])
    share_totals()
    unpack(1)

    def grads(u):
        def key_state(h):
            dfe[h] = nn(sextb[h // 2], lanes(vtm.at[h], (slice(0, 256),), u))

        key_state(0)
        for h in range(4):
            if h < 3:
                key_state(h + 1)
            v_rows = slice(64 * h, 64 * h + 64)
            out = nn(sextt[h, 0:64, :], lanes(feat.at[1, h], (slice(0, NP),), u))
            for q in range(2):
                cols = slice(256 * q + 128 * u, 256 * q + 128 * u + 128)
                dvt[v_rows, cols] += out[:, 128 * q : 128 * q + 128]
            feature_grad(1, h, u, h)
        keep(2, u, lanes(dvt, (slice(0, 256),), u))
        keep(1, u, through_sketch(1, u))
        return hand_kv(u)

    for p in range(2):
        sextb[p] = sext[p, 0:NF, :].astype(BF)
    copy_kv = [grads(0)]
    copy_kv.append(grads(1))

    rs = [
        [
            rc(
                rsend.at[u, i], rrecv.at[u, i], rs_s, rs_r.at[u, i],
                head=right if i in (0, 2, 4) else left,
            )
            for i in range(6)
        ]
        for u in range(2)
    ]

    def block(b, u, ahead=False):
        rows = slice(128 * u, 128 * u + 128)
        out = acc2[b, rows, :] + pull(1, b, rows, oc) + pull(2, b, rows, oc)
        return out if ahead else out + pull(1, b, rows, c) + pull(2, b, rows, c)

    def own_part(b, u):
        rows = slice(128 * u, 128 * u + 128)
        acc2[b, rows, :] += pull(1, b, rows, c) + pull(2, b, rows, c)

    def outgoing(u):
        rows = slice(128 * u, 128 * u + 128)
        out = block(far, u, u == 0)
        rsend[u, 0] = out[:, 0:256].astype(BF)
        rs[u][0].start()
        rsend[u, 1] = out[:, 256:512].astype(BF)
        rs[u][1].start()
        out_r = block(right, u)
        out_l = block(left, u)
        rsend[u, 2] = out_r[:, 256:512].astype(BF)
        rsend[u, 3] = out_l[:, 0:256].astype(BF)
        acc2[right, rows, 0:256] = out_r[:, 0:256]
        acc2[left, rows, 256:512] = out_l[:, 256:512]
        rs[u][2].start()
        rs[u][3].start()

    def merge(u):
        rows = slice(128 * u, 128 * u + 128)
        rs[u][0].wait_recv()
        rsend[u, 4] = (acc2[right, rows, 0:256] + rrecv[u, 0].astype(F32)).astype(BF)
        rs[u][4].start()
        rs[u][1].wait_recv()
        rsend[u, 5] = (acc2[left, rows, 256:512] + rrecv[u, 1].astype(F32)).astype(BF)
        rs[u][5].start()

    def arrived(u):
        rows = slice(128 * u, 128 * u + 128)
        rs[u][3].wait_recv()
        rs[u][4].wait_recv()
        oin[rows, 0:256] = (
            acc2[x, rows, 0:256] + rrecv[u, 3].astype(F32) + rrecv[u, 4].astype(F32)
        ).astype(BF)
        rs[u][2].wait_recv()
        rs[u][5].wait_recv()
        oin[rows, 256:512] = (
            acc2[x, rows, 256:512] + rrecv[u, 2].astype(F32) + rrecv[u, 5].astype(F32)
        ).astype(BF)

    own_part(far, 0)
    copy_kv[0].wait_recv()
    outgoing(0)
    copy_kv[1].wait_recv()
    outgoing(1)
    merge(0)
    for u in range(2):
        acc2[x, 128 * u : 128 * u + 128, :] = block(x, u)
    merge(1)
    for t in range(3):
        for k in range(2):
            oqkv[t, :, 256 * k : 256 * k + 256] = dall[t, k]

    from_owners(tot.at[c], t_r)
    whole = tot.at[c]
    copy_t = rc(whole, whole, ex_s.at[8], ex_r.at[8], seq_2=oc)
    copy_t.start()

    def totals(k):
        for p in range(2):
            tmp[0:NF, :] = tot[k, NF * p : NF * p + NF, :].astype(F32)
            part = nn(jnp.transpose(tmp[...]).astype(BF), fsel[...])
            for hh in range(2):
                h = 4 * k + 2 * p + hh
                dps[h] = dev[h] + part[64 * hh : 64 * hh + 64, :]
        zst[...] = tot[k, ZROW:WIRE, :].astype(F32)
        for j in range(5):
            zpad[pl.ds(pl.multiple_of(8 * k, 8), 4), 128 * j : 128 * j + 128] = zst[4 * j : 4 * j + 4, :]

    totals(c)
    copy_t.wait_recv()
    totals(oc)
    norms = nn(zpad[0:16, :].astype(BF), fsel[...])
    dpn[0:4, :] = dnv[0:4, :] + norms[0:4, :]
    dpn[4:8, :] = dnv[4:8, :] + norms[8:12, :]

    arrived(0)
    arrived(1)

    sends = xg.at[0:4]
    rc(sends, sends, ag_s.at[2], t_r, seq_2=oc).wait_send()
    for one in list(cqkv.values()) + [cga, copy_t] + copy_q + copy_kv:
        one.wait_send()
    sends = rsend.at[:]
    rc(sends, sends, rs_s, t_r, seq_2=oc).wait_send()
    sends_done()


def put_kernel(oin, oqkv, dps, dpn, oi_hbm, oq_hbm, ok_hbm, ov_hbm, os_hbm, on_hbm, sem):
    copies = [
        pltpu.make_async_copy(dps.at[4 * k : 4 * k + 4], os_hbm.at[4 * k : 4 * k + 4], sem.at[k])
        for k in range(2)
    ]
    copies += [
        pltpu.make_async_copy(oqkv.at[t], ref, sem.at[2 + t])
        for t, ref in enumerate((oq_hbm, ok_hbm, ov_hbm))
    ]
    copies.append(pltpu.make_async_copy(oin, oi_hbm, sem.at[5]))
    copies.append(pltpu.make_async_copy(dpn, on_hbm, sem.at[6]))
    for copy in copies:
        copy.start()
    for copy in copies:
        copy.wait()


def body(x, wq, wk, wv, sketch, prefix_state, prefix_norm, d_attn, d_state, d_norm):
    any_ = pl.BlockSpec(memory_space=pl.ANY)
    v = pltpu.VMEM
    scratch = [
        v((8, TOK, 256), BF),
        v((3, 2048, 512), BF),
        v((3, TOK, 512), F32),
        v((3, 2, TOK, 256), BF),
        v((3, TOK, 256), BF),
        v((2, TOK, 256), BF),
        v((2, SK, 64), F32),
        v((4, 64, 1024), F32),
        v((8, 1024), F32),
        v((8, 64, 1024), F32),
        v((8, 1024), F32),
        v((256, 256), F32),
        v((256, 256), BF),
        v((256, 256), BF),
        v((2, 256, 256), BF),
        v((2, 256, CT), F32),
        v((2, 128, CT), F32),
        v((2, 128, CT), BF),
        v((CT, 128), BF),
        v((2, NF, 256), F32),
        v((2, 4, NP, CT), BF),
        v((4, 256, CT), BF),
        v((2, CT, 256), BF),
        v((4, 256, CT), BF),
        v((2, NP, 384), F32),
        v((384, 1024), BF),
        v((NP, 1024), BF),
        v((4, 80, CT), F32),
        v((256, CT), F32),
        v((4, CT, CT), BF),
        v((4, CT, CT), BF),
        v((4, CT, CT), BF),
        v((4, 80, CT), F32),
        v((NP, 128), F32),
        v((SK, 128), F32),
        v((128, NP), F32),
        v((4, NF, 256), F32),
        v((2, 128, CT), F32),
        v((256, CT), F32),
        v((2, NP, 256), F32),
        v((4, 80, NP), BF),
        v((2, NF, 256), BF),
        v((2, WIRE, 128), BF),
        v((2, CH, ROWS, 128), BF),
        v((2, CH, ROWS, 128), BF),
        v((2, WIRE, 128), BF),
        v((ROWS, 128), BF),
        v((2, WIRE, 128), BF),
        v((2, 3, 256, 256), BF),
        v((3, 2, TOK, 256), BF),
        v((4, TOK, 512), F32),
        v((2, 6, 128, 256), BF),
        v((2, 6, 128, 256), BF),
    ]
    sem = pltpu.SemaphoreType.DMA
    scratch += [
        sem((11,)), sem((3,)), sem((6,)), sem((9,)), sem((9,)), sem((2,)), sem((2,)),
        sem((2,)), sem((2,)), sem, sem, sem, sem((2, 6)),
    ]
    swap = (0, 2, 1)
    made = (
        v((TOK, 512), BF),
        v((3, TOK, 512), BF),
        v((8, 64, 1024), F32),
        v((8, 1024), F32),
    )
    held = pl.BlockSpec(memory_space=pltpu.VMEM)
    outs = pl.pallas_call(
        kernel,
        out_shape=made,
        in_specs=[any_] * 10,
        out_specs=(held,) * 4,
        scratch_shapes=scratch,
        compiler_params=pltpu.CompilerParams(
            collective_id=0, has_side_effects=True, vmem_limit_bytes=60 * 1024 * 1024
        ),
        name="sketch_bwd",
    )(
        x, wq, wk, wv, jnp.transpose(sketch, swap), jnp.transpose(prefix_state, swap),
        prefix_norm, d_attn, jnp.transpose(d_state, swap), d_norm,
    )
    rows = jax.ShapeDtypeStruct((TOK, 512), BF)
    outs = pl.pallas_call(
        put_kernel,
        out_shape=(
            rows, rows, rows, rows,
            jax.ShapeDtypeStruct((8, 64, 1024), F32),
            jax.ShapeDtypeStruct((8, 1024), F32),
        ),
        in_specs=[held] * 4,
        out_specs=(any_,) * 6,
        scratch_shapes=[sem((7,))],
        compiler_params=pltpu.CompilerParams(vmem_limit_bytes=1024 * 1024),
        name="put_out",
    )(*(pltpu.with_memory_space_constraint(o, pltpu.VMEM) for o in outs))
    return outs[:4] + (jnp.transpose(outs[4], swap), outs[5])


def solution(mesh):
    finer = Mesh(
        mesh.devices.reshape(4, 4, 2, mesh.shape["head"]), ("seq_0", "seq_1", "seq_2", "head")
    )
    state, rows = P("head", None, None), P("head", None)
    tokens, weight = P(SEQ, "head"), P(None, "head")
    return jax.shard_map(
        body,
        mesh=finer,
        in_specs=(tokens, weight, weight, weight, P(), state, rows, tokens, state, rows),
        out_specs=(tokens, tokens, tokens, tokens, state, rows),
        check_vma=False,
    )
```

```python
import jax
import jax.numpy as jnp
from jax import lax
from jax.experimental import pallas as pl
from jax.experimental.pallas import tpu as pltpu
from jax.sharding import Mesh
from jax.sharding import PartitionSpec as P

SEQ = ("seq_0", "seq_1", "seq_2")
MESH = pl.DeviceIdType.MESH
F32 = jnp.float32
BF = jnp.bfloat16

SK = 32
NS = 17
NF = NS * SK
NP = 640
TOK = 256
CT = 512
CH = 16
ROWS = 80
OWN = 14
WIRE = OWN * ROWS
FAR_FIRST = (10, 9, 11, 6, 14, 2, 8, 5, 7, 13, 15, 1, 3, 4, 12)
ZROW = 2 * NF


def nn(a, b):
    return lax.dot_general(a, b, (((1,), (0,)), ((), ())), preferred_element_type=F32)


def nt(a, b):
    return lax.dot_general(a, b, (((1,), (1,)), ((), ())), preferred_element_type=F32)


def kernel(
    x_hbm, wq_hbm, wk_hbm, wv_hbm, g_hbm, ps_hbm, pn_hbm, da_hbm, de_hbm, dn_hbm,
    oin, oqkv, dps, dpn,
    xg, w, acc, qkv, xsend, ga, gt, psv, pnv, dev, dnv,
    bd, bdh, bdl, bdt, lrt, skt, skb, stok, st, feat, vtm, vtok, dext, fold, stk, fsel,
    yloc, gtr, scr, dmat, wmat, yv, tmp, zst, zpad, dfe, dst, dvt, sext, sextt, sextb,
    wire, inb, outb, res, totb, tot, dtok, dall, acc2, rsend, rrecv,
    loc, ag_s, ag_r, ex_s, ex_r, a_s, a_r, b_s, b_r, t_s, t_r, rs_s, rs_r,
):
    y = lax.axis_index("seq_0")
    z = lax.axis_index("seq_1")
    c = lax.axis_index("seq_2")
    x = lax.axis_index("head")
    m = y * 4 + z
    oc = 1 - c
    right, left, far = lax.rem(x + 1, 4), lax.rem(x + 3, 4), lax.rem(x + 2, 4)

    def rc(src, dst_, ss, rs, **where):
        return pltpu.make_async_remote_copy(
            src_ref=src, dst_ref=dst_, send_sem=ss, recv_sem=rs,
            device_id=where, device_id_type=MESH,
        )

    own_cols = pl.ds(pl.multiple_of(c * 256, 256), 256)
    oth_cols = pl.ds(pl.multiple_of(oc * 256, 256), 256)

    lx = [
        pltpu.make_async_copy(x_hbm.at[:, 256 * k : 256 * k + 256], xg.at[2 * x + k], loc.at[k])
        for k in range(2)
    ]
    lw = [
        pltpu.make_async_copy(src, w.at[t], loc.at[2 + t])
        for t, src in enumerate((wq_hbm, wk_hbm, wv_hbm))
    ]
    lg = pltpu.make_async_copy(g_hbm, gt, loc.at[5])
    la = pltpu.make_async_copy(da_hbm.at[:, own_cols], ga.at[c], loc.at[6])
    ln = pltpu.make_async_copy(pn_hbm, pnv, loc.at[7])
    lp = pltpu.make_async_copy(ps_hbm.at[pl.ds(4 * c, 4)], psv, loc.at[8])
    le = pltpu.make_async_copy(de_hbm, dev, loc.at[9])
    lm = pltpu.make_async_copy(dn_hbm, dnv, loc.at[10])
    for copy in (lx[0], lx[1], lw[1], lw[2], lw[0], lg, la, ln, lp, le, lm):
        copy.start()

    bar = pltpu.get_barrier_semaphore()
    for peer in (right, left):
        pl.semaphore_signal(bar, inc=1, device_id={"head": peer}, device_id_type=MESH)
    pl.semaphore_signal(bar, inc=1, device_id={"seq_2": oc}, device_id_type=MESH)

    def greet(d, _):
        r = lax.rem(m + d, CH)
        pl.semaphore_signal(
            bar, inc=1, device_id={"seq_0": r // 4, "seq_1": lax.rem(r, 4)}, device_id_type=MESH
        )
        return 0

    lax.fori_loop(1, CH, greet, 0)
    pl.semaphore_wait(bar, 18)

    def slab(src, k, peer, i):
        ref = xg.at[2 * src + k]
        return rc(ref, ref, ag_s.at[min(i, 2)], ag_r.at[i], head=peer)

    ag = [
        slab(x, 0, right, 0), slab(x, 1, left, 1), slab(x, 1, right, 2), slab(x, 0, left, 3),
        slab(left, 0, right, 4), slab(right, 1, left, 5),
    ]
    lx[0].wait()
    lx[1].wait()
    for i in range(2):
        ag[i].start()
    cga = rc(da_hbm.at[:, oth_cols], ga.at[c], ex_s.at[0], ex_r.at[0], seq_2=oc)
    cga.start()

    lg.wait()
    bd[...] = jnp.zeros((256, 256), F32)
    lane128 = lax.broadcasted_iota(jnp.int32, (SK, 128), 1) // 64
    for lr in range(2):
        wide = jnp.concatenate([gt[lr], gt[lr]], axis=1)
        for h in range(4):
            row = lr * 128 + h * SK
            col = 128 * (h // 2)
            bd[row : row + SK, col : col + 128] = jnp.where(lane128 == h % 2, wide, 0.0)
    bdh[...] = bd[...].astype(BF)
    bdl[...] = (bd[...] - bdh[...].astype(F32)).astype(BF)
    bdt[0] = jnp.transpose(bd[...]).astype(BF)
    bdt[1] = (jnp.transpose(bd[...]) - bdt[0].astype(F32)).astype(BF)

    for t in range(3):
        lw[(1, 2, 0)[t]].wait()

    def project(src, first):
        for t in range(3):
            out = nn(xg[2 * src], w[t, pl.ds(pl.multiple_of(src * 512, 512), 256), :])
            out = out + nn(xg[2 * src + 1], w[t, pl.ds(pl.multiple_of(src * 512 + 256, 256), 256), :])
            if first:
                acc[t] = out
            else:
                acc[t] += out

    project(x, True)
    def build(i, _):
        f = lax.broadcasted_iota(jnp.int32, (SK, 1024), 1)
        fi, fj = f // SK, lax.rem(f, SK)
        a = lax.broadcasted_iota(jnp.int32, (SK, 1024), 0)
        b = lax.rem(a + i, SK)
        hit = ((fi == a) & (fj == b)) | ((fi == b) & (fj == a))
        value = jnp.where(i == 16, 0.5, 1.0)
        keep = jnp.where(i < NS, value, 0.0)
        fsel[pl.ds(pl.multiple_of(i * SK, SK), SK), :] = jnp.where(hit, keep, 0.0).astype(BF)
        return 0

    lax.fori_loop(0, NP // SK, build, 0)
    for h in range(4):
        for q in range(2):
            feat[q, h, NF:NP, :] = jnp.zeros((NP - NF, CT), BF)
    zpad[...] = jnp.zeros((128, NP), F32)
    tmp[...] = jnp.zeros((NP, 128), F32)
    dext[...] = jnp.zeros(dext.shape, BF)
    stk[...] = jnp.zeros(stk.shape, BF)
    zst[...] = jnp.zeros((SK, 128), F32)
    vtm[...] = jnp.zeros(vtm.shape, BF)
    sext[...] = jnp.zeros(sext.shape, F32)

    for i in range(2):
        ag[i].wait_send()
        ag[2 + i].start()
    ag[0].wait_recv()
    ag[4].start()
    ag[1].wait_recv()
    ag[5].start()
    ag[2].wait_recv()
    project(left, False)
    ag[3].wait_recv()
    project(right, False)
    ag[4].wait_recv()
    ag[5].wait_recv()

    cqkv = {}

    def last_projection(t):
        cqkv[t] = rc(xsend.at[t], qkv.at[t, c], ex_s.at[1 + t], ex_r.at[1 + t], seq_2=oc)
        for cols, target in ((oth_cols, None), (own_cols, c)):
            out = acc[t, :, cols] + nn(
                xg[2 * far], w[t, pl.ds(pl.multiple_of(far * 512, 512), 256), cols]
            )
            out = out + nn(
                xg[2 * far + 1], w[t, pl.ds(pl.multiple_of(far * 512 + 256, 256), 256), cols]
            )
            if target is None:
                xsend[t] = out.astype(BF)
            else:
                qkv[t, target] = out.astype(BF)
        cqkv[t].start()

    last_projection(1)
    last_projection(2)

    scale = SK ** (-0.5)

    def eights(v, k):
        return v if k == 0 else jnp.concatenate([v[8 * k :], v[: 8 * k]], axis=0)

    def ones(v, k):
        return v if k == 0 else pltpu.roll(v, SK - k, 0)

    def sketch(t, k):
        part = pl.ds(pl.multiple_of(256 * k, 256), 256)
        src = qkv[t, k]
        lr = nt(bdh[...], src) + nt(bdl[...], src)
        lrt[t, :, part] = lr
        st_ = lr[:128] * lr[128:] * scale
        skt[t, :, part] = st_
        skb[t, :, part] = st_.astype(BF)

        for h in range(4):
            for q in range(2):
                cols = pl.ds(pl.multiple_of(256 * k + 128 * q, 128), 128)
                s = st_[SK * h : SK * h + SK, 128 * q : 128 * q + 128]
                for b in range(8):
                    turned = ones(s, b)
                    for a in range(3 if b == 0 else 2):
                        i = 8 * a + b
                        feat[t, h, SK * i : SK * i + SK, cols] = (s * eights(turned, a)).astype(BF)

    def sketch_tokens(t):
        for k in range(2):
            tok = nt(qkv[t, k], bdh[...]) + nt(qkv[t, k], bdl[...])
            stok[256 * k : 256 * k + 256, :] = (tok[:, :128] * tok[:, 128:] * scale).astype(BF)

    lane256 = lax.broadcasted_iota(jnp.int32, (256, 256), 1)

    def pack_z(n, total):
        tmp[0:NF, :] = total
        zt = jnp.transpose(tmp[...])
        for j in range(5):
            zst[4 * j : 4 * j + 4, :] = zt[0:4, 128 * j : 128 * j + 128]
        wire[n, ZROW:WIRE, :] = zst[...].astype(BF)

    def others():
        for d in FAR_FIRST:
            py, pz = lax.rem(y + d // 4, 4), lax.rem(z + d % 4, 4)
            yield py * 4 + pz, {"seq_0": py, "seq_1": pz}

    def rows_of(r):
        return pl.ds(pl.multiple_of(r * ROWS, ROWS), ROWS)

    def scan_send(n, lo, hi):
        for r, where in others():

            @pl.when((r >= lo) & (r < hi))
            def _(r=r, where=where):
                rc(wire.at[n, rows_of(r)], inb.at[n, m], a_s.at[n], a_r.at[n], **where).start()

        @pl.when((m >= lo) & (m < hi))
        def _():
            inb[n, m] = wire[n, rows_of(m), :]

    def scan_own(n, reverse):
        @pl.when(m < OWN)
        def _():
            part = inb.at[n, 0 : CH - 1]
            rc(part, part, t_s, a_r.at[n], seq_2=oc).wait_recv()
            running = jnp.zeros((ROWS, 128), F32)
            for i in range(CH):
                r = CH - 1 - i if reverse else i
                outb[n, r] = running.astype(BF)
                running = running + inb[n, r].astype(F32)
            if reverse:
                totb[...] = running.astype(BF)
            for r, where in others():
                rc(outb.at[n, r], res.at[n, rows_of(m)], b_s.at[n], b_r.at[n], **where).start()
            res[n, rows_of(m), :] = outb[n, m]

    def share_totals():
        @pl.when(m < OWN)
        def _():
            for r, where in others():
                rc(totb, tot.at[c, rows_of(m)], t_s, t_r, **where).start()
            tot[c, rows_of(m), :] = totb[...]

    def from_owners(ref, sem):
        def all_of(count):
            part = ref.at[pl.ds(0, count * ROWS)]
            rc(part, part, t_s, sem, seq_2=oc).wait_recv()

        @pl.when(m < OWN)
        def _():
            all_of(OWN - 1)

        @pl.when(m >= OWN)
        def _():
            all_of(OWN)

    def sends_done():
        def all_of(part, sem):
            rc(part, part, sem, t_r, seq_2=oc).wait_send()

        @pl.when(m < OWN)
        def _():
            for n in range(2):
                all_of(wire.at[n, pl.ds(0, (OWN - 1) * ROWS)], a_s.at[n])
                all_of(outb.at[n, 0 : CH - 1], b_s.at[n])
            all_of(outb.at[0, 0 : CH - 1], t_s)

        @pl.when(m >= OWN)
        def _():
            for n in range(2):
                all_of(wire.at[n, pl.ds(0, OWN * ROWS)], a_s.at[n])

    def fold_in(n, state, norm):
        stk[0:256, :] = state
        pick = jnp.where(c == 0, norm[0:4, :], norm[4:8, :])
        stk[256:272, :] = jnp.concatenate([pick, jnp.zeros((12, 1024), F32)], axis=0).astype(BF)
        fold[n] = nt(fsel[...], stk[...])

    row_w = lax.broadcasted_iota(jnp.int32, (NF, 128), 0)
    weight = jnp.where((row_w < SK) | (row_w >= 16 * SK), 1.0, 2.0)

    def unpack(n):
        zst[...] = res[n, ZROW:WIRE, :].astype(F32)
        for j in range(5):
            zpad[0:4, 128 * j : 128 * j + 128] = zst[4 * j : 4 * j + 4, :]
        zc = jnp.transpose(zpad[...])[0:NF, :] * weight + fold[n, 0:NF, 256:384]
        for p in range(2):
            part = res[n, NF * p : NF * p + NF, :].astype(F32)
            sext[p, 0:NF, 0:128] = part * weight + fold[n, 0:NF, 128 * p : 128 * p + 128]
            sext[p, 0:NF, 128:256] = zc
            turned = jnp.transpose(sext[p]).astype(BF)
            for hh in range(2):
                sextt[2 * p + hh, 0:64, :] = turned[64 * hh : 64 * hh + 64, :]
                sextt[2 * p + hh, 64:80, :] = turned[128:144, :]

    def state_half(k, last):
        part = pl.ds(pl.multiple_of(256 * k, 256), 256)
        for p in range(2):
            vtok[p, part, 0:128] = qkv[2, k, :, 128 * p : 128 * p + 128]
            vtok[p, part, 128:256] = jnp.ones((256, 128), BF)
        ztot = None
        for p in range(2):
            out = st[p] if last else None
            for hh in range(2):
                h = 2 * p + hh
                keep = (lane256 // 64 == hh) | (lane256 == 128 + h)
                vm = jnp.where(keep, vtok[p, part, :].astype(F32), 0.0).astype(BF)
                term = nn(feat[1, h, 0:NF, part], vm)
                out = term if out is None else out + term
            if not last:
                st[p] = out
                continue
            wire[0, NF * p : NF * p + NF, :] = out[:, 0:128].astype(BF)
            ztot = out[:, 128:256] if ztot is None else ztot + out[:, 128:256]
        if last:
            pack_z(0, ztot)
            scan_send(0, 0, OWN)

    sketch(1, c)
    state_half(c, False)
    cqkv[1].wait_recv()
    sketch(1, oc)
    cqkv[2].wait_recv()
    state_half(oc, True)

    last_projection(0)
    sketch_tokens(1)
    lp.wait()
    ln.wait()
    fold_in(0, psv[...].reshape(256, 1024).astype(BF), pnv)
    sketch(0, c)
    cqkv[0].wait_recv()
    sketch(0, oc)

    scan_own(0, False)

    la.wait()
    cga.wait_recv()
    for k in range(2):
        part = slice(256 * k, 256 * k + 256)
        gtr[:, part] = jnp.transpose(ga[k].astype(F32))
        vt = jnp.transpose(qkv[2, k].astype(F32)).astype(BF)
        for h in range(4):
            vtm[h, 64 * (h % 2) : 64 * (h % 2) + 64, part] = vt[64 * h : 64 * h + 64, :]
    row16 = lax.broadcasted_iota(jnp.int32, (16, CT), 0)
    for h in range(4):
        vtm[h, 128:144, :] = jnp.where(row16 == h, 1.0, 0.0).astype(BF)

    diag = lax.broadcasted_iota(jnp.int32, (256, 256), 0) <= lax.broadcasted_iota(
        jnp.int32, (256, 256), 1
    )
    lane_k = lax.broadcasted_iota(jnp.int32, (256, 128), 1) // SK

    def scores(h, hh):
        d_rows = slice(64 * hh, 64 * hh + 64)
        for jb in range(2):
            keys = jnp.where(lane_k == h, stok[256 * jb : 256 * jb + 256, :].astype(F32), 0.0)
            keys = keys.astype(BF)
            for ib in range(jb, 2):
                d = nn(keys, skb[0, :, 256 * ib : 256 * ib + 256])
                if ib == jb:
                    d = jnp.where(diag, d, 0.0)
                at = (h, slice(256 * jb, 256 * jb + 256), slice(256 * ib, 256 * ib + 256))
                scr[at] = (d * d).astype(BF)
                dmat[at] = (d + d).astype(BF)
        values = jnp.concatenate([vtm[h, d_rows, :], vtm[h, 128:144, :]], axis=0)
        yloc[h, :, 0:256] = nn(values[:, 0:256], scr[h, 0:256, 0:256])
        yloc[h, :, 256:512] = nn(values, scr[h, :, 256:512])

    def by_pairs(make):
        def one(p, _):
            for hh in range(2):
                make(2 * p + hh, hh)
            return 0

        lax.fori_loop(0, 2, one, 0)

    by_pairs(scores)
    le.wait()
    lm.wait()
    fold_in(1, dev[pl.ds(4 * c, 4)].reshape(256, 1024).astype(BF), dnv)

    from_owners(res.at[0], b_r.at[0])
    unpack(0)
    for h in range(4):
        yv[h] = nn(sextt[h], feat[0, h]) + yloc[h]
    for h in range(4):
        inv = 1.0 / (1.0 + yv[h, 64 + h : 65 + h, :])
        g = gtr[64 * h : 64 * h + 64, :]
        dden = -jnp.sum(g * yv[h, 0:64, :], axis=0, keepdims=True) * inv * inv
        dext[h, 64 * (h % 2) : 64 * (h % 2) + 64, :] = (g * inv).astype(BF)
        dext[h, 128:144, :] = jnp.where(row16 == h, dden, 0.0).astype(BF)
    ztot = None
    for p in range(2):
        out = nt(feat[0, 2 * p, 0:NF, :], dext[2 * p])
        out = out + nt(feat[0, 2 * p + 1, 0:NF, :], dext[2 * p + 1])
        wire[1, NF * p : NF * p + NF, :] = out[:, 0:128].astype(BF)
        ztot = out[:, 128:256] if ztot is None else ztot + out[:, 128:256]
    pack_z(1, ztot)
    scan_send(1, 0, OWN)

    def lanes(ref, at, u):
        return jnp.concatenate(
            [ref[at + (slice(128 * u, 128 * u + 128),)], ref[at + (slice(256 + 128 * u, 384 + 128 * u),)]],
            axis=1,
        )

    def feature_grad(t, h, u, slot):
        rows = pl.ds(pl.multiple_of(h * SK, SK), SK)
        for q in range(2):
            cols = slice(256 * q + 128 * u, 256 * q + 128 * u + 128)
            mine_ = slice(128 * q, 128 * q + 128)
            s = skt[t, rows, cols]
            here = dst[t, rows, cols] + 2.0 * s * dfe[slot, 0:SK, mine_]
            for b in range(8):
                turned = ones(s, b)
                back = None
                for a in range(3 if b == 0 else 2):
                    i = 8 * a + b
                    if i == 0:
                        continue
                    d = dfe[slot, SK * i : SK * i + SK, mine_]
                    here = here + d * eights(turned, a)
                    term = eights(d * s, (4 - a) % 4)
                    back = term if back is None else back + term
                here = here + (back if b == 0 else pltpu.roll(back, b, 0))
            dst[t, rows, cols] = here

    def local_grads(h, hh):
        p = h // 2
        for jb in range(2):
            for ib in range(jb, 2):
                at = (h, slice(256 * jb, 256 * jb + 256), slice(256 * ib, 256 * ib + 256))
                ds = nn(vtok[p, 256 * jb : 256 * jb + 256, :], dext[h, :, 256 * ib : 256 * ib + 256])
                wmat[at] = (dmat[at].astype(F32) * ds).astype(BF)
        sk_rows = pl.ds(pl.multiple_of(h * SK, SK), SK)
        d_rows = slice(64 * hh, 64 * hh + 64)
        v_rows = pl.ds(pl.multiple_of(64 * h, 64), 64)
        dst[0, sk_rows, 0:256] = nn(skb[1, sk_rows, 0:256], wmat[h, 0:256, 0:256])
        dst[0, sk_rows, 256:512] = nn(skb[1, sk_rows, :], wmat[h, :, 256:512])
        dst[1, sk_rows, 0:256] = nt(skb[0, sk_rows, :], wmat[h, 0:256, :])
        dst[1, sk_rows, 256:512] = nt(skb[0, sk_rows, 256:512], wmat[h, 256:512, 256:512])
        dvt[v_rows, 0:256] = nt(dext[h, d_rows, :], scr[h, 0:256, :])
        dvt[v_rows, 256:512] = nt(dext[h, d_rows, 256:512], scr[h, 256:512, 256:512])

    def through_sketch(t, u):
        at = (slice(0, 128),)
        lt, rt = lanes(lrt.at[t], at, u), lanes(lrt.at[t], (slice(128, 256),), u)
        ds = lanes(dst.at[t], at, u) * scale
        dlr = jnp.concatenate([ds * rt, ds * lt], axis=0).astype(BF)
        return nn(bdt[0], dlr) + nn(bdt[1], dlr)

    def keep(t, u, grad):
        dtok[u, t] = jnp.transpose(grad).astype(BF)
        dall[t, c, 128 * u : 128 * u + 128, :] = dtok[
            u, t, pl.ds(pl.multiple_of(128 * c, 128), 128), :
        ]

    oth_half = pl.ds(pl.multiple_of(128 * oc, 128), 128)

    def hand_q(u):
        copy = rc(
            dtok.at[u, 0, oth_half], dall.at[0, c, 128 * u : 128 * u + 128],
            ex_s.at[4 + u], ex_r.at[4 + u], seq_2=oc,
        )
        copy.start()
        return copy

    def hand_kv(u):
        copy = rc(
            dtok.at[u, 1:3, oth_half], dall.at[1:3, c, 128 * u : 128 * u + 128],
            ex_s.at[6 + u], ex_r.at[6 + u], seq_2=oc,
        )
        copy.start()
        return copy

    by_pairs(local_grads)

    copy_q = []

    def queries_half(u):
        def grad_q(p, _):
            for hh in range(2):
                h = 2 * p + hh
                dfe[hh] = nn(sext[p, 0:NF, :].astype(BF), lanes(dext.at[h], (slice(0, 256),), u))
                feature_grad(0, h, u, hh)
            return 0

        lax.fori_loop(0, 2, grad_q, 0)
        keep(0, u, through_sketch(0, u))
        copy_q.append(hand_q(u))

    queries_half(0)
    scan_own(1, True)
    queries_half(1)

    for u in range(2):
        copy_q[u].wait_recv()

    def pull(t, b, rows, k):
        cols = pl.ds(pl.multiple_of(256 * k, 256), 256)
        return nt(dall[t, k, rows], w[t, pl.ds(pl.multiple_of(b * 512, 512), 512), cols])

    def pull_q(b, _):
        acc2[b] = pull(0, b, slice(0, 256), 0) + pull(0, b, slice(0, 256), 1)
        return 0

    lax.fori_loop(0, 4, pull_q, 0)

    from_owners(res.at[1], b_r.at[1])
    share_totals()
    unpack(1)

    def grads(u):
        def key_state(h):
            dfe[h] = nn(sextb[h // 2], lanes(vtm.at[h], (slice(0, 256),), u))

        key_state(0)
        for h in range(4):
            if h < 3:
                key_state(h + 1)
            v_rows = slice(64 * h, 64 * h + 64)
            out = nn(sextt[h, 0:64, :], lanes(feat.at[1, h], (slice(0, NP),), u))
            for q in range(2):
                cols = slice(256 * q + 128 * u, 256 * q + 128 * u + 128)
                dvt[v_rows, cols] += out[:, 128 * q : 128 * q + 128]
            feature_grad(1, h, u, h)
        keep(2, u, lanes(dvt, (slice(0, 256),), u))
        keep(1, u, through_sketch(1, u))
        return hand_kv(u)

    for p in range(2):
        sextb[p] = sext[p, 0:NF, :].astype(BF)
    copy_kv = [grads(0)]
    copy_kv.append(grads(1))

    rs = [
        [
            rc(
                rsend.at[u, i], rrecv.at[u, i], rs_s, rs_r.at[u, i],
                head=right if i in (0, 2, 4) else left,
            )
            for i in range(6)
        ]
        for u in range(2)
    ]

    def block(b, u, ahead=False):
        rows = slice(128 * u, 128 * u + 128)
        out = acc2[b, rows, :] + pull(1, b, rows, oc) + pull(2, b, rows, oc)
        return out if ahead else out + pull(1, b, rows, c) + pull(2, b, rows, c)

    def own_part(b, u):
        rows = slice(128 * u, 128 * u + 128)
        acc2[b, rows, :] += pull(1, b, rows, c) + pull(2, b, rows, c)

    def outgoing(u):
        rows = slice(128 * u, 128 * u + 128)
        out = block(far, u, u == 0)
        rsend[u, 0] = out[:, 0:256].astype(BF)
        rs[u][0].start()
        rsend[u, 1] = out[:, 256:512].astype(BF)
        rs[u][1].start()
        out = block(right, u)
        rsend[u, 2] = out[:, 256:512].astype(BF)
        rs[u][2].start()
        acc2[right, rows, 0:256] = out[:, 0:256]
        out = block(left, u)
        rsend[u, 3] = out[:, 0:256].astype(BF)
        rs[u][3].start()
        acc2[left, rows, 256:512] = out[:, 256:512]

    def merge(u):
        rows = slice(128 * u, 128 * u + 128)
        rs[u][0].wait_recv()
        rsend[u, 4] = (acc2[right, rows, 0:256] + rrecv[u, 0].astype(F32)).astype(BF)
        rs[u][4].start()
        rs[u][1].wait_recv()
        rsend[u, 5] = (acc2[left, rows, 256:512] + rrecv[u, 1].astype(F32)).astype(BF)
        rs[u][5].start()

    def arrived(u):
        rows = slice(128 * u, 128 * u + 128)
        rs[u][3].wait_recv()
        rs[u][4].wait_recv()
        oin[rows, 0:256] = (
            acc2[x, rows, 0:256] + rrecv[u, 3].astype(F32) + rrecv[u, 4].astype(F32)
        ).astype(BF)
        rs[u][2].wait_recv()
        rs[u][5].wait_recv()
        oin[rows, 256:512] = (
            acc2[x, rows, 256:512] + rrecv[u, 2].astype(F32) + rrecv[u, 5].astype(F32)
        ).astype(BF)

    own_part(far, 0)
    copy_kv[0].wait_recv()
    outgoing(0)
    copy_kv[1].wait_recv()
    outgoing(1)
    merge(0)
    for u in range(2):
        acc2[x, 128 * u : 128 * u + 128, :] = block(x, u)
    merge(1)
    for t in range(3):
        for k in range(2):
            oqkv[t, :, 256 * k : 256 * k + 256] = dall[t, k]

    from_owners(tot.at[c], t_r)
    whole = tot.at[c]
    copy_t = rc(whole, whole, ex_s.at[8], ex_r.at[8], seq_2=oc)
    copy_t.start()

    def totals(k):
        for p in range(2):
            tmp[0:NF, :] = tot[k, NF * p : NF * p + NF, :].astype(F32)
            part = nn(jnp.transpose(tmp[...]).astype(BF), fsel[...])
            for hh in range(2):
                h = 4 * k + 2 * p + hh
                dps[h] = dev[h] + part[64 * hh : 64 * hh + 64, :]
        zst[...] = tot[k, ZROW:WIRE, :].astype(F32)
        for j in range(5):
            zpad[pl.ds(pl.multiple_of(8 * k, 8), 4), 128 * j : 128 * j + 128] = zst[4 * j : 4 * j + 4, :]

    totals(c)
    copy_t.wait_recv()
    totals(oc)
    norms = nn(zpad[0:16, :].astype(BF), fsel[...])
    dpn[0:4, :] = dnv[0:4, :] + norms[0:4, :]
    dpn[4:8, :] = dnv[4:8, :] + norms[8:12, :]

    arrived(0)
    arrived(1)

    sends = xg.at[0:4]
    rc(sends, sends, ag_s.at[2], t_r, seq_2=oc).wait_send()
    for one in list(cqkv.values()) + [cga, copy_t] + copy_q + copy_kv:
        one.wait_send()
    sends = rsend.at[:]
    rc(sends, sends, rs_s, t_r, seq_2=oc).wait_send()
    sends_done()


def put_kernel(oin, oqkv, dps, dpn, oi_hbm, oq_hbm, ok_hbm, ov_hbm, os_hbm, on_hbm, sem):
    copies = [
        pltpu.make_async_copy(dps.at[4 * k : 4 * k + 4], os_hbm.at[4 * k : 4 * k + 4], sem.at[k])
        for k in range(2)
    ]
    copies += [
        pltpu.make_async_copy(oqkv.at[t], ref, sem.at[2 + t])
        for t, ref in enumerate((oq_hbm, ok_hbm, ov_hbm))
    ]
    copies.append(pltpu.make_async_copy(oin, oi_hbm, sem.at[5]))
    copies.append(pltpu.make_async_copy(dpn, on_hbm, sem.at[6]))
    for copy in copies:
        copy.start()
    for copy in copies:
        copy.wait()


def body(x, wq, wk, wv, sketch, prefix_state, prefix_norm, d_attn, d_state, d_norm):
    any_ = pl.BlockSpec(memory_space=pl.ANY)
    v = pltpu.VMEM
    scratch = [
        v((8, TOK, 256), BF),
        v((3, 2048, 512), BF),
        v((3, TOK, 512), F32),
        v((3, 2, TOK, 256), BF),
        v((3, TOK, 256), BF),
        v((2, TOK, 256), BF),
        v((2, SK, 64), F32),
        v((4, 64, 1024), F32),
        v((8, 1024), F32),
        v((8, 64, 1024), F32),
        v((8, 1024), F32),
        v((256, 256), F32),
        v((256, 256), BF),
        v((256, 256), BF),
        v((2, 256, 256), BF),
        v((2, 256, CT), F32),
        v((2, 128, CT), F32),
        v((2, 128, CT), BF),
        v((CT, 128), BF),
        v((2, NF, 256), F32),
        v((2, 4, NP, CT), BF),
        v((4, 256, CT), BF),
        v((2, CT, 256), BF),
        v((4, 256, CT), BF),
        v((2, NP, 384), F32),
        v((384, 1024), BF),
        v((NP, 1024), BF),
        v((4, 80, CT), F32),
        v((256, CT), F32),
        v((4, CT, CT), BF),
        v((4, CT, CT), BF),
        v((4, CT, CT), BF),
        v((4, 80, CT), F32),
        v((NP, 128), F32),
        v((SK, 128), F32),
        v((128, NP), F32),
        v((4, NF, 256), F32),
        v((2, 128, CT), F32),
        v((256, CT), F32),
        v((2, NP, 256), F32),
        v((4, 80, NP), BF),
        v((2, NF, 256), BF),
        v((2, WIRE, 128), BF),
        v((2, CH, ROWS, 128), BF),
        v((2, CH, ROWS, 128), BF),
        v((2, WIRE, 128), BF),
        v((ROWS, 128), BF),
        v((2, WIRE, 128), BF),
        v((2, 3, 256, 256), BF),
        v((3, 2, TOK, 256), BF),
        v((4, TOK, 512), F32),
        v((2, 6, 128, 256), BF),
        v((2, 6, 128, 256), BF),
    ]
    sem = pltpu.SemaphoreType.DMA
    scratch += [
        sem((11,)), sem((3,)), sem((6,)), sem((9,)), sem((9,)), sem((2,)), sem((2,)),
        sem((2,)), sem((2,)), sem, sem, sem, sem((2, 6)),
    ]
    swap = (0, 2, 1)
    made = (
        v((TOK, 512), BF),
        v((3, TOK, 512), BF),
        v((8, 64, 1024), F32),
        v((8, 1024), F32),
    )
    held = pl.BlockSpec(memory_space=pltpu.VMEM)
    outs = pl.pallas_call(
        kernel,
        out_shape=made,
        in_specs=[any_] * 10,
        out_specs=(held,) * 4,
        scratch_shapes=scratch,
        compiler_params=pltpu.CompilerParams(
            collective_id=0, has_side_effects=True, vmem_limit_bytes=60 * 1024 * 1024
        ),
        name="sketch_bwd",
    )(
        x, wq, wk, wv, jnp.transpose(sketch, swap), jnp.transpose(prefix_state, swap),
        prefix_norm, d_attn, jnp.transpose(d_state, swap), d_norm,
    )
    rows = jax.ShapeDtypeStruct((TOK, 512), BF)
    outs = pl.pallas_call(
        put_kernel,
        out_shape=(
            rows, rows, rows, rows,
            jax.ShapeDtypeStruct((8, 64, 1024), F32),
            jax.ShapeDtypeStruct((8, 1024), F32),
        ),
        in_specs=[held] * 4,
        out_specs=(any_,) * 6,
        scratch_shapes=[sem((7,))],
        compiler_params=pltpu.CompilerParams(vmem_limit_bytes=1024 * 1024),
        name="put_out",
    )(*(pltpu.with_memory_space_constraint(o, pltpu.VMEM) for o in outs))
    return outs[:4] + (jnp.transpose(outs[4], swap), outs[5])


def solution(mesh):
    finer = Mesh(
        mesh.devices.reshape(4, 4, 2, mesh.shape["head"]), ("seq_0", "seq_1", "seq_2", "head")
    )
    state, rows = P("head", None, None), P("head", None)
    tokens, weight = P(SEQ, "head"), P(None, "head")
    return jax.shard_map(
        body,
        mesh=finer,
        in_specs=(tokens, weight, weight, weight, P(), state, rows, tokens, state, rows),
        out_specs=(tokens, tokens, tokens, tokens, state, rows),
        check_vma=False,
    )
```
